512 devices in a mesh: seq: 64 (over x, z), tensor: 8 (over y, core).
Axes of the slice: x: 4, y: 4, z: 16, core: 2. Of those that a mesh axis runs over, the one named last changes fastest.
Arguments:
- hidden: bfloat16 [8, 16384, 8192], P(None, 'seq', 'tensor'), may hold values from -160 to 160
- norm_gain: bfloat16 [8192], P('tensor'), may hold values from 0.25 to 1.75
- value_weight: bfloat16 [8192], P('tensor'), may hold values from -0.0625 to 0.0625
- rewards: float32 [8, 16384], P(None, 'seq'), may hold values from -6 to 6
- done_flags: int32 [8, 16384], P(None, 'seq'), may hold values 0 or 1
- valid_mask: int32 [8, 16384], P('tensor', 'seq'), may hold values 0 or 1
- new_logprob: float32 [8, 16384], P('tensor', 'seq'), may hold values from -1 to 1
- old_logprob: float32 [8, 16384], P('tensor', 'seq'), may hold values from -1 to 1
- discount: float32 [8], replicated, may hold values from 0.9 to 1
- trace_decay: float32 [8], replicated, may hold values from 0.9 to 1
- bootstrap: float32 [8], replicated, may hold values from -5 to 5
Outputs:
- values: float32 [8, 16384], P('tensor', 'seq')
- white_adv: float32 [8, 16384], P('tensor', 'seq')
- token_loss: float32 [8, 16384], P('tensor', 'seq')
- policy_loss: float32 [], replicated
The draws below stay inside these ranges and needn't reach their ends.
All inputs are finite; a program needn't handle non-finite values. No bound on the sum of `done_flags` or of `valid_mask` on one device may be relied on, other than what follows from the above.
Results may differ from the reference program's by a relative error of at most 0.00035.
Values sent between devices are 32-bit elements; how exact they have to be, the bound alone decides.
No kernel may reach another device: no remote copies, remote signals or barrier semaphores. Data moves between devices by JAX's collectives and lax.ppermute only.
A program may use at most 64 MiB of HBM per device.

```python
import math
from functools import partial
import jax
import jax.numpy as jnp
from jax import lax

H = 8192
LEN_DEV = 256
SEQS = 8
LENGTH = 16384


def draw_hidden(key, part):
    k_base, k_cols = jax.random.split(jax.random.fold_in(key, 11), 2)
    base = jax.random.truncated_normal(k_base, -4.0, 4.0, (SEQS, LENGTH, H), jnp.float32)
    columns = jnp.exp(jax.random.uniform(k_cols, (H,), jnp.float32) * math.log(10.0))
    drawn = base * columns
    return drawn.astype(jnp.bfloat16)


def draw_discount(key, part):
    k_main = jax.random.fold_in(key, 23)
    spread = jax.random.uniform(k_main, (SEQS,), jnp.float32, 0.1, 0.5)
    return 1.0 - spread / LENGTH


def draw_trace_decay(key, part):
    k_pick, k_slow, k_fast = jax.random.split(jax.random.fold_in(key, 37), 3)
    quick = jax.random.bernoulli(k_pick, 0.5, (SEQS,))
    slow_rate = 1.0 - jax.random.uniform(k_slow, (SEQS,), jnp.float32, 0.2, 1.0) / LENGTH
    fast_rate = 1.0 - jax.random.uniform(k_fast, (SEQS,), jnp.float32, 0.02, 0.033)
    return jnp.where(quick, fast_rate, slow_rate)


def touch_ends(entries, stream_key, low, largest):
    index_at = [jax.random.randint(jax.random.fold_in(stream_key, axis), (), 0, length) for axis, length in enumerate(entries.shape)]
    longest = entries.shape.index(max(entries.shape))
    beside = index_at[:longest] + [(index_at[longest] + 1) % entries.shape[longest]] + index_at[longest + 1:]
    return entries.at[tuple(index_at)].set(low).at[tuple(beside)].set(largest)


def block_scale(own_key, extent, shards, smallest, high):
    factor_of = 1.0
    for position, parts in shards:
        steps = jax.random.uniform(jax.random.fold_in(jax.random.fold_in(own_key, 6), position), (parts,), jnp.float32, smallest / len(shards), high / len(shards))
        factor_of = factor_of * jnp.repeat(jnp.exp(steps), extent[position] // parts).reshape((-1,) + (1,) * (len(extent) - 1 - position))
    return factor_of


def noise(key, dims, deviation, limit, shards=(), held_as=jnp.bfloat16):
    values = deviation * jax.random.normal(key, dims, jnp.float32)
    if shards:
        values = values * block_scale(key, dims, shards, -0.22, 0.18)
    return jnp.clip(values, -limit, limit).astype(held_as)


def setup_inputs(seed: int = 0) -> dict:
    seeds = jax.random.split(jax.random.key(seed), 12)
    return {
        "hidden": draw_hidden(jax.random.fold_in(seeds[11], 71), 0),
        "norm_gain": jnp.clip(1.0 + 0.15 * jax.random.normal(seeds[1], (H,), jnp.float32), 0.25, 1.75).astype(jnp.bfloat16),
        "value_weight": noise(seeds[2], (H,), H ** -0.5, 0.0625, ((0, 8),)),
        "rewards": noise(seeds[3], (SEQS, LENGTH), 1.0, 6.0, ((1, 64),), jnp.float32),
        "done_flags": touch_ends((jax.random.randint(seeds[4], (SEQS, LENGTH), 0, 128 * LEN_DEV) < 1).astype(jnp.int32), jax.random.fold_in(seeds[4], 1), 0, 1),
        "valid_mask": touch_ends((jax.random.randint(seeds[5], (SEQS, LENGTH), 0, 4) < 3).astype(jnp.int32), jax.random.fold_in(seeds[5], 1), 0, 1),
        "new_logprob": noise(seeds[6], (SEQS, LENGTH), 0.15, 1.0, ((0, 8), (1, 64)), jnp.float32),
        "old_logprob": noise(seeds[7], (SEQS, LENGTH), 0.15, 1.0, ((0, 8), (1, 64)), jnp.float32),
        "discount": draw_discount(jax.random.fold_in(seeds[11], 71), 0),
        "trace_decay": draw_trace_decay(jax.random.fold_in(seeds[11], 71), 0),
        "bootstrap": noise(seeds[10], (SEQS,), 1.0, 5.0, (), jnp.float32),
    }


EPS_NORM = 1e-06
EPS_WHITE = 1e-08
CLIP = 0.2

def head_block(scaled, block):
    wide = block.astype(jnp.float32)
    squares = lax.optimization_barrier(jnp.sum(wide * wide, axis=-1))
    products = jnp.dot(wide, scaled, precision=lax.Precision.HIGHEST)
    return products * lax.rsqrt(squares / H + EPS_NORM)

def backward_step(carry, inputs):
    delta_now, coef_now = inputs
    fresh = delta_now + coef_now * carry
    return (fresh, fresh)

def reference(hidden, norm_gain, value_weight, rewards, done_flags, valid_mask, new_logprob, old_logprob, discount, trace_decay, bootstrap):
    scaled = norm_gain.astype(jnp.float32) * value_weight.astype(jnp.float32)
    blocks = hidden.reshape(SEQS * LENGTH // LEN_DEV, LEN_DEV, H)
    values = lax.map(partial(head_block, scaled), blocks).reshape(SEQS, LENGTH)
    alive = 1.0 - done_flags.astype(jnp.float32)
    following = jnp.concatenate([values[:, 1:], bootstrap[:, None]], axis=1)
    delta = rewards + discount[:, None] * alive * following - values
    decay = discount * trace_decay
    coefs = decay[:, None] * alive
    start = jnp.zeros((SEQS,), jnp.float32)
    _, stacked = lax.scan(backward_step, start, (delta.T, coefs.T), reverse=True)
    advantages = stacked.T
    weight = valid_mask.astype(jnp.float32)
    count = jnp.sum(weight)
    mean = jnp.sum(weight * advantages) / count
    variance = jnp.sum(weight * (advantages - mean) ** 2) / count
    white_adv = (advantages - mean) * lax.rsqrt(variance + EPS_WHITE)
    ratio = jnp.exp(new_logprob - old_logprob)
    surrogate = jnp.minimum(ratio * white_adv, jnp.clip(ratio, 1.0 - CLIP, 1.0 + CLIP) * white_adv)
    token_loss = -weight * surrogate
    policy_loss = jnp.sum(token_loss) / count
    return (values, white_adv, token_loss, policy_loss)
```

```python
import jax
import jax.numpy as jnp
from jax import lax
from jax.experimental import pallas as pl
from jax.experimental.pallas import tpu as pltpu
from jax.sharding import PartitionSpec as P

EPS_NORM = 1e-06
EPS_WHITE = 1e-08
CLIP = 0.2

HEAD_ROWS = 40
TOKEN_ROWS = 5
WIDTH = 16
OFFSET, SLOPE, COUNT, MEAN_L, MEAN_C, VAR_L, COV, VAR_C, LAST_DONE = range(9)

CONTRACT_LANES = (((1,), (1,)), ((), ()))


def head_kernel(gain_ref, weight_ref, mask_ref, hidden_ref, out_ref, held, arrived):
    rollouts, length, width = held.shape
    peers = out_ref.shape[0] // HEAD_ROWS
    copies = [
        pltpu.make_async_copy(hidden_ref.at[r], held.at[r], arrived.at[r]) for r in range(rollouts)
    ]
    for copy in copies:
        copy.start()
    scaled = gain_ref[...].astype(jnp.float32) * weight_ref[...].astype(jnp.float32)
    coarse = scaled.astype(jnp.bfloat16).astype(jnp.float32)
    fine = scaled - coarse
    row = lax.broadcasted_iota(jnp.int32, (8, 128), 0)
    tiles = []
    for j in range(width // 128):
        tile = jnp.where(row == 0, coarse[j : j + 1, :], 0.0)
        tiles.append(jnp.where(row == 1, fine[j : j + 1, :], tile))
    lhs = jnp.concatenate(tiles, axis=1).astype(jnp.bfloat16)
    ones = jnp.ones((8, 256), jnp.bfloat16)
    mask = mask_ref[...].astype(jnp.float32)
    out_ref[32:33, :] = mask[:, :128]
    out_ref[33:34, :] = mask[:, 128:]
    out_ref[34:40, :] = jnp.zeros((6, 128), jnp.float32)
    for r in range(rollouts):
        copies[r].wait()
        block = held[r]
        products = lax.dot_general(lhs, block, CONTRACT_LANES, preferred_element_type=jnp.float32)
        products = products[0:1, :] + products[1:2, :]
        total = jnp.zeros((length, 128), jnp.float32)
        for j in range(width // 128):
            wide = held[r, :, 128 * j : 128 * (j + 1)].astype(jnp.float32)
            total = total + wide * wide
        high = total.astype(jnp.bfloat16)
        low = (total - high.astype(jnp.float32)).astype(jnp.bfloat16)
        squares = lax.dot_general(
            ones,
            jnp.concatenate([high, low], axis=1),
            CONTRACT_LANES,
            preferred_element_type=jnp.float32,
        )
        out_ref[r : r + 1, :] = squares[0:1, :128]
        out_ref[8 + r : 9 + r, :] = squares[0:1, 128:]
        out_ref[16 + r : 17 + r, :] = products[:, :128]
        out_ref[24 + r : 25 + r, :] = products[:, 128:]
    own = out_ref[0:HEAD_ROWS, :]
    for peer in range(1, peers):
        out_ref[HEAD_ROWS * peer : HEAD_ROWS * (peer + 1), :] = own


def column(ref, shape):
    row = lax.broadcasted_iota(jnp.int32, shape, 0)
    out = jnp.full(shape, ref[0], jnp.float32)
    for r in range(1, shape[0]):
        out = jnp.where(row == r, ref[r], out)
    return out


def lane_sum(x):
    return jnp.sum(x, axis=1, keepdims=True)


def local_kernel(
    hidden_width,
    discount_ref,
    trace_ref,
    recv_ref,
    rewards_ref,
    done_ref,
    new_ref,
    old_ref,
    mask_ref,
    values_ref,
    out_ref,
):
    me = lax.axis_index("tensor")
    rollouts, length = rewards_ref.shape
    peers = recv_ref.shape[0] // HEAD_ROWS
    shape = (rollouts, length)
    total = recv_ref[0:32, :]
    for peer in range(1, peers):
        total = total + recv_ref[HEAD_ROWS * peer : HEAD_ROWS * peer + 32, :]
    squares = jnp.concatenate([total[0:8], total[8:16]], axis=1)
    products = jnp.concatenate([total[16:24], total[24:32]], axis=1)
    weight = jnp.concatenate(
        [
            recv_ref[pl.ds(32, peers, stride=HEAD_ROWS), :],
            recv_ref[pl.ds(33, peers, stride=HEAD_ROWS), :],
        ],
        axis=1,
    )
    values = products * lax.rsqrt(squares / hidden_width + EPS_NORM)
    discount, trace = column(discount_ref, shape), column(trace_ref, shape)
    alive = 1.0 - done_ref[...].astype(jnp.float32)
    lane = lax.broadcasted_iota(jnp.int32, shape, 1)
    inner_next = jnp.where(lane < length - 1, pltpu.roll(values, length - 1, 1), 0.0)
    local = rewards_ref[...] + discount * alive * inner_next - values
    chain = discount * trace * alive
    step = 1
    while step < length:
        inside = lane < length - step
        local_later = jnp.where(inside, pltpu.roll(local, length - step, 1), 0.0)
        chain_later = jnp.where(inside, pltpu.roll(chain, length - step, 1), 1.0)
        local = local + chain * local_later
        chain = chain * chain_later
        step *= 2
    coef = chain / trace
    count = lane_sum(weight)
    safe = 1.0 / jnp.maximum(count, 1.0)
    mean_l = lane_sum(weight * local) * safe
    mean_c = lane_sum(weight * coef) * safe
    off_l = weight * (local - mean_l)
    off_c = weight * (coef - mean_c)
    stats = {
        OFFSET: values[:, 0:1] + trace[:, 0:1] * local[:, 0:1],
        SLOPE: chain[:, 0:1],
        COUNT: count,
        MEAN_L: mean_l,
        MEAN_C: mean_c,
        VAR_L: lane_sum(off_l * off_l),
        COV: lane_sum(off_l * off_c),
        VAR_C: lane_sum(off_c * off_c),
        LAST_DONE: jnp.max(
            jnp.where(alive > 0.5, -1.0, lane.astype(jnp.float32)), axis=1, keepdims=True
        ),
    }
    small_lane = lax.broadcasted_iota(jnp.int32, (rollouts, 128), 1)
    summary = jnp.zeros((rollouts, 128), jnp.float32)
    for at, stat in stats.items():
        summary = jnp.where(small_lane == at, stat, summary)
    summary = pltpu.roll(summary, 0, 1, stride=WIDTH, stride_axis=0)
    summary = jnp.sum(summary, axis=0, keepdims=True)
    mine = lax.broadcasted_iota(jnp.int32, shape, 0) == me
    own_local = jnp.sum(jnp.where(mine, local, 0.0), axis=0, keepdims=True)
    values_ref[...] = jnp.sum(jnp.where(mine, values, 0.0), axis=0, keepdims=True)
    ratio = mask_ref[...].astype(jnp.float32) * jnp.exp(new_ref[...] - old_ref[...])
    row = lax.broadcasted_iota(jnp.int32, (8, 128), 0)
    message = jnp.where(row == 0, summary, 0.0)
    message = jnp.where(row == 1, own_local[:, :128], message)
    message = jnp.where(row == 2, own_local[:, 128:], message)
    message = jnp.where(row == 3, ratio[:, :128], message)
    message = jnp.where(row == 4, ratio[:, 128:], message)
    for peer in range(out_ref.shape[0] // TOKEN_ROWS):
        out_ref[TOKEN_ROWS * peer : TOKEN_ROWS * (peer + 1), :] = message[0:TOKEN_ROWS, :]


def full_sum(x):
    return jnp.sum(jnp.sum(x, axis=0, keepdims=True), axis=1, keepdims=True)


def final_kernel(
    discount_ref, trace_ref, bootstrap_ref, recv_ref, white_ref, loss_ref, out_ref
):
    tensor, seq = lax.axis_index("tensor"), lax.axis_index("seq")
    blocks = recv_ref.shape[0] // TOKEN_ROWS
    rollouts = out_ref.shape[0]
    shape = (blocks, 128)
    table = recv_ref[pl.ds(0, blocks, stride=TOKEN_ROWS), :]
    row = lax.broadcasted_iota(jnp.int32, shape, 0)
    lane = lax.broadcasted_iota(jnp.int32, shape, 1)

    def stat(at):
        return pltpu.roll(table, 128 - at, 1)

    start = jnp.full(shape, bootstrap_ref[0], jnp.float32)
    for r in range(1, rollouts):
        start = jnp.where(lane == WIDTH * r, bootstrap_ref[r], start)
    last = row == blocks - 1
    offset = jnp.where(last, start, pltpu.roll(table, blocks - 1, 0))
    slope = jnp.where(last, 0.0, pltpu.roll(stat(SLOPE), blocks - 1, 0))
    step = 1
    while step < blocks:
        inside = row < blocks - step
        offset_later = jnp.where(inside, pltpu.roll(offset, blocks - step, 0), 0.0)
        slope_later = jnp.where(inside, pltpu.roll(slope, blocks - step, 0), 0.0)
        offset = offset + slope * offset_later
        slope = slope * slope_later
        step *= 2
    entering = offset
    used = (lane % WIDTH == 0) & (lane < WIDTH * rollouts)
    members = jnp.where(used, stat(COUNT), 0.0)
    block_mean = jnp.where(used, stat(MEAN_L) + entering * stat(MEAN_C), 0.0)
    count = full_sum(members)
    mean = full_sum(members * block_mean) / count
    within = stat(VAR_L) + entering * (2.0 * stat(COV) + entering * stat(VAR_C))
    apart = block_mean - mean
    variance = full_sum(jnp.where(used, within, 0.0) + members * apart * apart) / count
    scale = lax.rsqrt(variance + EPS_WHITE)

    mine = lane == WIDTH * tensor
    own_entering = lane_sum(jnp.where(mine, entering, 0.0))
    own_done = lane_sum(jnp.where(mine, stat(LAST_DONE), 0.0))
    discount = discount_ref[tensor]
    decay = discount * trace_ref[tensor]
    loss = jnp.zeros(shape, jnp.float32)
    own = pl.ds(TOKEN_ROWS * seq, 1)
    for half in range(2):
        position = lax.broadcasted_iota(jnp.int32, (1, 128), 1) + 128 * half
        left = 255 - position
        power, factor = jnp.full((1, 128), discount, jnp.float32), jnp.full((1, 128), decay)
        for bit in range(8):
            power = jnp.where((left >> bit) & 1 == 1, power * factor, power)
            factor = factor * factor
        coef = jnp.where(position.astype(jnp.float32) > own_done, power, 0.0)
        local = recv_ref[pl.ds(1 + half, blocks, stride=TOKEN_ROWS), :]
        ratio = recv_ref[pl.ds(3 + half, blocks, stride=TOKEN_ROWS), :]
        white = (local + coef * own_entering - mean) * scale
        clipped = jnp.clip(ratio, 1.0 - CLIP, 1.0 + CLIP)
        token = jnp.where(ratio > 0.0, -jnp.minimum(ratio * white, clipped * white), 0.0)
        loss = loss + token
        mine_row = row == seq
        white_ref[:, 128 * half : 128 * (half + 1)] = jnp.sum(
            jnp.where(mine_row, white, 0.0), axis=0, keepdims=True
        )
        loss_ref[:, 128 * half : 128 * (half + 1)] = jnp.sum(
            jnp.where(mine_row, token, 0.0), axis=0, keepdims=True
        )
    out_ref[...] = jnp.broadcast_to(full_sum(loss) / count, out_ref.shape)


VMEM = pl.BlockSpec(memory_space=pltpu.VMEM)
SMEM = pl.BlockSpec(memory_space=pltpu.SMEM)
ANY = pl.BlockSpec(memory_space=pl.ANY)


def exchange(x, axis):
    return lax.all_to_all(x, axis, 0, 0, tiled=True)


def shards(
    hidden,
    norm_gain,
    value_weight,
    rewards,
    done_flags,
    valid_mask,
    new_logprob,
    old_logprob,
    discount,
    trace_decay,
    bootstrap,
):
    rollouts, length, width = hidden.shape
    peers, blocks = lax.axis_size("tensor"), lax.axis_size("seq")
    f32 = jnp.float32
    sent = pl.pallas_call(
        head_kernel,
        out_shape=jax.ShapeDtypeStruct((peers * HEAD_ROWS, 128), f32),
        in_specs=[VMEM, VMEM, VMEM, ANY],
        out_specs=VMEM,
        scratch_shapes=[
            pltpu.VMEM(hidden.shape, hidden.dtype),
            pltpu.SemaphoreType.DMA((rollouts,)),
        ],
        name="head",
    )(
        norm_gain.reshape(-1, 128),
        value_weight.reshape(-1, 128),
        valid_mask,
        hidden,
    )
    got = exchange(sent.reshape(peers, 1, HEAD_ROWS * 128), "tensor")
    own_row = jax.ShapeDtypeStruct((1, length), f32)
    values, sent = pl.pallas_call(
        lambda *refs: local_kernel(width * peers, *refs),
        out_shape=(own_row, jax.ShapeDtypeStruct((blocks * TOKEN_ROWS, 128), f32)),
        in_specs=[SMEM, SMEM] + [VMEM] * 6,
        out_specs=(VMEM, VMEM),
        name="local",
    )(
        discount,
        trace_decay,
        got.reshape(peers * HEAD_ROWS, 128),
        rewards,
        done_flags,
        new_logprob,
        old_logprob,
        valid_mask,
    )
    got = exchange(sent.reshape(blocks, 1, TOKEN_ROWS * 128), "seq")
    white, loss, sent = pl.pallas_call(
        final_kernel,
        out_shape=(own_row, own_row, jax.ShapeDtypeStruct((peers, 128), f32)),
        in_specs=[SMEM, SMEM, SMEM, VMEM],
        out_specs=(VMEM, VMEM, VMEM),
        name="final",
    )(discount, trace_decay, bootstrap, got.reshape(blocks * TOKEN_ROWS, 128))
    got = exchange(sent.reshape(peers, 1, 128), "tensor")
    return values, white, loss, jnp.sum(got[:, 0, 0])


def solution(mesh):
    in_specs = (
        P(None, "seq", "tensor"),
        P("tensor"),
        P("tensor"),
        P(None, "seq"),
        P(None, "seq"),
        P("tensor", "seq"),
        P("tensor", "seq"),
        P("tensor", "seq"),
        P(),
        P(),
        P(),
    )
    out_specs = (P("tensor", "seq"), P("tensor", "seq"), P("tensor", "seq"), P())
    return jax.shard_map(
        shards, mesh=mesh, in_specs=in_specs, out_specs=out_specs, check_vma=False
    )
```

```python
import jax
import jax.numpy as jnp
from jax import lax
from jax.experimental import pallas as pl
from jax.experimental.pallas import tpu as pltpu
from jax.sharding import PartitionSpec as P

EPS_NORM = 1e-06
EPS_WHITE = 1e-08
CLIP = 0.2

HEAD_ROWS = 40
TOKEN_ROWS = 5
WIDTH = 16
OFFSET, SLOPE, COUNT, MEAN_L, MEAN_C, VAR_L, COV, VAR_C, LAST_DONE = range(9)

CONTRACT_LANES = (((1,), (1,)), ((), ()))


def column(ref, shape):
    row = lax.broadcasted_iota(jnp.int32, shape, 0)
    out = jnp.full(shape, ref[0], jnp.float32)
    for r in range(1, shape[0]):
        out = jnp.where(row == r, ref[r], out)
    return out


def lane_sum(x):
    return jnp.sum(x, axis=1, keepdims=True)


def head_kernel(
    gain_hbm,
    weight_hbm,
    done_hbm,
    mask_hbm,
    new_hbm,
    old_hbm,
    discount_hbm,
    trace_hbm,
    bootstrap_hbm,
    hidden_ref,
    out_ref,
    gate_ref,
    chain_ref,
    coef_ref,
    power_ref,
    fixed_ref,
    trace_ref,
    ratio_ref,
    start_ref,
    held,
    gain_ref,
    weight_ref,
    done_ref,
    mask_ref,
    new_ref,
    old_ref,
    discount_smem,
    trace_smem,
    bootstrap_smem,
    arrived,
):
    rollouts, length, width = held.shape
    peers = out_ref.shape[0] // HEAD_ROWS
    small = [
        pltpu.make_async_copy(source, target, arrived.at[rollouts + i])
        for i, (source, target) in enumerate(
            (
                (gain_hbm, gain_ref),
                (weight_hbm, weight_ref),
                (done_hbm, done_ref),
                (mask_hbm, mask_ref),
                (new_hbm, new_ref),
                (old_hbm, old_ref),
                (discount_hbm, discount_smem),
                (trace_hbm, trace_smem),
                (bootstrap_hbm, bootstrap_smem),
            )
        )
    ]
    copies = [
        pltpu.make_async_copy(hidden_ref.at[r], held.at[r], arrived.at[r]) for r in range(rollouts)
    ]
    for copy in small + copies:
        copy.start()
    for copy in small:
        copy.wait()

    shape = (rollouts, length)
    lane = lax.broadcasted_iota(jnp.int32, shape, 1)
    discount, trace = column(discount_smem, shape), column(trace_smem, shape)
    alive = 1.0 - done_ref[...].astype(jnp.float32)
    gate_ref[...] = discount * alive
    decay = discount * trace
    chain = decay * alive
    step, at = 1, 0
    while step < length:
        chain_ref[rollouts * at : rollouts * (at + 1), :] = chain
        later = pltpu.roll(chain, length - step, 1)
        chain = chain * jnp.where(lane < length - step, later, 1.0)
        step, at = 2 * step, at + 1
    coef_ref[...] = chain / trace
    left = length - 1 - lane
    power, factor, bit = discount, decay, 1
    while bit < length:
        power = jnp.where(left & bit != 0, power * factor, power)
        factor = factor * factor
        bit *= 2
    power_ref[...] = power
    last_done = jnp.max(
        jnp.where(alive > 0.5, -1.0, lane.astype(jnp.float32)), axis=1, keepdims=True
    )
    small_lane = lax.broadcasted_iota(jnp.int32, (rollouts, 128), 1)
    fixed = jnp.where(small_lane == SLOPE, chain[:, 0:1], 0.0)
    fixed_ref[...] = jnp.where(small_lane == LAST_DONE, last_done, fixed)
    trace_ref[...] = trace[:, :128]
    mask = mask_ref[...].astype(jnp.float32)
    ratio_ref[...] = mask * jnp.exp(new_ref[...] - old_ref[...])
    start_lane = lax.broadcasted_iota(jnp.int32, (1, 128), 1)
    start = jnp.full((1, 128), bootstrap_smem[0], jnp.float32)
    for r in range(1, rollouts):
        start = jnp.where(start_lane == WIDTH * r, bootstrap_smem[r], start)
    start_ref[...] = start

    scaled = gain_ref[...].astype(jnp.float32) * weight_ref[...].astype(jnp.float32)
    coarse = scaled.astype(jnp.bfloat16).astype(jnp.float32)
    fine = scaled - coarse
    row = lax.broadcasted_iota(jnp.int32, (8, 128), 0)
    tiles = []
    for j in range(width // 128):
        tile = jnp.where(row == 0, coarse[j : j + 1, :], 0.0)
        tiles.append(jnp.where(row == 1, fine[j : j + 1, :], tile))
    lhs = jnp.concatenate(tiles, axis=1).astype(jnp.bfloat16)
    ones = jnp.ones((8, 256), jnp.bfloat16)
    out_ref[32:33, :] = mask[:, :128]
    out_ref[33:34, :] = mask[:, 128:]
    out_ref[34:40, :] = jnp.zeros((6, 128), jnp.float32)
    for r in range(rollouts):
        copies[r].wait()
        block = held[r]
        products = lax.dot_general(lhs, block, CONTRACT_LANES, preferred_element_type=jnp.float32)
        products = products[0:1, :] + products[1:2, :]
        total = jnp.zeros((length, 128), jnp.float32)
        for j in range(width // 128):
            wide = held[r, :, 128 * j : 128 * (j + 1)].astype(jnp.float32)
            total = total + wide * wide
        high = total.astype(jnp.bfloat16)
        low = (total - high.astype(jnp.float32)).astype(jnp.bfloat16)
        squares = lax.dot_general(
            ones,
            jnp.concatenate([high, low], axis=1),
            CONTRACT_LANES,
            preferred_element_type=jnp.float32,
        )
        out_ref[r : r + 1, :] = squares[0:1, :128]
        out_ref[8 + r : 9 + r, :] = squares[0:1, 128:]
        out_ref[16 + r : 17 + r, :] = products[:, :128]
        out_ref[24 + r : 25 + r, :] = products[:, 128:]
    own = out_ref[0:HEAD_ROWS, :]
    for peer in range(1, peers):
        out_ref[HEAD_ROWS * peer : HEAD_ROWS * (peer + 1), :] = own


def local_kernel(
    hidden_width,
    recv_ref,
    rewards_ref,
    gate_ref,
    chain_ref,
    coef_ref,
    fixed_ref,
    trace_ref,
    ratio_ref,
    values_ref,
    out_ref,
):
    me = lax.axis_index("tensor")
    rollouts, length = rewards_ref.shape
    peers = recv_ref.shape[0] // HEAD_ROWS
    shape = (rollouts, length)
    total = recv_ref[0:32, :]
    for peer in range(1, peers):
        total = total + recv_ref[HEAD_ROWS * peer : HEAD_ROWS * peer + 32, :]
    squares = jnp.concatenate([total[0:8], total[8:16]], axis=1)
    products = jnp.concatenate([total[16:24], total[24:32]], axis=1)
    weight = jnp.concatenate(
        [
            recv_ref[pl.ds(32, peers, stride=HEAD_ROWS), :],
            recv_ref[pl.ds(33, peers, stride=HEAD_ROWS), :],
        ],
        axis=1,
    )
    values = products * lax.rsqrt(squares / hidden_width + EPS_NORM)
    lane = lax.broadcasted_iota(jnp.int32, shape, 1)
    inner_next = jnp.where(lane < length - 1, pltpu.roll(values, length - 1, 1), 0.0)
    local = rewards_ref[...] + gate_ref[...] * inner_next - values
    step, at = 1, 0
    while step < length:
        later = jnp.where(lane < length - step, pltpu.roll(local, length - step, 1), 0.0)
        local = local + chain_ref[rollouts * at : rollouts * (at + 1), :] * later
        step, at = 2 * step, at + 1
    coef = coef_ref[...]
    count = lane_sum(weight)
    safe = 1.0 / jnp.maximum(count, 1.0)
    mean_l = lane_sum(weight * local) * safe
    mean_c = lane_sum(weight * coef) * safe
    off_l = weight * (local - mean_l)
    off_c = weight * (coef - mean_c)
    stats = {
        OFFSET: values[:, 0:1] + trace_ref[:, 0:1] * local[:, 0:1],
        COUNT: count,
        MEAN_L: mean_l,
        MEAN_C: mean_c,
        VAR_L: lane_sum(off_l * off_l),
        COV: lane_sum(off_l * off_c),
        VAR_C: lane_sum(off_c * off_c),
    }
    small_lane = lax.broadcasted_iota(jnp.int32, (rollouts, 128), 1)
    summary = fixed_ref[...]
    for at, stat in stats.items():
        summary = jnp.where(small_lane == at, stat, summary)
    summary = pltpu.roll(summary, 0, 1, stride=WIDTH, stride_axis=0)
    summary = jnp.sum(summary, axis=0, keepdims=True)
    mine = lax.broadcasted_iota(jnp.int32, shape, 0) == me
    own_local = jnp.sum(jnp.where(mine, local, 0.0), axis=0, keepdims=True)
    values_ref[...] = jnp.sum(jnp.where(mine, values, 0.0), axis=0, keepdims=True)
    row = lax.broadcasted_iota(jnp.int32, (8, 128), 0)
    message = jnp.where(row == 0, summary, 0.0)
    message = jnp.where(row == 1, own_local[:, :128], message)
    message = jnp.where(row == 2, own_local[:, 128:], message)
    message = jnp.where(row == 3, ratio_ref[:, :128], message)
    message = jnp.where(row == 4, ratio_ref[:, 128:], message)
    for peer in range(out_ref.shape[0] // TOKEN_ROWS):
        out_ref[TOKEN_ROWS * peer : TOKEN_ROWS * (peer + 1), :] = message[0:TOKEN_ROWS, :]


def full_sum(x):
    return jnp.sum(jnp.sum(x, axis=0, keepdims=True), axis=1, keepdims=True)


def final_kernel(
    recv_ref,
    power_ref,
    start_ref,
    values_ref,
    values_hbm,
    white_hbm,
    loss_hbm,
    out_ref,
    white_ref,
    loss_ref,
    sent,
):
    tensor, seq = lax.axis_index("tensor"), lax.axis_index("seq")
    writes = [
        pltpu.make_async_copy(source, target, sent.at[i])
        for i, (source, target) in enumerate(
            ((values_ref, values_hbm), (white_ref, white_hbm), (loss_ref, loss_hbm))
        )
    ]
    writes[0].start()
    blocks = recv_ref.shape[0] // TOKEN_ROWS
    rollouts = out_ref.shape[0]
    shape = (blocks, 128)
    table = recv_ref[pl.ds(0, blocks, stride=TOKEN_ROWS), :]
    row = lax.broadcasted_iota(jnp.int32, shape, 0)
    lane = lax.broadcasted_iota(jnp.int32, shape, 1)

    def stat(at):
        return pltpu.roll(table, 128 - at, 1)

    last = row == blocks - 1
    offset = jnp.where(last, start_ref[...], pltpu.roll(table, blocks - 1, 0))
    slope = jnp.where(last, 0.0, pltpu.roll(stat(SLOPE), blocks - 1, 0))
    step = 1
    while step < blocks:
        inside = row < blocks - step
        offset_later = jnp.where(inside, pltpu.roll(offset, blocks - step, 0), 0.0)
        slope_later = jnp.where(inside, pltpu.roll(slope, blocks - step, 0), 0.0)
        offset = offset + slope * offset_later
        slope = slope * slope_later
        step *= 2
    entering = offset
    used = (lane % WIDTH == 0) & (lane < WIDTH * rollouts)
    members = jnp.where(used, stat(COUNT), 0.0)
    block_mean = jnp.where(used, stat(MEAN_L) + entering * stat(MEAN_C), 0.0)
    count = full_sum(members)
    mean = full_sum(members * block_mean) / count
    within = stat(VAR_L) + entering * (2.0 * stat(COV) + entering * stat(VAR_C))
    apart = block_mean - mean
    variance = full_sum(jnp.where(used, within, 0.0) + members * apart * apart) / count
    scale = lax.rsqrt(variance + EPS_WHITE)

    mine = lane == WIDTH * tensor
    own_entering = lane_sum(jnp.where(mine, entering, 0.0))
    own_done = lane_sum(jnp.where(mine, stat(LAST_DONE), 0.0))
    power = power_ref[pl.ds(tensor, 1), :]
    loss = jnp.zeros(shape, jnp.float32)
    mine_row = row == seq
    for half in range(2):
        lanes = slice(128 * half, 128 * (half + 1))
        position = (lane + 128 * half).astype(jnp.float32)
        coef = jnp.where(position > own_done, power[:, lanes], 0.0)
        local = recv_ref[pl.ds(1 + half, blocks, stride=TOKEN_ROWS), :]
        ratio = recv_ref[pl.ds(3 + half, blocks, stride=TOKEN_ROWS), :]
        white = (local + coef * own_entering - mean) * scale
        clipped = jnp.clip(ratio, 1.0 - CLIP, 1.0 + CLIP)
        token = jnp.where(ratio > 0.0, -jnp.minimum(ratio * white, clipped * white), 0.0)
        loss = loss + token
        white_ref[:, lanes] = jnp.sum(jnp.where(mine_row, white, 0.0), axis=0, keepdims=True)
        loss_ref[:, lanes] = jnp.sum(jnp.where(mine_row, token, 0.0), axis=0, keepdims=True)
    writes[1].start()
    writes[2].start()
    out_ref[...] = jnp.broadcast_to(full_sum(loss) / count, out_ref.shape)
    for write in writes:
        write.wait()


VMEM = pl.BlockSpec(memory_space=pltpu.VMEM)
ANY = pl.BlockSpec(memory_space=pl.ANY)


def on_chip(x):
    return pltpu.with_memory_space_constraint(x, pltpu.VMEM)


def on_chip_shape(shape):
    return pltpu.VMEM(shape, jnp.float32)


def exchange(x, axis):
    return lax.all_to_all(x, axis, 0, 0, tiled=True)


def shards(
    hidden,
    norm_gain,
    value_weight,
    rewards,
    done_flags,
    valid_mask,
    new_logprob,
    old_logprob,
    discount,
    trace_decay,
    bootstrap,
):
    rollouts, length, width = hidden.shape
    peers, blocks = lax.axis_size("tensor"), lax.axis_size("seq")
    f32 = jnp.float32
    steps = length.bit_length() - 1
    sent, gate, chain, coef, power, fixed, trace, ratio, start = pl.pallas_call(
        head_kernel,
        out_shape=(
            on_chip_shape((peers * HEAD_ROWS, 128)),
            on_chip_shape((rollouts, length)),
            on_chip_shape((rollouts * steps, length)),
            on_chip_shape((rollouts, length)),
            on_chip_shape((rollouts, length)),
            on_chip_shape((rollouts, 128)),
            on_chip_shape((rollouts, 128)),
            on_chip_shape((1, length)),
            on_chip_shape((1, 128)),
        ),
        in_specs=[ANY] * 10,
        out_specs=(VMEM,) * 9,
        scratch_shapes=[
            pltpu.VMEM(hidden.shape, hidden.dtype),
            pltpu.VMEM((width // 128, 128), norm_gain.dtype),
            pltpu.VMEM((width // 128, 128), value_weight.dtype),
            pltpu.VMEM(done_flags.shape, done_flags.dtype),
            pltpu.VMEM(valid_mask.shape, valid_mask.dtype),
            pltpu.VMEM(new_logprob.shape, f32),
            pltpu.VMEM(old_logprob.shape, f32),
            pltpu.SMEM(discount.shape, f32),
            pltpu.SMEM(trace_decay.shape, f32),
            pltpu.SMEM(bootstrap.shape, f32),
            pltpu.SemaphoreType.DMA((rollouts + 9,)),
        ],
        name="head",
    )(
        norm_gain.reshape(-1, 128),
        value_weight.reshape(-1, 128),
        done_flags,
        valid_mask,
        new_logprob,
        old_logprob,
        discount,
        trace_decay,
        bootstrap,
        hidden,
    )
    got = exchange(sent.reshape(peers, 1, HEAD_ROWS * 128), "tensor")
    values, sent = pl.pallas_call(
        lambda *refs: local_kernel(width * peers, *refs),
        out_shape=(
            on_chip_shape((1, length)),
            on_chip_shape((blocks * TOKEN_ROWS, 128)),
        ),
        in_specs=[VMEM] * 8,
        out_specs=(VMEM, VMEM),
        name="local",
    )(
        *map(
            on_chip,
            (
                got.reshape(peers * HEAD_ROWS, 128),
                rewards,
                gate,
                chain,
                coef,
                fixed,
                trace,
                ratio,
            ),
        )
    )
    got = exchange(sent.reshape(blocks, 1, TOKEN_ROWS * 128), "seq")
    own_row = jax.ShapeDtypeStruct((1, length), f32)
    values, white, loss, sent = pl.pallas_call(
        final_kernel,
        out_shape=(own_row, own_row, own_row, on_chip_shape((peers, 128))),
        in_specs=[VMEM] * 4,
        out_specs=(ANY, ANY, ANY, VMEM),
        scratch_shapes=[
            pltpu.VMEM((1, length), f32),
            pltpu.VMEM((1, length), f32),
            pltpu.SemaphoreType.DMA((3,)),
        ],
        name="final",
    )(*map(on_chip, (got.reshape(blocks * TOKEN_ROWS, 128), power, start, values)))
    got = exchange(sent.reshape(peers, 1, 128), "tensor")
    return values, white, loss, jnp.sum(got[:, 0, 0])


def solution(mesh):
    in_specs = (
        P(None, "seq", "tensor"),
        P("tensor"),
        P("tensor"),
        P(None, "seq"),
        P(None, "seq"),
        P("tensor", "seq"),
        P("tensor", "seq"),
        P("tensor", "seq"),
        P(),
        P(),
        P(),
    )
    out_specs = (P("tensor", "seq"), P("tensor", "seq"), P("tensor", "seq"), P())
    return jax.shard_map(
        shards, mesh=mesh, in_specs=in_specs, out_specs=out_specs, check_vma=False
    )
```

```python
from functools import partial

import jax
import jax.numpy as jnp
from jax import lax
from jax.experimental import pallas as pl
from jax.experimental.pallas import tpu as pltpu
from jax.sharding import PartitionSpec as P

EPS_NORM = 1e-06
EPS_WHITE = 1e-08
CLIP = 0.2

HEAD_ROWS = 40
TOKEN_ROWS = 5
WIDTH = 16
OFFSET, SLOPE, COUNT, MEAN_L, MEAN_C, VAR_L, COV, VAR_C, LAST_DONE = range(9)

CHUNK = 64

CONTRACT_LANES = (((1,), (1,)), ((), ()))


def column(ref, shape):
    row = lax.broadcasted_iota(jnp.int32, shape, 0)
    out = jnp.full(shape, ref[0], jnp.float32)
    for r in range(1, shape[0]):
        out = jnp.where(row == r, ref[r], out)
    return out


def lane_sum(x):
    return jnp.sum(x, axis=1, keepdims=True)


def head_kernel(
    gain_hbm,
    weight_hbm,
    done_hbm,
    mask_hbm,
    new_hbm,
    old_hbm,
    discount_hbm,
    trace_hbm,
    bootstrap_hbm,
    hidden_ref,
    out_ref,
    gate_ref,
    chain_ref,
    coef_ref,
    power_ref,
    fixed_ref,
    trace_ref,
    ratio_ref,
    start_ref,
    held,
    gain_ref,
    weight_ref,
    done_ref,
    mask_ref,
    new_ref,
    old_ref,
    discount_smem,
    trace_smem,
    bootstrap_smem,
    fold_ref,
    arrived,
):
    rollouts, length, width = held.shape
    peers = out_ref.shape[0] // HEAD_ROWS
    small = [
        pltpu.make_async_copy(source, target, arrived.at[rollouts + i])
        for i, (source, target) in enumerate(
            (
                (gain_hbm, gain_ref),
                (weight_hbm, weight_ref),
                (done_hbm, done_ref),
                (mask_hbm, mask_ref),
                (new_hbm, new_ref),
                (old_hbm, old_ref),
                (discount_hbm, discount_smem),
                (trace_hbm, trace_smem),
                (bootstrap_hbm, bootstrap_smem),
            )
        )
    ]
    copies = [
        pltpu.make_async_copy(hidden_ref.at[r], held.at[r], arrived.at[r]) for r in range(rollouts)
    ]
    for copy in copies[:1] + small + copies[1:]:
        copy.start()
    for copy in small:
        copy.wait()

    scaled = gain_ref[...].astype(jnp.float32) * weight_ref[...].astype(jnp.float32)
    small_lane = lax.broadcasted_iota(jnp.int32, (8, 128), 1)
    levels = rollouts.bit_length() - 1
    group = 64 >> levels

    def fold(even, odd, distance):
        even = even + pltpu.roll(even, 128 - distance, 1)
        odd = odd + pltpu.roll(odd, distance, 1)
        return jnp.where((small_lane[0:1] // distance) % 2 == 0, even, odd)

    def partial_sums(r, here):
        squares = products = jnp.zeros((CHUNK, 128), jnp.float32)
        for j in range(width // 128):
            wide = held[r, here, 128 * j : 128 * (j + 1)].astype(jnp.float32)
            squares = squares + wide * wide
            products = products + wide * scaled[j : j + 1, :]
        folded, distance = fold(squares, products, 64), 32
        for level in range(levels):
            if not (r >> level) & 1:
                fold_ref[level, here] = folded
                return None
            folded, distance = fold(fold_ref[level, here], folded, distance), distance // 2
        return folded

    def finish(half, folded):
        turned = jnp.transpose(folded)
        sublane = lax.broadcasted_iota(jnp.int32, (8, 128), 0)
        for kind in range(2):
            rows = []
            for r in range(rollouts):
                at = kind
                for level in range(levels):
                    at = 2 * at + (r >> level) % 2
                rows.append(turned[group * at : group * (at + 1)])
            distance = group // 2
            while distance:
                even, odd = rows[:distance], rows[distance:]
                rows = []
                for e, o in zip(even, odd, strict=True):
                    e = e + pltpu.roll(e, 8 - distance, 0)
                    o = o + pltpu.roll(o, distance, 0)
                    rows.append(jnp.where((sublane // distance) % 2 == 0, e, o))
                distance //= 2
            for peer in range(peers):
                at = HEAD_ROWS * peer + 8 * (2 * kind + half)
                out_ref[at : at + 8, :] = rows[0]

    shape = (rollouts, length)
    lane = lax.broadcasted_iota(jnp.int32, shape, 1)

    def piece_own():
        mask = mask_ref[...].astype(jnp.float32)
        ratio_ref[...] = mask * jnp.exp(new_ref[...] - old_ref[...])
        row = lax.broadcasted_iota(jnp.int32, (8, 128), 0)
        rest = jnp.where(row == 0, mask[:, :128], jnp.where(row == 1, mask[:, 128:], 0.0))
        for peer in range(peers):
            out_ref[HEAD_ROWS * peer + 32 : HEAD_ROWS * (peer + 1), :] = rest
        start_lane = lax.broadcasted_iota(jnp.int32, (1, 128), 1)
        start = jnp.full((1, 128), bootstrap_smem[0], jnp.float32)
        for r in range(1, rollouts):
            start = jnp.where(start_lane == WIDTH * r, bootstrap_smem[r], start)
        start_ref[...] = start

    def piece_chain_start():
        discount, trace = column(discount_smem, shape), column(trace_smem, shape)
        alive = 1.0 - done_ref[...].astype(jnp.float32)
        gate_ref[...] = discount * alive
        chain_ref[0:rollouts, :] = discount * trace * alive
        trace_ref[...] = trace[:, :128]
        last_done = jnp.where(alive > 0.5, -1.0, lane.astype(jnp.float32))
        last_done = jnp.max(last_done, axis=1, keepdims=True)
        fixed_ref[...] = jnp.where(small_lane == LAST_DONE, last_done, 0.0)

    def piece_chain(at):
        step = 1 << at
        chain = chain_ref[rollouts * at : rollouts * (at + 1), :]
        later = pltpu.roll(chain, length - step, 1)
        chain = chain * jnp.where(lane < length - step, later, 1.0)
        if 2 * step < length:
            chain_ref[rollouts * (at + 1) : rollouts * (at + 2), :] = chain
            return
        coef_ref[...] = chain / column(trace_smem, shape)
        fixed_ref[...] = jnp.where(small_lane == SLOPE, chain[:, 0:1], fixed_ref[...])

    def piece_power():
        discount = column(discount_smem, shape)
        left = length - 1 - lane
        power, factor, bit = discount, discount * column(trace_smem, shape), 1
        while bit < length:
            power = jnp.where(left & bit != 0, power * factor, power)
            factor = factor * factor
            bit *= 2
        power_ref[...] = power

    steps = length.bit_length() - 1
    pieces = [[] for _ in range(rollouts)]
    pieces[0] = [piece_chain_start]
    for at in range(steps):
        pieces[1 + at * (rollouts - 2) // steps].append(partial(piece_chain, at))
    pieces[0].append(piece_own)
    pieces[rollouts - 2].append(piece_power)

    for r in range(rollouts):
        copies[r].wait()
        for piece in pieces[r]:
            piece()
        for half in range(2):
            folded = [
                partial_sums(r, slice(first, first + CHUNK))
                for first in range(128 * half, 128 * (half + 1), CHUNK)
            ]
            if r == rollouts - 1:
                finish(half, jnp.concatenate(folded, axis=0))


def local_kernel(
    hidden_width,
    recv_ref,
    rewards_ref,
    gate_ref,
    chain_ref,
    coef_ref,
    fixed_ref,
    trace_ref,
    ratio_ref,
    values_ref,
    out_ref,
):
    me = lax.axis_index("tensor")
    rollouts, length = rewards_ref.shape
    peers = recv_ref.shape[0] // HEAD_ROWS
    shape = (rollouts, length)
    total = recv_ref[0:32, :]
    for peer in range(1, peers):
        total = total + recv_ref[HEAD_ROWS * peer : HEAD_ROWS * peer + 32, :]
    squares = jnp.concatenate([total[0:8], total[8:16]], axis=1)
    products = jnp.concatenate([total[16:24], total[24:32]], axis=1)
    weight = jnp.concatenate(
        [
            recv_ref[pl.ds(32, peers, stride=HEAD_ROWS), :],
            recv_ref[pl.ds(33, peers, stride=HEAD_ROWS), :],
        ],
        axis=1,
    )
    values = products * lax.rsqrt(squares / hidden_width + EPS_NORM)
    lane = lax.broadcasted_iota(jnp.int32, shape, 1)
    inner_next = jnp.where(lane < length - 1, pltpu.roll(values, length - 1, 1), 0.0)
    local = rewards_ref[...] + gate_ref[...] * inner_next - values
    step, at = 1, 0
    while step < length:
        later = jnp.where(lane < length - step, pltpu.roll(local, length - step, 1), 0.0)
        local = local + chain_ref[rollouts * at : rollouts * (at + 1), :] * later
        step, at = 2 * step, at + 1
    coef = coef_ref[...]
    count = lane_sum(weight)
    safe = 1.0 / jnp.maximum(count, 1.0)
    mean_l = lane_sum(weight * local) * safe
    mean_c = lane_sum(weight * coef) * safe
    off_l = weight * (local - mean_l)
    off_c = weight * (coef - mean_c)
    stats = {
        OFFSET: values[:, 0:1] + trace_ref[:, 0:1] * local[:, 0:1],
        COUNT: count,
        MEAN_L: mean_l,
        MEAN_C: mean_c,
        VAR_L: lane_sum(off_l * off_l),
        COV: lane_sum(off_l * off_c),
        VAR_C: lane_sum(off_c * off_c),
    }
    small_lane = lax.broadcasted_iota(jnp.int32, (rollouts, 128), 1)
    summary = fixed_ref[...]
    for at, stat in stats.items():
        summary = jnp.where(small_lane == at, stat, summary)
    summary = pltpu.roll(summary, 0, 1, stride=WIDTH, stride_axis=0)
    summary = jnp.sum(summary, axis=0, keepdims=True)
    mine = lax.broadcasted_iota(jnp.int32, shape, 0) == me
    own_local = jnp.sum(jnp.where(mine, local, 0.0), axis=0, keepdims=True)
    values_ref[...] = jnp.sum(jnp.where(mine, values, 0.0), axis=0, keepdims=True)
    row = lax.broadcasted_iota(jnp.int32, (8, 128), 0)
    message = jnp.where(row == 0, summary, 0.0)
    message = jnp.where(row == 1, own_local[:, :128], message)
    message = jnp.where(row == 2, own_local[:, 128:], message)
    message = jnp.where(row == 3, ratio_ref[:, :128], message)
    message = jnp.where(row == 4, ratio_ref[:, 128:], message)
    for peer in range(out_ref.shape[0] // TOKEN_ROWS):
        out_ref[TOKEN_ROWS * peer : TOKEN_ROWS * (peer + 1), :] = message[0:TOKEN_ROWS, :]


def full_sum(x):
    return jnp.sum(jnp.sum(x, axis=0, keepdims=True), axis=1, keepdims=True)


def final_kernel(
    recv_ref,
    power_ref,
    start_ref,
    values_ref,
    values_hbm,
    white_hbm,
    loss_hbm,
    out_ref,
    white_ref,
    loss_ref,
    sent,
):
    tensor, seq = lax.axis_index("tensor"), lax.axis_index("seq")
    writes = [
        pltpu.make_async_copy(source, target, sent.at[i])
        for i, (source, target) in enumerate(
            ((values_ref, values_hbm), (white_ref, white_hbm), (loss_ref, loss_hbm))
        )
    ]
    writes[0].start()
    blocks = recv_ref.shape[0] // TOKEN_ROWS
    rollouts = out_ref.shape[0]
    shape = (blocks, 128)
    table = recv_ref[pl.ds(0, blocks, stride=TOKEN_ROWS), :]
    row = lax.broadcasted_iota(jnp.int32, shape, 0)
    lane = lax.broadcasted_iota(jnp.int32, shape, 1)

    def stat(at):
        return pltpu.roll(table, 128 - at, 1)

    last = row == blocks - 1
    offset = jnp.where(last, start_ref[...], pltpu.roll(table, blocks - 1, 0))
    slope = jnp.where(last, 0.0, pltpu.roll(stat(SLOPE), blocks - 1, 0))
    step = 1
    while step < blocks:
        inside = row < blocks - step
        offset_later = jnp.where(inside, pltpu.roll(offset, blocks - step, 0), 0.0)
        slope_later = jnp.where(inside, pltpu.roll(slope, blocks - step, 0), 0.0)
        offset = offset + slope * offset_later
        slope = slope * slope_later
        step *= 2
    entering = offset
    used = (lane % WIDTH == 0) & (lane < WIDTH * rollouts)
    members = jnp.where(used, stat(COUNT), 0.0)
    block_mean = jnp.where(used, stat(MEAN_L) + entering * stat(MEAN_C), 0.0)
    count = full_sum(members)
    mean = full_sum(members * block_mean) / count
    within = stat(VAR_L) + entering * (2.0 * stat(COV) + entering * stat(VAR_C))
    apart = block_mean - mean
    variance = full_sum(jnp.where(used, within, 0.0) + members * apart * apart) / count
    scale = lax.rsqrt(variance + EPS_WHITE)

    mine = lane == WIDTH * tensor
    own_entering = lane_sum(jnp.where(mine, entering, 0.0))
    own_done = lane_sum(jnp.where(mine, stat(LAST_DONE), 0.0))
    power = power_ref[pl.ds(tensor, 1), :]
    loss = jnp.zeros(shape, jnp.float32)
    mine_row = row == seq
    for half in range(2):
        lanes = slice(128 * half, 128 * (half + 1))
        position = (lane + 128 * half).astype(jnp.float32)
        coef = jnp.where(position > own_done, power[:, lanes], 0.0)
        local = recv_ref[pl.ds(1 + half, blocks, stride=TOKEN_ROWS), :]
        ratio = recv_ref[pl.ds(3 + half, blocks, stride=TOKEN_ROWS), :]
        white = (local + coef * own_entering - mean) * scale
        clipped = jnp.clip(ratio, 1.0 - CLIP, 1.0 + CLIP)
        token = jnp.where(ratio > 0.0, -jnp.minimum(ratio * white, clipped * white), 0.0)
        loss = loss + token
        white_ref[:, lanes] = jnp.sum(jnp.where(mine_row, white, 0.0), axis=0, keepdims=True)
        loss_ref[:, lanes] = jnp.sum(jnp.where(mine_row, token, 0.0), axis=0, keepdims=True)
    writes[1].start()
    writes[2].start()
    out_ref[...] = jnp.broadcast_to(full_sum(loss) / count, out_ref.shape)
    for write in writes:
        write.wait()


VMEM = pl.BlockSpec(memory_space=pltpu.VMEM)
ANY = pl.BlockSpec(memory_space=pl.ANY)


def on_chip(x):
    return pltpu.with_memory_space_constraint(x, pltpu.VMEM)


def on_chip_shape(shape):
    return pltpu.VMEM(shape, jnp.float32)


def exchange(x, axis):
    return lax.all_to_all(x, axis, 0, 0, tiled=True)


def run_head(
    peers,
    hidden,
    norm_gain,
    value_weight,
    done_flags,
    valid_mask,
    new_logprob,
    old_logprob,
    discount,
    trace_decay,
    bootstrap,
):
    rollouts, length, width = hidden.shape
    f32 = jnp.float32
    steps = length.bit_length() - 1
    return pl.pallas_call(
        head_kernel,
        out_shape=(
            on_chip_shape((peers * HEAD_ROWS, 128)),
            on_chip_shape((rollouts, length)),
            on_chip_shape((rollouts * steps, length)),
            on_chip_shape((rollouts, length)),
            on_chip_shape((rollouts, length)),
            on_chip_shape((rollouts, 128)),
            on_chip_shape((rollouts, 128)),
            on_chip_shape((1, length)),
            on_chip_shape((1, 128)),
        ),
        in_specs=[ANY] * 10,
        out_specs=(VMEM,) * 9,
        scratch_shapes=[
            pltpu.VMEM(hidden.shape, hidden.dtype),
            pltpu.VMEM((width // 128, 128), norm_gain.dtype),
            pltpu.VMEM((width // 128, 128), value_weight.dtype),
            pltpu.VMEM(done_flags.shape, done_flags.dtype),
            pltpu.VMEM(valid_mask.shape, valid_mask.dtype),
            pltpu.VMEM(new_logprob.shape, f32),
            pltpu.VMEM(old_logprob.shape, f32),
            pltpu.SMEM(discount.shape, f32),
            pltpu.SMEM(trace_decay.shape, f32),
            pltpu.SMEM(bootstrap.shape, f32),
            pltpu.VMEM((3, length, 128), f32),
            pltpu.SemaphoreType.DMA((rollouts + 9,)),
        ],
        name="head",
    )(
        norm_gain.reshape(-1, 128),
        value_weight.reshape(-1, 128),
        done_flags,
        valid_mask,
        new_logprob,
        old_logprob,
        discount,
        trace_decay,
        bootstrap,
        hidden,
    )


def shards(
    hidden,
    norm_gain,
    value_weight,
    rewards,
    done_flags,
    valid_mask,
    new_logprob,
    old_logprob,
    discount,
    trace_decay,
    bootstrap,
):
    rollouts, length, width = hidden.shape
    peers, blocks = lax.axis_size("tensor"), lax.axis_size("seq")
    sent, gate, chain, coef, power, fixed, trace, ratio, start = run_head(
        peers,
        hidden,
        norm_gain,
        value_weight,
        done_flags,
        valid_mask,
        new_logprob,
        old_logprob,
        discount,
        trace_decay,
        bootstrap,
    )
    got = exchange(sent.reshape(peers, 1, HEAD_ROWS * 128), "tensor")
    values, sent = pl.pallas_call(
        lambda *refs: local_kernel(width * peers, *refs),
        out_shape=(
            on_chip_shape((1, length)),
            on_chip_shape((blocks * TOKEN_ROWS, 128)),
        ),
        in_specs=[VMEM] * 8,
        out_specs=(VMEM, VMEM),
        name="local",
    )(
        *map(
            on_chip,
            (
                got.reshape(peers * HEAD_ROWS, 128),
                rewards,
                gate,
                chain,
                coef,
                fixed,
                trace,
                ratio,
            ),
        )
    )
    got = exchange(sent.reshape(blocks, 1, TOKEN_ROWS * 128), "seq")
    own_row = jax.ShapeDtypeStruct((1, length), jnp.float32)
    values, white, loss, sent = pl.pallas_call(
        final_kernel,
        out_shape=(own_row, own_row, own_row, on_chip_shape((peers, 128))),
        in_specs=[VMEM] * 4,
        out_specs=(ANY, ANY, ANY, VMEM),
        scratch_shapes=[
            pltpu.VMEM((1, length), jnp.float32),
            pltpu.VMEM((1, length), jnp.float32),
            pltpu.SemaphoreType.DMA((3,)),
        ],
        name="final",
    )(*map(on_chip, (got.reshape(blocks * TOKEN_ROWS, 128), power, start, values)))
    got = exchange(sent.reshape(peers, 1, 128), "tensor")
    return values, white, loss, jnp.sum(got[:, 0, 0])


def solution(mesh):
    in_specs = (
        P(None, "seq", "tensor"),
        P("tensor"),
        P("tensor"),
        P(None, "seq"),
        P(None, "seq"),
        P("tensor", "seq"),
        P("tensor", "seq"),
        P("tensor", "seq"),
        P(),
        P(),
        P(),
    )
    out_specs = (P("tensor", "seq"), P("tensor", "seq"), P("tensor", "seq"), P())
    return jax.shard_map(
        shards, mesh=mesh, in_specs=in_specs, out_specs=out_specs, check_vma=False
    )
```

```python
from functools import partial

import jax
import jax.numpy as jnp
from jax import lax
from jax.experimental import pallas as pl
from jax.experimental.pallas import tpu as pltpu
from jax.sharding import PartitionSpec as P

EPS_NORM = 1e-06
EPS_WHITE = 1e-08
CLIP = 0.2

HEAD_ROWS = 40
TOKEN_ROWS = 5
WIDTH = 16
OFFSET, SLOPE, COUNT, MEAN_L, MEAN_C, VAR_L, COV, VAR_C, LAST_DONE = range(9)

CHUNK = 64

CONTRACT_LANES = (((1,), (1,)), ((), ()))


def column(ref, shape):
    row = lax.broadcasted_iota(jnp.int32, shape, 0)
    out = jnp.full(shape, ref[0], jnp.float32)
    for r in range(1, shape[0]):
        out = jnp.where(row == r, ref[r], out)
    return out


def lane_sum(x):
    return jnp.sum(x, axis=1, keepdims=True)


def head_kernel(
    gain_hbm,
    weight_hbm,
    done_hbm,
    mask_hbm,
    new_hbm,
    old_hbm,
    discount_hbm,
    trace_hbm,
    bootstrap_hbm,
    hidden_ref,
    out_ref,
    gate_ref,
    chain_ref,
    coef_ref,
    power_ref,
    fixed_ref,
    trace_ref,
    ratio_ref,
    start_ref,
    held,
    gain_ref,
    weight_ref,
    done_ref,
    mask_ref,
    new_ref,
    old_ref,
    discount_smem,
    trace_smem,
    bootstrap_smem,
    fold_ref,
    arrived,
):
    rollouts, length, width = held.shape
    peers = out_ref.shape[0] // HEAD_ROWS
    small = [
        pltpu.make_async_copy(source, target, arrived.at[rollouts + i])
        for i, (source, target) in enumerate(
            (
                (gain_hbm, gain_ref),
                (weight_hbm, weight_ref),
                (done_hbm, done_ref),
                (mask_hbm, mask_ref),
                (new_hbm, new_ref),
                (old_hbm, old_ref),
                (discount_hbm, discount_smem),
                (trace_hbm, trace_smem),
                (bootstrap_hbm, bootstrap_smem),
            )
        )
    ]
    copies = [
        pltpu.make_async_copy(hidden_ref.at[r], held.at[r], arrived.at[r]) for r in range(rollouts)
    ]
    for copy in copies[:1] + small + copies[1:]:
        copy.start()
    for copy in small:
        copy.wait()

    scaled = gain_ref[...].astype(jnp.float32) * weight_ref[...].astype(jnp.float32)
    small_lane = lax.broadcasted_iota(jnp.int32, (8, 128), 1)
    levels = rollouts.bit_length() - 1
    group = 64 >> levels

    def fold(even, odd, distance):
        even = even + pltpu.roll(even, 128 - distance, 1)
        odd = odd + pltpu.roll(odd, distance, 1)
        return jnp.where((small_lane[0:1] // distance) % 2 == 0, even, odd)

    def partial_sums(r, here):
        squares = products = jnp.zeros((CHUNK, 128), jnp.float32)
        for j in range(width // 128):
            wide = held[r, here, 128 * j : 128 * (j + 1)].astype(jnp.float32)
            squares = squares + wide * wide
            products = products + wide * scaled[j : j + 1, :]
        folded, distance = fold(squares, products, 64), 32
        for level in range(levels):
            if not (r >> level) & 1:
                fold_ref[level, here] = folded
                return None
            folded, distance = fold(fold_ref[level, here], folded, distance), distance // 2
        return folded

    def finish(half, folded):
        turned = jnp.transpose(folded)
        sublane = lax.broadcasted_iota(jnp.int32, (8, 128), 0)
        for kind in range(2):
            rows = []
            for r in range(rollouts):
                at = kind
                for level in range(levels):
                    at = 2 * at + (r >> level) % 2
                rows.append(turned[group * at : group * (at + 1)])
            distance = group // 2
            while distance:
                even, odd = rows[:distance], rows[distance:]
                rows = []
                for e, o in zip(even, odd, strict=True):
                    e = e + pltpu.roll(e, 8 - distance, 0)
                    o = o + pltpu.roll(o, distance, 0)
                    rows.append(jnp.where((sublane // distance) % 2 == 0, e, o))
                distance //= 2
            for peer in range(peers):
                at = HEAD_ROWS * peer + 8 * (2 * kind + half)
                out_ref[at : at + 8, :] = rows[0]

    shape = (rollouts, length)
    lane = lax.broadcasted_iota(jnp.int32, shape, 1)

    def piece_own():
        mask = mask_ref[...].astype(jnp.float32)
        ratio_ref[...] = mask * jnp.exp(new_ref[...] - old_ref[...])
        row = lax.broadcasted_iota(jnp.int32, (8, 128), 0)
        rest = jnp.where(row == 0, mask[:, :128], jnp.where(row == 1, mask[:, 128:], 0.0))
        for peer in range(peers):
            out_ref[HEAD_ROWS * peer + 32 : HEAD_ROWS * (peer + 1), :] = rest
        start_lane = lax.broadcasted_iota(jnp.int32, (1, 128), 1)
        start = jnp.full((1, 128), bootstrap_smem[0], jnp.float32)
        for r in range(1, rollouts):
            start = jnp.where(start_lane == WIDTH * r, bootstrap_smem[r], start)
        start_ref[...] = start

    def piece_chain_start():
        discount, trace = column(discount_smem, shape), column(trace_smem, shape)
        alive = 1.0 - done_ref[...].astype(jnp.float32)
        gate_ref[...] = discount * alive
        chain_ref[0:rollouts, :] = discount * trace * alive
        trace_ref[...] = trace[:, :128]
        last_done = jnp.where(alive > 0.5, -1.0, lane.astype(jnp.float32))
        last_done = jnp.max(last_done, axis=1, keepdims=True)
        fixed_ref[...] = jnp.where(small_lane == LAST_DONE, last_done, 0.0)

    def piece_chain(at):
        step = 1 << at
        chain = chain_ref[rollouts * at : rollouts * (at + 1), :]
        later = pltpu.roll(chain, length - step, 1)
        chain = chain * jnp.where(lane < length - step, later, 1.0)
        if 2 * step < length:
            chain_ref[rollouts * (at + 1) : rollouts * (at + 2), :] = chain
            return
        coef_ref[...] = chain / column(trace_smem, shape)
        fixed_ref[...] = jnp.where(small_lane == SLOPE, chain[:, 0:1], fixed_ref[...])

    def piece_power():
        discount = column(discount_smem, shape)
        left = length - 1 - lane
        power, factor, bit = discount, discount * column(trace_smem, shape), 1
        while bit < length:
            power = jnp.where(left & bit != 0, power * factor, power)
            factor = factor * factor
            bit *= 2
        power_ref[...] = power

    steps = length.bit_length() - 1
    pieces = [[] for _ in range(rollouts)]
    pieces[0] = [piece_chain_start]
    for at in range(steps):
        pieces[1 + at * (rollouts - 2) // steps].append(partial(piece_chain, at))
    pieces[0].append(piece_own)
    pieces[rollouts - 2].append(piece_power)

    for r in range(rollouts):
        copies[r].wait()
        for piece in pieces[r]:
            piece()
        for half in range(2):
            folded = [
                partial_sums(r, slice(first, first + CHUNK))
                for first in range(128 * half, 128 * (half + 1), CHUNK)
            ]
            if r == rollouts - 1:
                finish(half, jnp.concatenate(folded, axis=0))


def local_kernel(
    hidden_width,
    recv_ref,
    rewards_ref,
    gate_ref,
    chain_ref,
    coef_ref,
    fixed_ref,
    trace_ref,
    ratio_ref,
    values_ref,
    out_ref,
):
    me = lax.axis_index("tensor")
    rollouts, length = rewards_ref.shape
    peers = recv_ref.shape[0] // HEAD_ROWS
    shape = (rollouts, length)
    total = recv_ref[0:32, :]
    for peer in range(1, peers):
        total = total + recv_ref[HEAD_ROWS * peer : HEAD_ROWS * peer + 32, :]
    squares = jnp.concatenate([total[0:8], total[8:16]], axis=1)
    products = jnp.concatenate([total[16:24], total[24:32]], axis=1)
    weight = jnp.concatenate(
        [
            recv_ref[pl.ds(32, peers, stride=HEAD_ROWS), :],
            recv_ref[pl.ds(33, peers, stride=HEAD_ROWS), :],
        ],
        axis=1,
    )
    values = products * lax.rsqrt(squares / hidden_width + EPS_NORM)
    lane = lax.broadcasted_iota(jnp.int32, shape, 1)
    inner_next = jnp.where(lane < length - 1, pltpu.roll(values, length - 1, 1), 0.0)
    local = rewards_ref[...] + gate_ref[...] * inner_next - values
    step, at = 1, 0
    while step < length:
        later = jnp.where(lane < length - step, pltpu.roll(local, length - step, 1), 0.0)
        local = local + chain_ref[rollouts * at : rollouts * (at + 1), :] * later
        step, at = 2 * step, at + 1
    coef = coef_ref[...]
    count = lane_sum(weight)
    safe = 1.0 / jnp.maximum(count, 1.0)
    mean_l = lane_sum(weight * local) * safe
    mean_c = lane_sum(weight * coef) * safe
    off_l = weight * (local - mean_l)
    off_c = weight * (coef - mean_c)
    stats = {
        OFFSET: values[:, 0:1] + trace_ref[:, 0:1] * local[:, 0:1],
        COUNT: count,
        MEAN_L: mean_l,
        MEAN_C: mean_c,
        VAR_L: lane_sum(off_l * off_l),
        COV: lane_sum(off_l * off_c),
        VAR_C: lane_sum(off_c * off_c),
    }
    small_lane = lax.broadcasted_iota(jnp.int32, (rollouts, 128), 1)
    summary = fixed_ref[...]
    for at, stat in stats.items():
        summary = jnp.where(small_lane == at, stat, summary)
    summary = pltpu.roll(summary, 0, 1, stride=WIDTH, stride_axis=0)
    summary = jnp.sum(summary, axis=0, keepdims=True)
    mine = lax.broadcasted_iota(jnp.int32, shape, 0) == me
    own_local = jnp.sum(jnp.where(mine, local, 0.0), axis=0, keepdims=True)
    values_ref[...] = jnp.sum(jnp.where(mine, values, 0.0), axis=0, keepdims=True)
    row = lax.broadcasted_iota(jnp.int32, (8, 128), 0)
    message = jnp.where(row == 0, summary, 0.0)
    message = jnp.where(row == 1, own_local[:, :128], message)
    message = jnp.where(row == 2, own_local[:, 128:], message)
    message = jnp.where(row == 3, ratio_ref[:, :128], message)
    message = jnp.where(row == 4, ratio_ref[:, 128:], message)
    for peer in range(out_ref.shape[0] // TOKEN_ROWS):
        out_ref[TOKEN_ROWS * peer : TOKEN_ROWS * (peer + 1), :] = message[0:TOKEN_ROWS, :]


def in_order(ref, at, first):
    blocks = ref.shape[0] // TOKEN_ROWS
    rows = ref[pl.ds(at, blocks, stride=TOKEN_ROWS), :]
    return jnp.concatenate([rows[blocks - first :], rows[: blocks - first]], axis=0)


def full_sum(x):
    return jnp.sum(jnp.sum(x, axis=0, keepdims=True), axis=1, keepdims=True)


def final_kernel(
    first,
    recv_ref,
    power_ref,
    start_ref,
    values_ref,
    values_hbm,
    white_hbm,
    loss_hbm,
    out_ref,
    white_ref,
    loss_ref,
    sent,
):
    tensor, seq = lax.axis_index("tensor"), lax.axis_index("seq")
    writes = [
        pltpu.make_async_copy(source, target, sent.at[i])
        for i, (source, target) in enumerate(
            ((values_ref, values_hbm), (white_ref, white_hbm), (loss_ref, loss_hbm))
        )
    ]
    writes[0].start()
    blocks = recv_ref.shape[0] // TOKEN_ROWS
    rollouts = out_ref.shape[0]
    shape = (blocks, 128)
    table = in_order(recv_ref, 0, first)
    row = lax.broadcasted_iota(jnp.int32, shape, 0)
    lane = lax.broadcasted_iota(jnp.int32, shape, 1)

    def stat(at):
        return pltpu.roll(table, 128 - at, 1)

    last = row == blocks - 1
    offset = jnp.where(last, start_ref[...], pltpu.roll(table, blocks - 1, 0))
    slope = jnp.where(last, 0.0, pltpu.roll(stat(SLOPE), blocks - 1, 0))
    step = 1
    while step < blocks:
        inside = row < blocks - step
        offset_later = jnp.where(inside, pltpu.roll(offset, blocks - step, 0), 0.0)
        slope_later = jnp.where(inside, pltpu.roll(slope, blocks - step, 0), 0.0)
        offset = offset + slope * offset_later
        slope = slope * slope_later
        step *= 2
    entering = offset
    used = (lane % WIDTH == 0) & (lane < WIDTH * rollouts)
    members = jnp.where(used, stat(COUNT), 0.0)
    block_mean = jnp.where(used, stat(MEAN_L) + entering * stat(MEAN_C), 0.0)
    count = full_sum(members)
    mean = full_sum(members * block_mean) / count
    within = stat(VAR_L) + entering * (2.0 * stat(COV) + entering * stat(VAR_C))
    apart = block_mean - mean
    variance = full_sum(jnp.where(used, within, 0.0) + members * apart * apart) / count
    scale = lax.rsqrt(variance + EPS_WHITE)

    mine = lane == WIDTH * tensor
    own_entering = lane_sum(jnp.where(mine, entering, 0.0))
    own_done = lane_sum(jnp.where(mine, stat(LAST_DONE), 0.0))
    power = power_ref[pl.ds(tensor, 1), :]
    loss = jnp.zeros(shape, jnp.float32)
    mine_row = row == seq
    for half in range(2):
        lanes = slice(128 * half, 128 * (half + 1))
        position = (lane + 128 * half).astype(jnp.float32)
        coef = jnp.where(position > own_done, power[:, lanes], 0.0)
        local = in_order(recv_ref, 1 + half, first)
        ratio = in_order(recv_ref, 3 + half, first)
        white = (local + coef * own_entering - mean) * scale
        clipped = jnp.clip(ratio, 1.0 - CLIP, 1.0 + CLIP)
        token = jnp.where(ratio > 0.0, -jnp.minimum(ratio * white, clipped * white), 0.0)
        loss = loss + token
        white_ref[:, lanes] = jnp.sum(jnp.where(mine_row, white, 0.0), axis=0, keepdims=True)
        loss_ref[:, lanes] = jnp.sum(jnp.where(mine_row, token, 0.0), axis=0, keepdims=True)
    writes[1].start()
    writes[2].start()
    out_ref[...] = jnp.broadcast_to(full_sum(loss) / count, out_ref.shape)
    for write in writes:
        write.wait()


VMEM = pl.BlockSpec(memory_space=pltpu.VMEM)
ANY = pl.BlockSpec(memory_space=pl.ANY)


def on_chip(x):
    return pltpu.with_memory_space_constraint(x, pltpu.VMEM)


def on_chip_shape(shape):
    return pltpu.VMEM(shape, jnp.float32)


def exchange(x, axis, first=0):
    size = lax.axis_size(axis)
    order = [(first + i) % size for i in range(size)]
    return lax.all_to_all(x, axis, 0, 0, axis_index_groups=[order], tiled=True)


def run_head(
    peers,
    hidden,
    norm_gain,
    value_weight,
    done_flags,
    valid_mask,
    new_logprob,
    old_logprob,
    discount,
    trace_decay,
    bootstrap,
):
    rollouts, length, width = hidden.shape
    f32 = jnp.float32
    steps = length.bit_length() - 1
    return pl.pallas_call(
        head_kernel,
        out_shape=(
            on_chip_shape((peers * HEAD_ROWS, 128)),
            on_chip_shape((rollouts, length)),
            on_chip_shape((rollouts * steps, length)),
            on_chip_shape((rollouts, length)),
            on_chip_shape((rollouts, length)),
            on_chip_shape((rollouts, 128)),
            on_chip_shape((rollouts, 128)),
            on_chip_shape((1, length)),
            on_chip_shape((1, 128)),
        ),
        in_specs=[ANY] * 10,
        out_specs=(VMEM,) * 9,
        scratch_shapes=[
            pltpu.VMEM(hidden.shape, hidden.dtype),
            pltpu.VMEM((width // 128, 128), norm_gain.dtype),
            pltpu.VMEM((width // 128, 128), value_weight.dtype),
            pltpu.VMEM(done_flags.shape, done_flags.dtype),
            pltpu.VMEM(valid_mask.shape, valid_mask.dtype),
            pltpu.VMEM(new_logprob.shape, f32),
            pltpu.VMEM(old_logprob.shape, f32),
            pltpu.SMEM(discount.shape, f32),
            pltpu.SMEM(trace_decay.shape, f32),
            pltpu.SMEM(bootstrap.shape, f32),
            pltpu.VMEM((3, length, 128), f32),
            pltpu.SemaphoreType.DMA((rollouts + 9,)),
        ],
        name="head",
    )(
        norm_gain.reshape(-1, 128),
        value_weight.reshape(-1, 128),
        done_flags,
        valid_mask,
        new_logprob,
        old_logprob,
        discount,
        trace_decay,
        bootstrap,
        hidden,
    )


def shards(
    hidden,
    norm_gain,
    value_weight,
    rewards,
    done_flags,
    valid_mask,
    new_logprob,
    old_logprob,
    discount,
    trace_decay,
    bootstrap,
):
    rollouts, length, width = hidden.shape
    peers, blocks = lax.axis_size("tensor"), lax.axis_size("seq")
    sent, gate, chain, coef, power, fixed, trace, ratio, start = run_head(
        peers,
        hidden,
        norm_gain,
        value_weight,
        done_flags,
        valid_mask,
        new_logprob,
        old_logprob,
        discount,
        trace_decay,
        bootstrap,
    )
    got = exchange(sent.reshape(peers, 1, HEAD_ROWS * 128), "tensor")
    values, sent = pl.pallas_call(
        lambda *refs: local_kernel(width * peers, *refs),
        out_shape=(
            on_chip_shape((1, length)),
            on_chip_shape((blocks * TOKEN_ROWS, 128)),
        ),
        in_specs=[VMEM] * 8,
        out_specs=(VMEM, VMEM),
        name="local",
    )(
        *map(
            on_chip,
            (
                got.reshape(peers * HEAD_ROWS, 128),
                rewards,
                gate,
                chain,
                coef,
                fixed,
                trace,
                ratio,
            ),
        )
    )
    first = blocks * 7 // 8
    got = exchange(sent.reshape(blocks, 1, TOKEN_ROWS * 128), "seq", first)
    own_row = jax.ShapeDtypeStruct((1, length), jnp.float32)
    values, white, loss, sent = pl.pallas_call(
        partial(final_kernel, first),
        out_shape=(own_row, own_row, own_row, on_chip_shape((peers, 128))),
        in_specs=[VMEM] * 4,
        out_specs=(ANY, ANY, ANY, VMEM),
        scratch_shapes=[
            pltpu.VMEM((1, length), jnp.float32),
            pltpu.VMEM((1, length), jnp.float32),
            pltpu.SemaphoreType.DMA((3,)),
        ],
        name="final",
    )(*map(on_chip, (got.reshape(blocks * TOKEN_ROWS, 128), power, start, values)))
    got = exchange(sent.reshape(peers, 1, 128), "tensor")
    return values, white, loss, jnp.sum(got[:, 0, 0])


def solution(mesh):
    in_specs = (
        P(None, "seq", "tensor"),
        P("tensor"),
        P("tensor"),
        P(None, "seq"),
        P(None, "seq"),
        P("tensor", "seq"),
        P("tensor", "seq"),
        P("tensor", "seq"),
        P(),
        P(),
        P(),
    )
    out_specs = (P("tensor", "seq"), P("tensor", "seq"), P("tensor", "seq"), P())
    return jax.shard_map(
        shards, mesh=mesh, in_specs=in_specs, out_specs=out_specs, check_vma=False
    )
```

```python
from functools import partial

import jax
import jax.numpy as jnp
from jax import lax
from jax.experimental import pallas as pl
from jax.experimental.pallas import tpu as pltpu
from jax.sharding import PartitionSpec as P

EPS_NORM = 1e-06
EPS_WHITE = 1e-08
CLIP = 0.2

HEAD_ROWS = 40
TOKEN_ROWS = 5
WIDTH = 16
OFFSET, SLOPE, COUNT, MEAN_L, MEAN_C, VAR_L, COV, VAR_C, LAST_DONE = range(9)

CHUNK = 64

TENSOR_FIRST, SEQ_FIRST, LAST_FIRST = 5, 40, 5


def column(ref, shape):
    row = lax.broadcasted_iota(jnp.int32, shape, 0)
    out = jnp.full(shape, ref[0], jnp.float32)
    for r in range(1, shape[0]):
        out = jnp.where(row == r, ref[r], out)
    return out


def lane_sum(x):
    return jnp.sum(x, axis=1, keepdims=True)


def head_kernel(
    gain_hbm,
    weight_hbm,
    done_hbm,
    mask_hbm,
    new_hbm,
    old_hbm,
    discount_hbm,
    trace_hbm,
    bootstrap_hbm,
    hidden_ref,
    out_ref,
    gate_ref,
    chain_ref,
    coef_ref,
    power_ref,
    fixed_ref,
    trace_ref,
    ratio_ref,
    start_ref,
    held,
    gain_ref,
    weight_ref,
    done_ref,
    mask_ref,
    new_ref,
    old_ref,
    discount_smem,
    trace_smem,
    bootstrap_smem,
    fold_ref,
    arrived,
):
    rollouts, length, width = held.shape
    peers = out_ref.shape[0] // HEAD_ROWS
    small = [
        pltpu.make_async_copy(source, target, arrived.at[rollouts + i])
        for i, (source, target) in enumerate(
            (
                (gain_hbm, gain_ref),
                (weight_hbm, weight_ref),
                (done_hbm, done_ref),
                (mask_hbm, mask_ref),
                (new_hbm, new_ref),
                (old_hbm, old_ref),
                (discount_hbm, discount_smem),
                (trace_hbm, trace_smem),
                (bootstrap_hbm, bootstrap_smem),
            )
        )
    ]
    copies = [
        pltpu.make_async_copy(hidden_ref.at[r], held.at[r], arrived.at[r]) for r in range(rollouts)
    ]
    for copy in copies[:1] + small + copies[1:]:
        copy.start()
    for copy in small:
        copy.wait()

    scaled = gain_ref[...].astype(jnp.float32) * weight_ref[...].astype(jnp.float32)
    small_lane = lax.broadcasted_iota(jnp.int32, (8, 128), 1)
    levels = rollouts.bit_length() - 1
    group = 64 >> levels

    def fold(even, odd, distance):
        even = even + pltpu.roll(even, 128 - distance, 1)
        odd = odd + pltpu.roll(odd, distance, 1)
        return jnp.where((small_lane[0:1] // distance) % 2 == 0, even, odd)

    def partial_sums(r, here):
        squares = products = jnp.zeros((CHUNK, 128), jnp.float32)
        for j in range(width // 128):
            wide = held[r, here, 128 * j : 128 * (j + 1)].astype(jnp.float32)
            squares = squares + wide * wide
            products = products + wide * scaled[j : j + 1, :]
        folded, distance = fold(squares, products, 64), 32
        for level in range(levels):
            if not (r >> level) & 1:
                fold_ref[level, here] = folded
                return None
            folded, distance = fold(fold_ref[level, here], folded, distance), distance // 2
        return folded

    def finish(half, folded):
        turned = jnp.transpose(folded)
        sublane = lax.broadcasted_iota(jnp.int32, (8, 128), 0)
        for kind in range(2):
            rows = []
            for r in range(rollouts):
                at = kind
                for level in range(levels):
                    at = 2 * at + (r >> level) % 2
                rows.append(turned[group * at : group * (at + 1)])
            distance = group // 2
            while distance:
                even, odd = rows[:distance], rows[distance:]
                rows = []
                for e, o in zip(even, odd, strict=True):
                    e = e + pltpu.roll(e, 8 - distance, 0)
                    o = o + pltpu.roll(o, distance, 0)
                    rows.append(jnp.where((sublane // distance) % 2 == 0, e, o))
                distance //= 2
            for peer in range(peers):
                at = HEAD_ROWS * peer + 8 * (2 * kind + half)
                out_ref[at : at + 8, :] = rows[0]

    shape = (rollouts, length)
    lane = lax.broadcasted_iota(jnp.int32, shape, 1)

    def piece_own():
        mask = mask_ref[...].astype(jnp.float32)
        ratio_ref[...] = mask * jnp.exp(new_ref[...] - old_ref[...])
        row = lax.broadcasted_iota(jnp.int32, (8, 128), 0)
        rest = jnp.where(row == 0, mask[:, :128], jnp.where(row == 1, mask[:, 128:], 0.0))
        for peer in range(peers):
            out_ref[HEAD_ROWS * peer + 32 : HEAD_ROWS * (peer + 1), :] = rest
        start_lane = lax.broadcasted_iota(jnp.int32, (1, 128), 1)
        start = jnp.full((1, 128), bootstrap_smem[0], jnp.float32)
        for r in range(1, rollouts):
            start = jnp.where(start_lane == WIDTH * r, bootstrap_smem[r], start)
        start_ref[...] = start

    def piece_chain_start():
        discount, trace = column(discount_smem, shape), column(trace_smem, shape)
        alive = 1.0 - done_ref[...].astype(jnp.float32)
        gate_ref[...] = discount * alive
        chain_ref[0:rollouts, :] = discount * trace * alive
        trace_ref[...] = trace[:, :128]
        last_done = jnp.where(alive > 0.5, -1.0, lane.astype(jnp.float32))
        last_done = jnp.max(last_done, axis=1, keepdims=True)
        fixed_ref[...] = jnp.where(small_lane == LAST_DONE, last_done, 0.0)

    def piece_chain(at):
        step = 1 << at
        chain = chain_ref[rollouts * at : rollouts * (at + 1), :]
        later = pltpu.roll(chain, length - step, 1)
        chain = chain * jnp.where(lane < length - step, later, 1.0)
        if 2 * step < length:
            chain_ref[rollouts * (at + 1) : rollouts * (at + 2), :] = chain
            return
        coef_ref[...] = chain / column(trace_smem, shape)
        fixed_ref[...] = jnp.where(small_lane == SLOPE, chain[:, 0:1], fixed_ref[...])

    def piece_power():
        discount = column(discount_smem, shape)
        left = length - 1 - lane
        power, factor, bit = discount, discount * column(trace_smem, shape), 1
        while bit < length:
            power = jnp.where(left & bit != 0, power * factor, power)
            factor = factor * factor
            bit *= 2
        power_ref[...] = power

    steps = length.bit_length() - 1
    pieces = [[] for _ in range(rollouts)]
    pieces[0] = [piece_chain_start]
    for at in range(steps):
        pieces[1 + at * (rollouts - 2) // steps].append(partial(piece_chain, at))
    pieces[0].append(piece_own)
    pieces[rollouts - 2].append(piece_power)

    for r in range(rollouts):
        copies[r].wait()
        for piece in pieces[r]:
            piece()
        for half in range(2):
            folded = [
                partial_sums(r, slice(first, first + CHUNK))
                for first in range(128 * half, 128 * (half + 1), CHUNK)
            ]
            if r == rollouts - 1:
                finish(half, jnp.concatenate(folded, axis=0))


def local_kernel(
    hidden_width,
    first,
    recv_ref,
    rewards_ref,
    gate_ref,
    chain_ref,
    coef_ref,
    fixed_ref,
    trace_ref,
    ratio_ref,
    values_ref,
    out_ref,
):
    me = lax.axis_index("tensor")
    rollouts, length = rewards_ref.shape
    peers = recv_ref.shape[0] // HEAD_ROWS
    shape = (rollouts, length)
    total = recv_ref[0:32, :]
    for peer in range(1, peers):
        total = total + recv_ref[HEAD_ROWS * peer : HEAD_ROWS * peer + 32, :]
    squares = jnp.concatenate([total[0:8], total[8:16]], axis=1)
    products = jnp.concatenate([total[16:24], total[24:32]], axis=1)
    weight = jnp.concatenate(
        [
            recv_ref[pl.ds(32, peers, stride=HEAD_ROWS), :],
            recv_ref[pl.ds(33, peers, stride=HEAD_ROWS), :],
        ],
        axis=1,
    )
    weight = in_order(weight, first)
    values = products * lax.rsqrt(squares / hidden_width + EPS_NORM)
    lane = lax.broadcasted_iota(jnp.int32, shape, 1)
    inner_next = jnp.where(lane < length - 1, pltpu.roll(values, length - 1, 1), 0.0)
    local = rewards_ref[...] + gate_ref[...] * inner_next - values
    step, at = 1, 0
    while step < length:
        later = jnp.where(lane < length - step, pltpu.roll(local, length - step, 1), 0.0)
        local = local + chain_ref[rollouts * at : rollouts * (at + 1), :] * later
        step, at = 2 * step, at + 1
    coef = coef_ref[...]
    count = lane_sum(weight)
    safe = 1.0 / jnp.maximum(count, 1.0)
    mean_l = lane_sum(weight * local) * safe
    mean_c = lane_sum(weight * coef) * safe
    off_l = weight * (local - mean_l)
    off_c = weight * (coef - mean_c)
    stats = {
        OFFSET: values[:, 0:1] + trace_ref[:, 0:1] * local[:, 0:1],
        COUNT: count,
        MEAN_L: mean_l,
        MEAN_C: mean_c,
        VAR_L: lane_sum(off_l * off_l),
        COV: lane_sum(off_l * off_c),
        VAR_C: lane_sum(off_c * off_c),
    }
    small_lane = lax.broadcasted_iota(jnp.int32, (rollouts, 128), 1)
    summary = fixed_ref[...]
    for at, stat in stats.items():
        summary = jnp.where(small_lane == at, stat, summary)
    summary = pltpu.roll(summary, 0, 1, stride=WIDTH, stride_axis=0)
    summary = jnp.sum(summary, axis=0, keepdims=True)
    mine = lax.broadcasted_iota(jnp.int32, shape, 0) == me
    own_local = jnp.sum(jnp.where(mine, local, 0.0), axis=0, keepdims=True)
    values_ref[...] = jnp.sum(jnp.where(mine, values, 0.0), axis=0, keepdims=True)
    row = lax.broadcasted_iota(jnp.int32, (8, 128), 0)
    message = jnp.where(row == 0, summary, 0.0)
    message = jnp.where(row == 1, own_local[:, :128], message)
    message = jnp.where(row == 2, own_local[:, 128:], message)
    message = jnp.where(row == 3, ratio_ref[:, :128], message)
    message = jnp.where(row == 4, ratio_ref[:, 128:], message)
    for peer in range(out_ref.shape[0] // TOKEN_ROWS):
        out_ref[TOKEN_ROWS * peer : TOKEN_ROWS * (peer + 1), :] = message[0:TOKEN_ROWS, :]


def in_order(rows, first):
    row = lax.broadcasted_iota(jnp.int32, rows.shape, 0)
    swapped = jnp.where(row == 0, rows[first : first + 1], rows)
    return jnp.where(row == first, rows[0:1], swapped)


def full_sum(x):
    return jnp.sum(jnp.sum(x, axis=0, keepdims=True), axis=1, keepdims=True)


def final_kernel(
    first,
    recv_ref,
    power_ref,
    start_ref,
    values_ref,
    values_hbm,
    white_hbm,
    loss_hbm,
    out_ref,
    white_ref,
    loss_ref,
    sent,
):
    tensor, seq = lax.axis_index("tensor"), lax.axis_index("seq")
    writes = [
        pltpu.make_async_copy(source, target, sent.at[i])
        for i, (source, target) in enumerate(
            ((values_ref, values_hbm), (white_ref, white_hbm), (loss_ref, loss_hbm))
        )
    ]
    writes[0].start()
    blocks = recv_ref.shape[0] // TOKEN_ROWS
    rollouts = out_ref.shape[0]
    shape = (blocks, 128)
    table = in_order(recv_ref[pl.ds(0, blocks, stride=TOKEN_ROWS), :], first)
    row = lax.broadcasted_iota(jnp.int32, shape, 0)
    lane = lax.broadcasted_iota(jnp.int32, shape, 1)

    def stat(at):
        return pltpu.roll(table, 128 - at, 1)

    last = row == blocks - 1
    offset = jnp.where(last, start_ref[...], pltpu.roll(table, blocks - 1, 0))
    slope = jnp.where(last, 0.0, pltpu.roll(stat(SLOPE), blocks - 1, 0))
    step = 1
    while step < blocks:
        inside = row < blocks - step
        offset_later = jnp.where(inside, pltpu.roll(offset, blocks - step, 0), 0.0)
        slope_later = jnp.where(inside, pltpu.roll(slope, blocks - step, 0), 0.0)
        offset = offset + slope * offset_later
        slope = slope * slope_later
        step *= 2
    entering = offset
    used = (lane % WIDTH == 0) & (lane < WIDTH * rollouts)
    members = jnp.where(used, stat(COUNT), 0.0)
    block_mean = jnp.where(used, stat(MEAN_L) + entering * stat(MEAN_C), 0.0)
    count = full_sum(members)
    mean = full_sum(members * block_mean) / count
    within = stat(VAR_L) + entering * (2.0 * stat(COV) + entering * stat(VAR_C))
    apart = block_mean - mean
    variance = full_sum(jnp.where(used, within, 0.0) + members * apart * apart) / count
    scale = lax.rsqrt(variance + EPS_WHITE)

    mine = lane == WIDTH * tensor
    own_entering = lane_sum(jnp.where(mine, entering, 0.0))
    own_done = lane_sum(jnp.where(mine, stat(LAST_DONE), 0.0))
    power = power_ref[pl.ds(tensor, 1), :]
    loss = jnp.zeros(shape, jnp.float32)
    mine_row = row == seq
    for half in range(2):
        lanes = slice(128 * half, 128 * (half + 1))
        position = (lane + 128 * half).astype(jnp.float32)
        coef = jnp.where(position > own_done, power[:, lanes], 0.0)
        local = in_order(recv_ref[pl.ds(1 + half, blocks, stride=TOKEN_ROWS), :], first)
        ratio = in_order(recv_ref[pl.ds(3 + half, blocks, stride=TOKEN_ROWS), :], first)
        white = (local + coef * own_entering - mean) * scale
        clipped = jnp.clip(ratio, 1.0 - CLIP, 1.0 + CLIP)
        token = jnp.where(ratio > 0.0, -jnp.minimum(ratio * white, clipped * white), 0.0)
        loss = loss + token
        white_ref[:, lanes] = jnp.sum(jnp.where(mine_row, white, 0.0), axis=0, keepdims=True)
        loss_ref[:, lanes] = jnp.sum(jnp.where(mine_row, token, 0.0), axis=0, keepdims=True)
    writes[1].start()
    writes[2].start()
    out_ref[...] = jnp.broadcast_to(full_sum(loss) / count, out_ref.shape)
    for write in writes:
        write.wait()


VMEM = pl.BlockSpec(memory_space=pltpu.VMEM)
ANY = pl.BlockSpec(memory_space=pl.ANY)


def on_chip(x):
    return pltpu.with_memory_space_constraint(x, pltpu.VMEM)


def on_chip_shape(shape):
    return pltpu.VMEM(shape, jnp.float32)


def exchange(x, axis, first):
    order = list(range(lax.axis_size(axis)))
    order[0], order[first] = order[first], order[0]
    return lax.all_to_all(x, axis, 0, 0, axis_index_groups=[order], tiled=True)


def run_head(
    peers,
    hidden,
    norm_gain,
    value_weight,
    done_flags,
    valid_mask,
    new_logprob,
    old_logprob,
    discount,
    trace_decay,
    bootstrap,
):
    rollouts, length, width = hidden.shape
    f32 = jnp.float32
    steps = length.bit_length() - 1
    return pl.pallas_call(
        head_kernel,
        out_shape=(
            on_chip_shape((peers * HEAD_ROWS, 128)),
            on_chip_shape((rollouts, length)),
            on_chip_shape((rollouts * steps, length)),
            on_chip_shape((rollouts, length)),
            on_chip_shape((rollouts, length)),
            on_chip_shape((rollouts, 128)),
            on_chip_shape((rollouts, 128)),
            on_chip_shape((1, length)),
            on_chip_shape((1, 128)),
        ),
        in_specs=[ANY] * 10,
        out_specs=(VMEM,) * 9,
        scratch_shapes=[
            pltpu.VMEM(hidden.shape, hidden.dtype),
            pltpu.VMEM((width // 128, 128), norm_gain.dtype),
            pltpu.VMEM((width // 128, 128), value_weight.dtype),
            pltpu.VMEM(done_flags.shape, done_flags.dtype),
            pltpu.VMEM(valid_mask.shape, valid_mask.dtype),
            pltpu.VMEM(new_logprob.shape, f32),
            pltpu.VMEM(old_logprob.shape, f32),
            pltpu.SMEM(discount.shape, f32),
            pltpu.SMEM(trace_decay.shape, f32),
            pltpu.SMEM(bootstrap.shape, f32),
            pltpu.VMEM((3, length, 128), f32),
            pltpu.SemaphoreType.DMA((rollouts + 9,)),
        ],
        name="head",
    )(
        norm_gain.reshape(-1, 128),
        value_weight.reshape(-1, 128),
        done_flags,
        valid_mask,
        new_logprob,
        old_logprob,
        discount,
        trace_decay,
        bootstrap,
        hidden,
    )


def shards(
    hidden,
    norm_gain,
    value_weight,
    rewards,
    done_flags,
    valid_mask,
    new_logprob,
    old_logprob,
    discount,
    trace_decay,
    bootstrap,
):
    rollouts, length, width = hidden.shape
    peers, blocks = lax.axis_size("tensor"), lax.axis_size("seq")
    sent, gate, chain, coef, power, fixed, trace, ratio, start = run_head(
        peers,
        hidden,
        norm_gain,
        value_weight,
        done_flags,
        valid_mask,
        new_logprob,
        old_logprob,
        discount,
        trace_decay,
        bootstrap,
    )
    got = exchange(sent.reshape(peers, 1, HEAD_ROWS * 128), "tensor", TENSOR_FIRST)
    values, sent = pl.pallas_call(
        partial(local_kernel, width * peers, TENSOR_FIRST),
        out_shape=(
            on_chip_shape((1, length)),
            on_chip_shape((blocks * TOKEN_ROWS, 128)),
        ),
        in_specs=[VMEM] * 8,
        out_specs=(VMEM, VMEM),
        name="local",
    )(
        *map(
            on_chip,
            (
                got.reshape(peers * HEAD_ROWS, 128),
                rewards,
                gate,
                chain,
                coef,
                fixed,
                trace,
                ratio,
            ),
        )
    )
    got = exchange(sent.reshape(blocks, 1, TOKEN_ROWS * 128), "seq", SEQ_FIRST)
    own_row = jax.ShapeDtypeStruct((1, length), jnp.float32)
    values, white, loss, sent = pl.pallas_call(
        partial(final_kernel, SEQ_FIRST),
        out_shape=(own_row, own_row, own_row, on_chip_shape((peers, 128))),
        in_specs=[VMEM] * 4,
        out_specs=(ANY, ANY, ANY, VMEM),
        scratch_shapes=[
            pltpu.VMEM((1, length), jnp.float32),
            pltpu.VMEM((1, length), jnp.float32),
            pltpu.SemaphoreType.DMA((3,)),
        ],
        name="final",
    )(*map(on_chip, (got.reshape(blocks * TOKEN_ROWS, 128), power, start, values)))
    got = exchange(sent.reshape(peers, 1, 128), "tensor", LAST_FIRST)
    return values, white, loss, jnp.sum(got[:, 0, 0])


def solution(mesh):
    in_specs = (
        P(None, "seq", "tensor"),
        P("tensor"),
        P("tensor"),
        P(None, "seq"),
        P(None, "seq"),
        P("tensor", "seq"),
        P("tensor", "seq"),
        P("tensor", "seq"),
        P(),
        P(),
        P(),
    )
    out_specs = (P("tensor", "seq"), P("tensor", "seq"), P("tensor", "seq"), P())
    return jax.shard_map(
        shards, mesh=mesh, in_specs=in_specs, out_specs=out_specs, check_vma=False
    )
```

```python
from functools import partial

import jax
import jax.numpy as jnp
from jax import lax
from jax.experimental import pallas as pl
from jax.experimental.pallas import tpu as pltpu
from jax.sharding import PartitionSpec as P

EPS_NORM = 1e-06
EPS_WHITE = 1e-08
CLIP = 0.2

HEAD_ROWS = 40
TOKEN_ROWS = 5
WIDTH = 16
OFFSET, SLOPE, COUNT, MEAN_L, MEAN_C, VAR_L, COV, VAR_C, LAST_DONE = range(9)

CHUNK = 64

TENSOR_ORDER = [5, 1, 2, 3, 4, 0, 6, 7]
SEQ_RUNS = [5, 7, 3, 1, 0, 2, 4, 6]


def column(ref, shape):
    row = lax.broadcasted_iota(jnp.int32, shape, 0)
    out = jnp.full(shape, ref[0], jnp.float32)
    for r in range(1, shape[0]):
        out = jnp.where(row == r, ref[r], out)
    return out


def lane_sum(x):
    return jnp.sum(x, axis=1, keepdims=True)


def head_kernel(
    gain_hbm,
    weight_hbm,
    done_hbm,
    mask_hbm,
    new_hbm,
    old_hbm,
    discount_hbm,
    trace_hbm,
    bootstrap_hbm,
    hidden_ref,
    out_ref,
    gate_ref,
    chain_ref,
    coef_ref,
    power_ref,
    fixed_ref,
    trace_ref,
    ratio_ref,
    start_ref,
    held,
    gain_ref,
    weight_ref,
    done_ref,
    mask_ref,
    new_ref,
    old_ref,
    discount_smem,
    trace_smem,
    bootstrap_smem,
    split_ref,
    pick_ref,
    sums_ref,
    arrived,
):
    rollouts, length, width = held.shape
    peers = out_ref.shape[0] // HEAD_ROWS
    small = [
        pltpu.make_async_copy(source, target, arrived.at[rollouts + i])
        for i, (source, target) in enumerate(
            (
                (gain_hbm, gain_ref),
                (weight_hbm, weight_ref),
                (done_hbm, done_ref),
                (mask_hbm, mask_ref),
                (new_hbm, new_ref),
                (old_hbm, old_ref),
                (discount_hbm, discount_smem),
                (trace_hbm, trace_smem),
                (bootstrap_hbm, bootstrap_smem),
            )
        )
    ]
    copies = [
        pltpu.make_async_copy(hidden_ref.at[r], held.at[r], arrived.at[r]) for r in range(rollouts)
    ]
    for copy in copies[:1] + small + copies[1:]:
        copy.start()
    picked = lax.broadcasted_iota(jnp.int32, (3 * 128, 128), 0) % 128 // 64 * 8
    picked = lax.broadcasted_iota(jnp.int32, (3 * 128, 128), 1) - picked
    for r in range(rollouts):
        pick_ref[r] = jnp.where(picked == r, 1.0, 0.0).astype(jnp.bfloat16)
    for copy in small:
        copy.wait()

    scaled = gain_ref[...].astype(jnp.float32) * weight_ref[...].astype(jnp.float32)
    small_lane = lax.broadcasted_iota(jnp.int32, (8, 128), 1)

    def partial_sums(r, here):
        squares = products = jnp.zeros((CHUNK, 128), jnp.float32)
        for j in range(width // 128):
            wide = held[r, here, 128 * j : 128 * (j + 1)].astype(jnp.float32)
            squares = squares + wide * wide
            products = products + wide * scaled[j : j + 1, :]
        left = small_lane[0:1] < 64
        rest = jnp.where(left, squares, products)
        rest = rest + pltpu.roll(jnp.where(left, products, squares), 64, 1)
        for part in range(3):
            coarse = rest.astype(jnp.bfloat16)
            split_ref[r % 2, here, 128 * part : 128 * (part + 1)] = coarse
            rest = rest - coarse.astype(jnp.float32)

    def lane_sums(r):
        sums = jnp.dot(split_ref[r % 2], pick_ref[r], preferred_element_type=jnp.float32)
        sums_ref[...] = sums_ref[...] + sums if r else sums

    def finish():
        for half in range(length // 128):
            turned = jnp.transpose(sums_ref[128 * half : 128 * (half + 1), :])
            for peer in range(peers):
                for kind in range(2):
                    at = HEAD_ROWS * peer + 8 * (2 * kind + half)
                    out_ref[at : at + 8, :] = turned[8 * kind : 8 * (kind + 1)]

    shape = (rollouts, length)
    lane = lax.broadcasted_iota(jnp.int32, shape, 1)

    def piece_own():
        mask = mask_ref[...].astype(jnp.float32)
        ratio_ref[...] = mask * jnp.exp(new_ref[...] - old_ref[...])
        row = lax.broadcasted_iota(jnp.int32, (8, 128), 0)
        rest = jnp.where(row == 0, mask[:, :128], jnp.where(row == 1, mask[:, 128:], 0.0))
        for peer in range(peers):
            out_ref[HEAD_ROWS * peer + 32 : HEAD_ROWS * (peer + 1), :] = rest
        start_lane = lax.broadcasted_iota(jnp.int32, (1, 128), 1)
        start = jnp.full((1, 128), bootstrap_smem[0], jnp.float32)
        for r in range(1, rollouts):
            start = jnp.where(start_lane == WIDTH * r, bootstrap_smem[r], start)
        start_ref[...] = start

    def piece_chain_start():
        discount, trace = column(discount_smem, shape), column(trace_smem, shape)
        alive = 1.0 - done_ref[...].astype(jnp.float32)
        gate_ref[...] = discount * alive
        chain_ref[0:rollouts, :] = discount * trace * alive
        trace_ref[...] = trace[:, :128]
        last_done = jnp.where(alive > 0.5, -1.0, lane.astype(jnp.float32))
        last_done = jnp.max(last_done, axis=1, keepdims=True)
        fixed_ref[...] = jnp.where(small_lane == LAST_DONE, last_done, 0.0)

    def piece_chain(at):
        step = 1 << at
        chain = chain_ref[rollouts * at : rollouts * (at + 1), :]
        later = pltpu.roll(chain, length - step, 1)
        chain = chain * jnp.where(lane < length - step, later, 1.0)
        if 2 * step < length:
            chain_ref[rollouts * (at + 1) : rollouts * (at + 2), :] = chain
            return
        coef_ref[...] = chain / column(trace_smem, shape)
        fixed_ref[...] = jnp.where(small_lane == SLOPE, chain[:, 0:1], fixed_ref[...])

    def piece_power():
        discount = column(discount_smem, shape)
        left = length - 1 - lane
        power, factor, bit = discount, discount * column(trace_smem, shape), 1
        while bit < length:
            power = jnp.where(left & bit != 0, power * factor, power)
            factor = factor * factor
            bit *= 2
        power_ref[...] = power

    steps = length.bit_length() - 1
    pieces = [[] for _ in range(rollouts)]
    pieces[0] = [piece_chain_start]
    for at in range(steps):
        pieces[1 + at * (rollouts - 2) // steps].append(partial(piece_chain, at))
    pieces[0].append(piece_own)
    pieces[rollouts - 2].append(piece_power)

    for r in range(rollouts):
        copies[r].wait()
        for piece in pieces[r]:
            piece()
        if r:
            lane_sums(r - 1)
        for first in range(0, length, CHUNK):
            partial_sums(r, slice(first, first + CHUNK))
    lane_sums(rollouts - 1)
    finish()


def local_kernel(
    hidden_width,
    recv_ref,
    rewards_ref,
    gate_ref,
    chain_ref,
    coef_ref,
    fixed_ref,
    trace_ref,
    ratio_ref,
    values_ref,
    out_ref,
):
    me = lax.axis_index("tensor")
    rollouts, length = rewards_ref.shape
    peers = recv_ref.shape[0] // HEAD_ROWS
    shape = (rollouts, length)
    total = recv_ref[0:32, :]
    for peer in range(1, peers):
        total = total + recv_ref[HEAD_ROWS * peer : HEAD_ROWS * peer + 32, :]
    squares = jnp.concatenate([total[0:8], total[8:16]], axis=1)
    products = jnp.concatenate([total[16:24], total[24:32]], axis=1)
    weight = jnp.concatenate(
        [
            recv_ref[pl.ds(32, peers, stride=HEAD_ROWS), :],
            recv_ref[pl.ds(33, peers, stride=HEAD_ROWS), :],
        ],
        axis=1,
    )
    slot = lax.broadcasted_iota(jnp.int32, shape, 0)
    received = weight
    for peer, member in enumerate(TENSOR_ORDER):
        if peer != member:
            weight = jnp.where(slot == member, received[peer : peer + 1], weight)
    values = products * lax.rsqrt(squares / hidden_width + EPS_NORM)
    lane = lax.broadcasted_iota(jnp.int32, shape, 1)
    inner_next = jnp.where(lane < length - 1, pltpu.roll(values, length - 1, 1), 0.0)
    local = rewards_ref[...] + gate_ref[...] * inner_next - values
    step, at = 1, 0
    while step < length:
        later = jnp.where(lane < length - step, pltpu.roll(local, length - step, 1), 0.0)
        local = local + chain_ref[rollouts * at : rollouts * (at + 1), :] * later
        step, at = 2 * step, at + 1
    coef = coef_ref[...]
    count = lane_sum(weight)
    safe = 1.0 / jnp.maximum(count, 1.0)
    mean_l = lane_sum(weight * local) * safe
    mean_c = lane_sum(weight * coef) * safe
    off_l = weight * (local - mean_l)
    off_c = weight * (coef - mean_c)
    stats = {
        OFFSET: values[:, 0:1] + trace_ref[:, 0:1] * local[:, 0:1],
        COUNT: count,
        MEAN_L: mean_l,
        MEAN_C: mean_c,
        VAR_L: lane_sum(off_l * off_l),
        COV: lane_sum(off_l * off_c),
        VAR_C: lane_sum(off_c * off_c),
    }
    small_lane = lax.broadcasted_iota(jnp.int32, (rollouts, 128), 1)
    summary = fixed_ref[...]
    for at, stat in stats.items():
        summary = jnp.where(small_lane == at, stat, summary)
    summary = pltpu.roll(summary, 0, 1, stride=WIDTH, stride_axis=0)
    summary = jnp.sum(summary, axis=0, keepdims=True)
    mine = lax.broadcasted_iota(jnp.int32, shape, 0) == me
    own_local = jnp.sum(jnp.where(mine, local, 0.0), axis=0, keepdims=True)
    values_ref[...] = jnp.sum(jnp.where(mine, values, 0.0), axis=0, keepdims=True)
    row = lax.broadcasted_iota(jnp.int32, (8, 128), 0)
    message = jnp.where(row == 0, summary, 0.0)
    message = jnp.where(row == 1, own_local[:, :128], message)
    message = jnp.where(row == 2, own_local[:, 128:], message)
    message = jnp.where(row == 3, ratio_ref[:, :128], message)
    message = jnp.where(row == 4, ratio_ref[:, 128:], message)
    for peer in range(out_ref.shape[0] // TOKEN_ROWS):
        out_ref[TOKEN_ROWS * peer : TOKEN_ROWS * (peer + 1), :] = message[0:TOKEN_ROWS, :]


def seq_order(size):
    runs = size // 8
    order = SEQ_RUNS if runs == len(SEQ_RUNS) else range(runs)
    return [8 * run + i for run in order for i in range(8)]


def from_blocks(ref, at):
    blocks = ref.shape[0] // TOKEN_ROWS
    rows = ref[pl.ds(at, blocks, stride=TOKEN_ROWS), :]
    order = seq_order(blocks)
    slots = [order.index(8 * run) for run in range(blocks // 8)]
    return jnp.concatenate([rows[slot : slot + 8] for slot in slots], axis=0)


def full_sum(x):
    return jnp.sum(jnp.sum(x, axis=0, keepdims=True), axis=1, keepdims=True)


def final_kernel(recv_ref, power_ref, start_ref, white_ref, loss_ref, out_ref):
    tensor, seq = lax.axis_index("tensor"), lax.axis_index("seq")
    blocks = recv_ref.shape[0] // TOKEN_ROWS
    rollouts = out_ref.shape[0]
    shape = (blocks, 128)
    table = from_blocks(recv_ref, 0)
    row = lax.broadcasted_iota(jnp.int32, shape, 0)
    lane = lax.broadcasted_iota(jnp.int32, shape, 1)

    def stat(at):
        return pltpu.roll(table, 128 - at, 1)

    last = row == blocks - 1
    offset = jnp.where(last, start_ref[...], pltpu.roll(table, blocks - 1, 0))
    slope = jnp.where(last, 0.0, pltpu.roll(stat(SLOPE), blocks - 1, 0))
    step = 1
    while step < blocks:
        inside = row < blocks - step
        offset_later = jnp.where(inside, pltpu.roll(offset, blocks - step, 0), 0.0)
        slope_later = jnp.where(inside, pltpu.roll(slope, blocks - step, 0), 0.0)
        offset = offset + slope * offset_later
        slope = slope * slope_later
        step *= 2
    entering = offset
    used = (lane % WIDTH == 0) & (lane < WIDTH * rollouts)
    members = jnp.where(used, stat(COUNT), 0.0)
    block_mean = jnp.where(used, stat(MEAN_L) + entering * stat(MEAN_C), 0.0)
    count = full_sum(members)
    mean = full_sum(members * block_mean) / count
    within = stat(VAR_L) + entering * (2.0 * stat(COV) + entering * stat(VAR_C))
    apart = block_mean - mean
    variance = full_sum(jnp.where(used, within, 0.0) + members * apart * apart) / count
    scale = lax.rsqrt(variance + EPS_WHITE)

    mine = lane == WIDTH * tensor
    own_entering = lane_sum(jnp.where(mine, entering, 0.0))
    own_done = lane_sum(jnp.where(mine, stat(LAST_DONE), 0.0))
    power = power_ref[pl.ds(tensor, 1), :]
    loss = jnp.zeros(shape, jnp.float32)
    mine_row = row == seq
    for half in range(2):
        lanes = slice(128 * half, 128 * (half + 1))
        position = (lane + 128 * half).astype(jnp.float32)
        coef = jnp.where(position > own_done, power[:, lanes], 0.0)
        local = from_blocks(recv_ref, 1 + half)
        ratio = from_blocks(recv_ref, 3 + half)
        white = (local + coef * own_entering - mean) * scale
        clipped = jnp.clip(ratio, 1.0 - CLIP, 1.0 + CLIP)
        token = jnp.where(ratio > 0.0, -jnp.minimum(ratio * white, clipped * white), 0.0)
        loss = loss + token
        white_ref[:, lanes] = jnp.sum(jnp.where(mine_row, white, 0.0), axis=0, keepdims=True)
        loss_ref[:, lanes] = jnp.sum(jnp.where(mine_row, token, 0.0), axis=0, keepdims=True)
    out_ref[...] = jnp.broadcast_to(full_sum(loss) / count, out_ref.shape)


def last_kernel(
    values_ref, white_ref, loss_ref, recv_ref, values_hbm, white_hbm, loss_hbm, policy_ref, sent
):
    writes = [
        pltpu.make_async_copy(source, target, sent.at[i])
        for i, (source, target) in enumerate(
            ((values_ref, values_hbm), (white_ref, white_hbm), (loss_ref, loss_hbm))
        )
    ]
    for write in writes:
        write.start()
    policy_ref[0, 0] = jnp.sum(recv_ref[:, 0:1])
    for write in writes:
        write.wait()


VMEM = pl.BlockSpec(memory_space=pltpu.VMEM)
ANY = pl.BlockSpec(memory_space=pl.ANY)


def on_chip(x):
    return pltpu.with_memory_space_constraint(x, pltpu.VMEM)


def on_chip_shape(shape):
    return pltpu.VMEM(shape, jnp.float32)


def exchange(x, axis, order):
    return lax.all_to_all(x, axis, 0, 0, axis_index_groups=[order], tiled=True)


def run_head(
    peers,
    hidden,
    norm_gain,
    value_weight,
    done_flags,
    valid_mask,
    new_logprob,
    old_logprob,
    discount,
    trace_decay,
    bootstrap,
):
    rollouts, length, width = hidden.shape
    f32 = jnp.float32
    steps = length.bit_length() - 1
    return pl.pallas_call(
        head_kernel,
        out_shape=(
            on_chip_shape((peers * HEAD_ROWS, 128)),
            on_chip_shape((rollouts, length)),
            on_chip_shape((rollouts * steps, length)),
            on_chip_shape((rollouts, length)),
            on_chip_shape((rollouts, length)),
            on_chip_shape((rollouts, 128)),
            on_chip_shape((rollouts, 128)),
            on_chip_shape((1, length)),
            on_chip_shape((1, 128)),
        ),
        in_specs=[ANY] * 10,
        out_specs=(VMEM,) * 9,
        scratch_shapes=[
            pltpu.VMEM(hidden.shape, hidden.dtype),
            pltpu.VMEM((width // 128, 128), norm_gain.dtype),
            pltpu.VMEM((width // 128, 128), value_weight.dtype),
            pltpu.VMEM(done_flags.shape, done_flags.dtype),
            pltpu.VMEM(valid_mask.shape, valid_mask.dtype),
            pltpu.VMEM(new_logprob.shape, f32),
            pltpu.VMEM(old_logprob.shape, f32),
            pltpu.SMEM(discount.shape, f32),
            pltpu.SMEM(trace_decay.shape, f32),
            pltpu.SMEM(bootstrap.shape, f32),
            pltpu.VMEM((2, length, 3 * 128), jnp.bfloat16),
            pltpu.VMEM((rollouts, 3 * 128, 128), jnp.bfloat16),
            pltpu.VMEM((length, 128), f32),
            pltpu.SemaphoreType.DMA((rollouts + 9,)),
        ],
        name="head",
    )(
        norm_gain.reshape(-1, 128),
        value_weight.reshape(-1, 128),
        done_flags,
        valid_mask,
        new_logprob,
        old_logprob,
        discount,
        trace_decay,
        bootstrap,
        hidden,
    )


def shards(
    hidden,
    norm_gain,
    value_weight,
    rewards,
    done_flags,
    valid_mask,
    new_logprob,
    old_logprob,
    discount,
    trace_decay,
    bootstrap,
):
    rollouts, length, width = hidden.shape
    peers, blocks = lax.axis_size("tensor"), lax.axis_size("seq")
    sent, gate, chain, coef, power, fixed, trace, ratio, start = run_head(
        peers,
        hidden,
        norm_gain,
        value_weight,
        done_flags,
        valid_mask,
        new_logprob,
        old_logprob,
        discount,
        trace_decay,
        bootstrap,
    )
    got = exchange(sent.reshape(peers, 1, HEAD_ROWS * 128), "tensor", TENSOR_ORDER)
    values, sent = pl.pallas_call(
        partial(local_kernel, width * peers),
        out_shape=(
            on_chip_shape((1, length)),
            on_chip_shape((blocks * TOKEN_ROWS, 128)),
        ),
        in_specs=[VMEM] * 8,
        out_specs=(VMEM, VMEM),
        name="local",
    )(
        *map(
            on_chip,
            (
                got.reshape(peers * HEAD_ROWS, 128),
                rewards,
                gate,
                chain,
                coef,
                fixed,
                trace,
                ratio,
            ),
        )
    )
    got = exchange(sent.reshape(blocks, 1, TOKEN_ROWS * 128), "seq", seq_order(blocks))
    white, loss, sent = pl.pallas_call(
        final_kernel,
        out_shape=(
            on_chip_shape((1, length)),
            on_chip_shape((1, length)),
            on_chip_shape((peers, 128)),
        ),
        in_specs=[VMEM] * 3,
        out_specs=(VMEM, VMEM, VMEM),
        name="final",
    )(*map(on_chip, (got.reshape(blocks * TOKEN_ROWS, 128), power, start)))
    got = exchange(sent.reshape(peers, 1, 128), "tensor", TENSOR_ORDER)
    own_row = jax.ShapeDtypeStruct((1, length), jnp.float32)
    values, white, loss, policy = pl.pallas_call(
        last_kernel,
        out_shape=(own_row, own_row, own_row, jax.ShapeDtypeStruct((1, 1), jnp.float32)),
        in_specs=[VMEM] * 4,
        out_specs=(ANY, ANY, ANY, pl.BlockSpec(memory_space=pltpu.SMEM)),
        scratch_shapes=[pltpu.SemaphoreType.DMA((3,))],
        name="last",
    )(*map(on_chip, (values, white, loss, got.reshape(peers, 128))))
    return values, white, loss, policy.reshape(())


def solution(mesh):
    in_specs = (
        P(None, "seq", "tensor"),
        P("tensor"),
        P("tensor"),
        P(None, "seq"),
        P(None, "seq"),
        P("tensor", "seq"),
        P("tensor", "seq"),
        P("tensor", "seq"),
        P(),
        P(),
        P(),
    )
    out_specs = (P("tensor", "seq"), P("tensor", "seq"), P("tensor", "seq"), P())
    return jax.shard_map(
        shards, mesh=mesh, in_specs=in_specs, out_specs=out_specs, check_vma=False
    )
```

```python
from functools import partial

import jax
import jax.numpy as jnp
from jax import lax
from jax.experimental import pallas as pl
from jax.experimental.pallas import tpu as pltpu
from jax.sharding import PartitionSpec as P

EPS_NORM = 1e-06
EPS_WHITE = 1e-08
CLIP = 0.2

HEAD_ROWS = 40
TOKEN_ROWS = 3
WIDTH = 16
OFFSET, SLOPE, COUNT, MEAN_L, MEAN_C, VAR_L, COV, VAR_C, LAST_DONE = range(9)

CHUNK = 64

ALONG_Z = 16
TENSOR_FIRST, SEQ_FIRST, PAIR_FIRST = 5, 41, 13


def column(ref, shape):
    row = lax.broadcasted_iota(jnp.int32, shape, 0)
    out = jnp.full(shape, ref[0], jnp.float32)
    for r in range(1, shape[0]):
        out = jnp.where(row == r, ref[r], out)
    return out


def lane_sum(x):
    return jnp.sum(x, axis=1, keepdims=True)


def head_kernel(
    gain_hbm,
    weight_hbm,
    done_hbm,
    mask_hbm,
    new_hbm,
    old_hbm,
    discount_hbm,
    trace_hbm,
    bootstrap_hbm,
    hidden_ref,
    out_ref,
    gate_ref,
    chain_ref,
    coef_ref,
    power_ref,
    fixed_ref,
    trace_ref,
    ratio_ref,
    start_ref,
    held,
    gain_ref,
    weight_ref,
    done_ref,
    mask_ref,
    new_ref,
    old_ref,
    discount_smem,
    trace_smem,
    bootstrap_smem,
    split_ref,
    pick_ref,
    sums_ref,
    arrived,
):
    rollouts, length, width = held.shape
    peers = out_ref.shape[0] // HEAD_ROWS
    small = [
        pltpu.make_async_copy(source, target, arrived.at[rollouts + i])
        for i, (source, target) in enumerate(
            (
                (gain_hbm, gain_ref),
                (weight_hbm, weight_ref),
                (done_hbm, done_ref),
                (mask_hbm, mask_ref),
                (new_hbm, new_ref),
                (old_hbm, old_ref),
                (discount_hbm, discount_smem),
                (trace_hbm, trace_smem),
                (bootstrap_hbm, bootstrap_smem),
            )
        )
    ]
    copies = [
        pltpu.make_async_copy(hidden_ref.at[r], held.at[r], arrived.at[r]) for r in range(rollouts)
    ]
    for copy in copies[:1] + small + copies[1:]:
        copy.start()
    picked = lax.broadcasted_iota(jnp.int32, (3 * 128, 128), 0) % 128 // 64 * 8
    picked = lax.broadcasted_iota(jnp.int32, (3 * 128, 128), 1) - picked
    for r in range(rollouts):
        pick_ref[r] = jnp.where(picked == r, 1.0, 0.0).astype(jnp.bfloat16)
    for copy in small:
        copy.wait()

    scaled = gain_ref[...].astype(jnp.float32) * weight_ref[...].astype(jnp.float32)
    small_lane = lax.broadcasted_iota(jnp.int32, (8, 128), 1)

    def partial_sums(r, here):
        squares = products = jnp.zeros((CHUNK, 128), jnp.float32)
        for j in range(width // 128):
            wide = held[r, here, 128 * j : 128 * (j + 1)].astype(jnp.float32)
            squares = squares + wide * wide
            products = products + wide * scaled[j : j + 1, :]
        left = small_lane[0:1] < 64
        rest = jnp.where(left, squares, products)
        rest = rest + pltpu.roll(jnp.where(left, products, squares), 64, 1)
        for part in range(3):
            coarse = rest.astype(jnp.bfloat16)
            split_ref[r % 2, here, 128 * part : 128 * (part + 1)] = coarse
            rest = rest - coarse.astype(jnp.float32)

    def lane_sums(r):
        sums = jnp.dot(split_ref[r % 2], pick_ref[r], preferred_element_type=jnp.float32)
        sums_ref[...] = sums_ref[...] + sums if r else sums

    def finish():
        for half in range(length // 128):
            turned = jnp.transpose(sums_ref[128 * half : 128 * (half + 1), :])
            for peer in range(peers):
                for kind in range(2):
                    at = HEAD_ROWS * peer + 8 * (2 * kind + half)
                    out_ref[at : at + 8, :] = turned[8 * kind : 8 * (kind + 1)]

    shape = (rollouts, length)
    lane = lax.broadcasted_iota(jnp.int32, shape, 1)

    def piece_own():
        mask = mask_ref[...].astype(jnp.float32)
        ratio_ref[...] = mask * jnp.exp(new_ref[...] - old_ref[...])
        row = lax.broadcasted_iota(jnp.int32, (8, 128), 0)
        rest = jnp.where(row == 0, mask[:, :128], jnp.where(row == 1, mask[:, 128:], 0.0))
        for peer in range(peers):
            out_ref[HEAD_ROWS * peer + 32 : HEAD_ROWS * (peer + 1), :] = rest
        start_lane = lax.broadcasted_iota(jnp.int32, (1, 128), 1)
        start = jnp.full((1, 128), bootstrap_smem[0], jnp.float32)
        for r in range(1, rollouts):
            start = jnp.where(start_lane == WIDTH * r, bootstrap_smem[r], start)
        start_ref[...] = start

    def piece_chain_start():
        discount, trace = column(discount_smem, shape), column(trace_smem, shape)
        alive = 1.0 - done_ref[...].astype(jnp.float32)
        gate_ref[...] = discount * alive
        chain_ref[0:rollouts, :] = discount * trace * alive
        trace_ref[...] = trace[:, :128]
        last_done = jnp.where(alive > 0.5, -1.0, lane.astype(jnp.float32))
        last_done = jnp.max(last_done, axis=1, keepdims=True)
        fixed_ref[...] = jnp.where(small_lane == LAST_DONE, last_done, 0.0)

    def piece_chain(at):
        step = 1 << at
        chain = chain_ref[rollouts * at : rollouts * (at + 1), :]
        later = pltpu.roll(chain, length - step, 1)
        chain = chain * jnp.where(lane < length - step, later, 1.0)
        if 2 * step < length:
            chain_ref[rollouts * (at + 1) : rollouts * (at + 2), :] = chain
            return
        coef_ref[...] = chain / column(trace_smem, shape)
        fixed_ref[...] = jnp.where(small_lane == SLOPE, chain[:, 0:1], fixed_ref[...])

    def piece_power():
        discount = column(discount_smem, shape)
        left = length - 1 - lane
        power, factor, bit = discount, discount * column(trace_smem, shape), 1
        while bit < length:
            power = jnp.where(left & bit != 0, power * factor, power)
            factor = factor * factor
            bit *= 2
        power_ref[...] = power

    steps = length.bit_length() - 1
    pieces = [[] for _ in range(rollouts)]
    pieces[0] = [piece_chain_start]
    for at in range(steps):
        pieces[1 + at * (rollouts - 2) // steps].append(partial(piece_chain, at))
    pieces[0].append(piece_own)
    pieces[rollouts - 2].append(piece_power)

    for r in range(rollouts):
        copies[r].wait()
        for piece in pieces[r]:
            piece()
        if r:
            lane_sums(r - 1)
        for first in range(0, length, CHUNK):
            partial_sums(r, slice(first, first + CHUNK))
    lane_sums(rollouts - 1)
    finish()


def local_kernel(
    hidden_width,
    recv_ref,
    rewards_ref,
    gate_ref,
    chain_ref,
    coef_ref,
    fixed_ref,
    trace_ref,
    ratio_ref,
    values_ref,
    own_ref,
    out_ref,
):
    me = lax.axis_index("tensor")
    rollouts, length = rewards_ref.shape
    peers = recv_ref.shape[0] // HEAD_ROWS
    shape = (rollouts, length)
    total = recv_ref[0:32, :]
    for peer in range(1, peers):
        total = total + recv_ref[HEAD_ROWS * peer : HEAD_ROWS * peer + 32, :]
    squares = jnp.concatenate([total[0:8], total[8:16]], axis=1)
    products = jnp.concatenate([total[16:24], total[24:32]], axis=1)
    weight = jnp.concatenate(
        [
            recv_ref[pl.ds(32, peers, stride=HEAD_ROWS), :],
            recv_ref[pl.ds(33, peers, stride=HEAD_ROWS), :],
        ],
        axis=1,
    )
    weight = in_order(weight, TENSOR_FIRST)
    values = products * lax.rsqrt(squares / hidden_width + EPS_NORM)
    lane = lax.broadcasted_iota(jnp.int32, shape, 1)
    inner_next = jnp.where(lane < length - 1, pltpu.roll(values, length - 1, 1), 0.0)
    local = rewards_ref[...] + gate_ref[...] * inner_next - values
    step, at = 1, 0
    while step < length:
        later = jnp.where(lane < length - step, pltpu.roll(local, length - step, 1), 0.0)
        local = local + chain_ref[rollouts * at : rollouts * (at + 1), :] * later
        step, at = 2 * step, at + 1
    coef = coef_ref[...]
    count = lane_sum(weight)
    safe = 1.0 / jnp.maximum(count, 1.0)
    mean_l = lane_sum(weight * local) * safe
    mean_c = lane_sum(weight * coef) * safe
    off_l = weight * (local - mean_l)
    off_c = weight * (coef - mean_c)
    stats = {
        OFFSET: values[:, 0:1] + trace_ref[:, 0:1] * local[:, 0:1],
        COUNT: count,
        MEAN_L: mean_l,
        MEAN_C: mean_c,
        VAR_L: lane_sum(off_l * off_l),
        COV: lane_sum(off_l * off_c),
        VAR_C: lane_sum(off_c * off_c),
    }
    small_lane = lax.broadcasted_iota(jnp.int32, (rollouts, 128), 1)
    summary = fixed_ref[...]
    for at, stat in stats.items():
        summary = jnp.where(small_lane == at, stat, summary)
    summary = pltpu.roll(summary, 0, 1, stride=WIDTH, stride_axis=0)
    summary = jnp.sum(summary, axis=0, keepdims=True)
    mine = lax.broadcasted_iota(jnp.int32, shape, 0) == me
    own_local = jnp.sum(jnp.where(mine, local, 0.0), axis=0, keepdims=True)
    values_ref[...] = jnp.sum(jnp.where(mine, values, 0.0), axis=0, keepdims=True)
    row = lax.broadcasted_iota(jnp.int32, (8, 128), 0)
    own_ref[...] = own_local
    messages = []
    for half in range(2):
        lanes = slice(128 * half, 128 * (half + 1))
        message = jnp.where(row == 1, own_local[:, lanes], ratio_ref[:, lanes])
        messages.append(jnp.where(row == 0, summary, message)[0:TOKEN_ROWS])
    blocks = out_ref.shape[0] // TOKEN_ROWS
    for slot, member in enumerate(order_from(blocks, SEQ_FIRST)):
        half = member // ALONG_Z % 2
        out_ref[TOKEN_ROWS * slot : TOKEN_ROWS * (slot + 1), :] = messages[half]


def order_from(size, first):
    order = list(range(size))
    order[0], order[first] = order[first], order[0]
    return order


def in_order(rows, first):
    row = lax.broadcasted_iota(jnp.int32, rows.shape, 0)
    swapped = jnp.where(row == 0, rows[first : first + 1], rows)
    return jnp.where(row == first, rows[0:1], swapped)


def from_blocks(ref, at):
    blocks = ref.shape[0] // TOKEN_ROWS
    return in_order(ref[pl.ds(at, blocks, stride=TOKEN_ROWS), :], SEQ_FIRST)


def full_sum(x):
    return jnp.sum(jnp.sum(x, axis=0, keepdims=True), axis=1, keepdims=True)


def final_kernel(
    recv_ref, power_ref, start_ref, own_ref, ratio_ref, white_ref, loss_ref, out_ref
):
    tensor, seq = lax.axis_index("tensor"), lax.axis_index("seq")
    blocks = recv_ref.shape[0] // TOKEN_ROWS
    rollouts = power_ref.shape[0]
    shape = (blocks, 128)
    table = from_blocks(recv_ref, 0)
    row = lax.broadcasted_iota(jnp.int32, shape, 0)
    lane = lax.broadcasted_iota(jnp.int32, shape, 1)

    def stat(at):
        return pltpu.roll(table, 128 - at, 1)

    last = row == blocks - 1
    offset = jnp.where(last, start_ref[...], pltpu.roll(table, blocks - 1, 0))
    slope = jnp.where(last, 0.0, pltpu.roll(stat(SLOPE), blocks - 1, 0))
    step = 1
    while step < blocks:
        inside = row < blocks - step
        offset_later = jnp.where(inside, pltpu.roll(offset, blocks - step, 0), 0.0)
        slope_later = jnp.where(inside, pltpu.roll(slope, blocks - step, 0), 0.0)
        offset = offset + slope * offset_later
        slope = slope * slope_later
        step *= 2
    entering = offset
    used = (lane % WIDTH == 0) & (lane < WIDTH * rollouts)
    members = jnp.where(used, stat(COUNT), 0.0)
    block_mean = jnp.where(used, stat(MEAN_L) + entering * stat(MEAN_C), 0.0)
    count = full_sum(members)
    mean = full_sum(members * block_mean) / count
    within = stat(VAR_L) + entering * (2.0 * stat(COV) + entering * stat(VAR_C))
    apart = block_mean - mean
    variance = full_sum(jnp.where(used, within, 0.0) + members * apart * apart) / count
    scale = lax.rsqrt(variance + EPS_WHITE)

    mine = lane == WIDTH * tensor
    own_entering = lane_sum(jnp.where(mine, entering, 0.0))
    own_done = lane_sum(jnp.where(mine, stat(LAST_DONE), 0.0))
    power = power_ref[pl.ds(tensor, 1), :]

    def losses(local, ratio, coef, from_later):
        white = (local + coef * from_later - mean) * scale
        clipped = jnp.clip(ratio, 1.0 - CLIP, 1.0 + CLIP)
        return white, jnp.where(ratio > 0.0, -jnp.minimum(ratio * white, clipped * white), 0.0)

    half = seq // ALONG_Z % 2
    power_half = jnp.where(half == 0, power[:, :128], power[:, 128:])
    coef = jnp.where((lane + 128 * half).astype(jnp.float32) > own_done, power_half, 0.0)
    _, token = losses(from_blocks(recv_ref, 1), from_blocks(recv_ref, 2), coef, own_entering)
    out_ref[...] = jnp.broadcast_to(full_sum(token) / count, out_ref.shape)

    here = row[:, 0:1] == seq
    position = lax.broadcasted_iota(jnp.int32, power.shape, 1).astype(jnp.float32)
    own_done = jnp.sum(jnp.where(here, own_done, 0.0), axis=0, keepdims=True)
    own_entering = jnp.sum(jnp.where(here, own_entering, 0.0), axis=0, keepdims=True)
    coef = jnp.where(position > own_done, power, 0.0)
    white_ref[...], loss_ref[...] = losses(own_ref[...], ratio_ref[...], coef, own_entering)


def last_kernel(
    values_ref,
    white_ref,
    loss_ref,
    recv_ref,
    values_hbm,
    white_hbm,
    loss_hbm,
    policy_hbm,
    policy_ref,
    sent,
):
    writes = [
        pltpu.make_async_copy(source, target, sent.at[i])
        for i, (source, target) in enumerate(
            (
                (values_ref, values_hbm),
                (white_ref, white_hbm),
                (loss_ref, loss_hbm),
                (policy_ref, policy_hbm),
            )
        )
    ]
    for write in writes[:3]:
        write.start()
    policy_ref[0, 0] = jnp.sum(recv_ref[:, 0:1])
    writes[3].start()
    for write in writes:
        write.wait()


VMEM = pl.BlockSpec(memory_space=pltpu.VMEM)
ANY = pl.BlockSpec(memory_space=pl.ANY)


def on_chip(x):
    return pltpu.with_memory_space_constraint(x, pltpu.VMEM)


def on_chip_shape(shape):
    return pltpu.VMEM(shape, jnp.float32)


def exchange(x, axis, groups):
    return lax.all_to_all(x, axis, 0, 0, axis_index_groups=groups, tiled=True)


def pair_groups(blocks, peers):
    groups = []
    for first in range(0, blocks, 2 * ALONG_Z):
        for block in range(first, first + ALONG_Z):
            members = [b * peers + i for b in (block, block + ALONG_Z) for i in range(peers)]
            groups.append([members[i] for i in order_from(2 * peers, PAIR_FIRST)])
    return groups


def run_head(
    peers,
    hidden,
    norm_gain,
    value_weight,
    done_flags,
    valid_mask,
    new_logprob,
    old_logprob,
    discount,
    trace_decay,
    bootstrap,
):
    rollouts, length, width = hidden.shape
    f32 = jnp.float32
    steps = length.bit_length() - 1
    return pl.pallas_call(
        head_kernel,
        out_shape=(
            on_chip_shape((peers * HEAD_ROWS, 128)),
            on_chip_shape((rollouts, length)),
            on_chip_shape((rollouts * steps, length)),
            on_chip_shape((rollouts, length)),
            on_chip_shape((rollouts, length)),
            on_chip_shape((rollouts, 128)),
            on_chip_shape((rollouts, 128)),
            on_chip_shape((1, length)),
            on_chip_shape((1, 128)),
        ),
        in_specs=[ANY] * 10,
        out_specs=(VMEM,) * 9,
        scratch_shapes=[
            pltpu.VMEM(hidden.shape, hidden.dtype),
            pltpu.VMEM((width // 128, 128), norm_gain.dtype),
            pltpu.VMEM((width // 128, 128), value_weight.dtype),
            pltpu.VMEM(done_flags.shape, done_flags.dtype),
            pltpu.VMEM(valid_mask.shape, valid_mask.dtype),
            pltpu.VMEM(new_logprob.shape, f32),
            pltpu.VMEM(old_logprob.shape, f32),
            pltpu.SMEM(discount.shape, f32),
            pltpu.SMEM(trace_decay.shape, f32),
            pltpu.SMEM(bootstrap.shape, f32),
            pltpu.VMEM((2, length, 3 * 128), jnp.bfloat16),
            pltpu.VMEM((rollouts, 3 * 128, 128), jnp.bfloat16),
            pltpu.VMEM((length, 128), f32),
            pltpu.SemaphoreType.DMA((rollouts + 9,)),
        ],
        name="head",
    )(
        norm_gain.reshape(-1, 128),
        value_weight.reshape(-1, 128),
        done_flags,
        valid_mask,
        new_logprob,
        old_logprob,
        discount,
        trace_decay,
        bootstrap,
        hidden,
    )


def shards(
    hidden,
    norm_gain,
    value_weight,
    rewards,
    done_flags,
    valid_mask,
    new_logprob,
    old_logprob,
    discount,
    trace_decay,
    bootstrap,
):
    rollouts, length, width = hidden.shape
    peers, blocks = lax.axis_size("tensor"), lax.axis_size("seq")
    sent, gate, chain, coef, power, fixed, trace, ratio, start = run_head(
        peers,
        hidden,
        norm_gain,
        value_weight,
        done_flags,
        valid_mask,
        new_logprob,
        old_logprob,
        discount,
        trace_decay,
        bootstrap,
    )
    got = exchange(sent.reshape(peers, 1, HEAD_ROWS * 128), "tensor", [order_from(peers, TENSOR_FIRST)])
    values, own, sent = pl.pallas_call(
        partial(local_kernel, width * peers),
        out_shape=(
            on_chip_shape((1, length)),
            on_chip_shape((1, length)),
            on_chip_shape((blocks * TOKEN_ROWS, 128)),
        ),
        in_specs=[VMEM] * 8,
        out_specs=(VMEM,) * 3,
        name="local",
    )(
        *map(
            on_chip,
            (
                got.reshape(peers * HEAD_ROWS, 128),
                rewards,
                gate,
                chain,
                coef,
                fixed,
                trace,
                ratio,
            ),
        )
    )
    got = exchange(sent.reshape(blocks, 1, TOKEN_ROWS * 128), "seq", [order_from(blocks, SEQ_FIRST)])
    white, loss, sent = pl.pallas_call(
        final_kernel,
        out_shape=(
            on_chip_shape((1, length)),
            on_chip_shape((1, length)),
            on_chip_shape((2 * peers, 128)),
        ),
        in_specs=[VMEM] * 5,
        out_specs=(VMEM, VMEM, VMEM),
        name="final",
    )(*map(on_chip, (got.reshape(blocks * TOKEN_ROWS, 128), power, start, own, ratio)))
    groups = pair_groups(blocks, peers)
    got = exchange(sent.reshape(2 * peers, 1, 128), ("seq", "tensor"), groups)
    own_row = jax.ShapeDtypeStruct((1, length), jnp.float32)
    values, white, loss, policy = pl.pallas_call(
        last_kernel,
        out_shape=(own_row, own_row, own_row, jax.ShapeDtypeStruct((1, 1), jnp.float32)),
        in_specs=[VMEM] * 4,
        out_specs=(ANY,) * 4,
        scratch_shapes=[pltpu.SMEM((1, 1), jnp.float32), pltpu.SemaphoreType.DMA((4,))],
        name="last",
    )(*map(on_chip, (values, white, loss, got.reshape(2 * peers, 128))))
    return values, white, loss, policy.reshape(())


def solution(mesh):
    in_specs = (
        P(None, "seq", "tensor"),
        P("tensor"),
        P("tensor"),
        P(None, "seq"),
        P(None, "seq"),
        P("tensor", "seq"),
        P("tensor", "seq"),
        P("tensor", "seq"),
        P(),
        P(),
        P(),
    )
    out_specs = (P("tensor", "seq"), P("tensor", "seq"), P("tensor", "seq"), P())
    return jax.shard_map(
        shards, mesh=mesh, in_specs=in_specs, out_specs=out_specs, check_vma=False
    )
```

```python
from functools import partial

import jax
import jax.numpy as jnp
from jax import lax
from jax.experimental import pallas as pl
from jax.experimental.pallas import tpu as pltpu
from jax.sharding import PartitionSpec as P

EPS_NORM = 1e-06
EPS_WHITE = 1e-08
CLIP = 0.2

HEAD_ROWS = 34
TOKEN_ROWS = 3
WIDTH = 16
OFFSET, SLOPE, COUNT, MEAN_L, MEAN_C, VAR_L, COV, VAR_C, LAST_DONE = range(9)

CHUNK = 64

ALONG_Z = 16
TENSOR_FIRST, SEQ_FIRST, PAIR_FIRST = 5, 41, 13


def column(ref, shape):
    row = lax.broadcasted_iota(jnp.int32, shape, 0)
    out = jnp.full(shape, ref[0], jnp.float32)
    for r in range(1, shape[0]):
        out = jnp.where(row == r, ref[r], out)
    return out


def lane_sum(x):
    return jnp.sum(x, axis=1, keepdims=True)


def head_kernel(
    gain_hbm,
    weight_hbm,
    done_hbm,
    mask_hbm,
    new_hbm,
    old_hbm,
    discount_hbm,
    trace_hbm,
    bootstrap_hbm,
    hidden_ref,
    out_ref,
    gate_ref,
    chain_ref,
    triple_ref,
    coef_ref,
    power_ref,
    fixed_ref,
    trace_ref,
    ratio_ref,
    start_ref,
    held,
    gain_ref,
    weight_ref,
    done_ref,
    mask_ref,
    new_ref,
    old_ref,
    discount_smem,
    trace_smem,
    bootstrap_smem,
    split_ref,
    pick_ref,
    sums_ref,
    arrived,
):
    rollouts, length, width = held.shape
    peers = out_ref.shape[0] // HEAD_ROWS
    small = [
        pltpu.make_async_copy(source, target, arrived.at[rollouts + i])
        for i, (source, target) in enumerate(
            (
                (gain_hbm, gain_ref),
                (weight_hbm, weight_ref),
                (done_hbm, done_ref),
                (mask_hbm, mask_ref),
                (new_hbm, new_ref),
                (old_hbm, old_ref),
                (discount_hbm, discount_smem),
                (trace_hbm, trace_smem),
                (bootstrap_hbm, bootstrap_smem),
            )
        )
    ]
    copies = [
        pltpu.make_async_copy(hidden_ref.at[r], held.at[r], arrived.at[r]) for r in range(rollouts)
    ]
    for copy in copies[:1] + small + copies[1:]:
        copy.start()
    picked = lax.broadcasted_iota(jnp.int32, (3 * 128, 128), 0) % 128 // 64 * 8
    picked = lax.broadcasted_iota(jnp.int32, (3 * 128, 128), 1) - picked
    for r in range(rollouts):
        pick_ref[r] = jnp.where(picked == r, 1.0, 0.0).astype(jnp.bfloat16)
    for copy in small:
        copy.wait()

    scaled = gain_ref[...].astype(jnp.float32) * weight_ref[...].astype(jnp.float32)
    small_lane = lax.broadcasted_iota(jnp.int32, (8, 128), 1)

    def partial_sums(r, here):
        squares = products = jnp.zeros((CHUNK, 128), jnp.float32)
        for j in range(width // 128):
            wide = held[r, here, 128 * j : 128 * (j + 1)].astype(jnp.float32)
            squares = squares + wide * wide
            products = products + wide * scaled[j : j + 1, :]
        left = small_lane[0:1] < 64
        rest = jnp.where(left, squares, products)
        rest = rest + pltpu.roll(jnp.where(left, products, squares), 64, 1)
        for part in range(3):
            coarse = rest.astype(jnp.bfloat16)
            split_ref[r % 2, here, 128 * part : 128 * (part + 1)] = coarse
            rest = rest - coarse.astype(jnp.float32)

    def lane_sums(r):
        sums = jnp.dot(split_ref[r % 2], pick_ref[r], preferred_element_type=jnp.float32)
        sums_ref[...] = sums_ref[...] + sums if r else sums

    def finish():
        for half in range(length // 128):
            turned = jnp.transpose(sums_ref[128 * half : 128 * (half + 1), :])
            for peer in range(peers):
                for kind in range(2):
                    at = HEAD_ROWS * peer + 8 * (2 * kind + half)
                    out_ref[at : at + 8, :] = turned[8 * kind : 8 * (kind + 1)]

    shape = (rollouts, length)
    lane = lax.broadcasted_iota(jnp.int32, shape, 1)

    def piece_own():
        mask = mask_ref[...].astype(jnp.float32)
        ratio_ref[...] = mask * jnp.exp(new_ref[...] - old_ref[...])
        for peer in range(peers):
            at = HEAD_ROWS * peer + 32
            out_ref[at : at + 1, :] = mask[:, :128]
            out_ref[at + 1 : at + 2, :] = mask[:, 128:]
        start_lane = lax.broadcasted_iota(jnp.int32, (1, 128), 1)
        start = jnp.full((1, 128), bootstrap_smem[0], jnp.float32)
        for r in range(1, rollouts):
            start = jnp.where(start_lane == WIDTH * r, bootstrap_smem[r], start)
        start_ref[...] = start

    def piece_chain_start():
        discount, trace = column(discount_smem, shape), column(trace_smem, shape)
        alive = 1.0 - done_ref[...].astype(jnp.float32)
        gate_ref[...] = discount * alive
        chain_ref[0:rollouts, :] = discount * trace * alive
        trace_ref[...] = trace[:, :128]
        last_done = jnp.where(alive > 0.5, -1.0, lane.astype(jnp.float32))
        last_done = jnp.max(last_done, axis=1, keepdims=True)
        fixed_ref[...] = jnp.where(small_lane == LAST_DONE, last_done, 0.0)

    def piece_chain(at):
        step = 1 << at
        chain = chain_ref[rollouts * at : rollouts * (at + 1), :]
        later = pltpu.roll(chain, length - step, 1)
        chain = chain * jnp.where(lane < length - step, later, 1.0)
        if 2 * step < length:
            chain_ref[rollouts * (at + 1) : rollouts * (at + 2), :] = chain
            return
        coef_ref[...] = chain / column(trace_smem, shape)
        fixed_ref[...] = jnp.where(small_lane == SLOPE, chain[:, 0:1], fixed_ref[...])

    def piece_triple(at):
        step = 1 << at
        chain = chain_ref[rollouts * at : rollouts * (at + 1), :]
        later = pltpu.roll(chain, length - 2 * step, 1)
        triple = chain_ref[rollouts * (at + 1) : rollouts * (at + 2), :] * later
        triple_ref[rollouts * (at // 2) : rollouts * (at // 2 + 1), :] = triple

    def piece_power():
        discount = column(discount_smem, shape)
        left = length - 1 - lane
        power, factor, bit = discount, discount * column(trace_smem, shape), 1
        while bit < length:
            power = jnp.where(left & bit != 0, power * factor, power)
            factor = factor * factor
            bit *= 2
        power_ref[...] = power

    steps = length.bit_length() - 1
    pieces = [[] for _ in range(rollouts)]
    pieces[0] = [piece_chain_start]
    for at in range(steps):
        pieces[1 + at * (rollouts - 2) // steps].append(partial(piece_chain, at))
    for at in range(0, steps, 2):
        pieces[rollouts - 1].append(partial(piece_triple, at))
    pieces[0].append(piece_own)
    pieces[rollouts - 2].append(piece_power)

    for r in range(rollouts):
        copies[r].wait()
        for piece in pieces[r]:
            piece()
        if r:
            lane_sums(r - 1)
        for first in range(0, length, CHUNK):
            partial_sums(r, slice(first, first + CHUNK))
    lane_sums(rollouts - 1)
    finish()


def local_kernel(
    hidden_width,
    recv_ref,
    rewards_ref,
    gate_ref,
    chain_ref,
    triple_ref,
    coef_ref,
    fixed_ref,
    trace_ref,
    ratio_ref,
    values_ref,
    own_ref,
    out_ref,
):
    me = lax.axis_index("tensor")
    rollouts, length = rewards_ref.shape
    peers = recv_ref.shape[0] // HEAD_ROWS
    shape = (rollouts, length)
    total = recv_ref[0:32, :]
    for peer in range(1, peers):
        total = total + recv_ref[HEAD_ROWS * peer : HEAD_ROWS * peer + 32, :]
    squares = jnp.concatenate([total[0:8], total[8:16]], axis=1)
    products = jnp.concatenate([total[16:24], total[24:32]], axis=1)
    weight = jnp.concatenate(
        [
            recv_ref[pl.ds(32, peers, stride=HEAD_ROWS), :],
            recv_ref[pl.ds(33, peers, stride=HEAD_ROWS), :],
        ],
        axis=1,
    )
    weight = in_order(weight, TENSOR_FIRST)
    values = products * lax.rsqrt(squares / hidden_width + EPS_NORM)
    lane = lax.broadcasted_iota(jnp.int32, shape, 1)
    inner_next = jnp.where(lane < length - 1, pltpu.roll(values, length - 1, 1), 0.0)
    local = rewards_ref[...] + gate_ref[...] * inner_next - values
    step, at = 1, 0
    while step < length:
        factors = (
            chain_ref[rollouts * at : rollouts * (at + 1), :],
            chain_ref[rollouts * (at + 1) : rollouts * (at + 2), :],
            triple_ref[rollouts * (at // 2) : rollouts * (at // 2 + 1), :],
        )
        later = [
            factor * jnp.where(lane < length - k * step, pltpu.roll(local, length - k * step, 1), 0.0)
            for k, factor in enumerate(factors, 1)
        ]
        local = (local + later[0]) + (later[1] + later[2])
        step, at = 4 * step, at + 2
    coef = coef_ref[...]
    count = lane_sum(weight)
    safe = 1.0 / jnp.maximum(count, 1.0)
    mean_l = lane_sum(weight * local) * safe
    mean_c = lane_sum(weight * coef) * safe
    off_l = weight * (local - mean_l)
    off_c = weight * (coef - mean_c)
    stats = {
        OFFSET: values[:, 0:1] + trace_ref[:, 0:1] * local[:, 0:1],
        COUNT: count,
        MEAN_L: mean_l,
        MEAN_C: mean_c,
        VAR_L: lane_sum(off_l * off_l),
        COV: lane_sum(off_l * off_c),
        VAR_C: lane_sum(off_c * off_c),
    }
    small_lane = lax.broadcasted_iota(jnp.int32, (rollouts, 128), 1)
    summary = fixed_ref[...]
    for at, stat in stats.items():
        summary = jnp.where(small_lane == at, stat, summary)
    summary = pltpu.roll(summary, 0, 1, stride=WIDTH, stride_axis=0)
    summary = jnp.sum(summary, axis=0, keepdims=True)
    mine = lax.broadcasted_iota(jnp.int32, shape, 0) == me
    own_local = jnp.sum(jnp.where(mine, local, 0.0), axis=0, keepdims=True)
    values_ref[...] = jnp.sum(jnp.where(mine, values, 0.0), axis=0, keepdims=True)
    row = lax.broadcasted_iota(jnp.int32, (8, 128), 0)
    own_ref[...] = own_local
    messages = []
    for half in range(2):
        lanes = slice(128 * half, 128 * (half + 1))
        message = jnp.where(row == 1, own_local[:, lanes], ratio_ref[:, lanes])
        messages.append(jnp.where(row == 0, summary, message)[0:TOKEN_ROWS])
    blocks = out_ref.shape[0] // TOKEN_ROWS
    for slot, member in enumerate(order_from(blocks, SEQ_FIRST)):
        half = member // ALONG_Z % 2
        out_ref[TOKEN_ROWS * slot : TOKEN_ROWS * (slot + 1), :] = messages[half]


def order_from(size, first):
    order = list(range(size))
    order[0], order[first] = order[first], order[0]
    return order


def in_order(rows, first):
    row = lax.broadcasted_iota(jnp.int32, rows.shape, 0)
    swapped = jnp.where(row == 0, rows[first : first + 1], rows)
    return jnp.where(row == first, rows[0:1], swapped)


def from_blocks(ref, at):
    blocks = ref.shape[0] // TOKEN_ROWS
    return in_order(ref[pl.ds(at, blocks, stride=TOKEN_ROWS), :], SEQ_FIRST)


def full_sum(x):
    return jnp.sum(jnp.sum(x, axis=0, keepdims=True), axis=1, keepdims=True)


def final_kernel(
    recv_ref, power_ref, start_ref, own_ref, ratio_ref, white_ref, loss_ref, out_ref
):
    tensor, seq = lax.axis_index("tensor"), lax.axis_index("seq")
    blocks = recv_ref.shape[0] // TOKEN_ROWS
    rollouts = power_ref.shape[0]
    shape = (blocks, 128)
    table = from_blocks(recv_ref, 0)
    row = lax.broadcasted_iota(jnp.int32, shape, 0)
    lane = lax.broadcasted_iota(jnp.int32, shape, 1)

    def stat(at):
        return pltpu.roll(table, 128 - at, 1)

    last = row == blocks - 1
    offset = jnp.where(last, start_ref[...], pltpu.roll(table, blocks - 1, 0))
    slope = jnp.where(last, 0.0, pltpu.roll(stat(SLOPE), blocks - 1, 0))
    step = 1
    while step < blocks:
        inside = row < blocks - step
        offset_later = jnp.where(inside, pltpu.roll(offset, blocks - step, 0), 0.0)
        slope_later = jnp.where(inside, pltpu.roll(slope, blocks - step, 0), 0.0)
        offset = offset + slope * offset_later
        slope = slope * slope_later
        step *= 2
    entering = offset
    used = (lane % WIDTH == 0) & (lane < WIDTH * rollouts)
    members = jnp.where(used, stat(COUNT), 0.0)
    block_mean = jnp.where(used, stat(MEAN_L) + entering * stat(MEAN_C), 0.0)
    count = full_sum(members)
    mean = full_sum(members * block_mean) / count
    within = stat(VAR_L) + entering * (2.0 * stat(COV) + entering * stat(VAR_C))
    apart = block_mean - mean
    variance = full_sum(jnp.where(used, within, 0.0) + members * apart * apart) / count
    scale = lax.rsqrt(variance + EPS_WHITE)

    mine = lane == WIDTH * tensor
    own_entering = lane_sum(jnp.where(mine, entering, 0.0))
    own_done = lane_sum(jnp.where(mine, stat(LAST_DONE), 0.0))
    power = power_ref[pl.ds(tensor, 1), :]

    def losses(local, ratio, coef, from_later):
        white = (local + coef * from_later - mean) * scale
        clipped = jnp.clip(ratio, 1.0 - CLIP, 1.0 + CLIP)
        return white, jnp.where(ratio > 0.0, -jnp.minimum(ratio * white, clipped * white), 0.0)

    half = seq // ALONG_Z % 2
    power_half = jnp.where(half == 0, power[:, :128], power[:, 128:])
    coef = jnp.where((lane + 128 * half).astype(jnp.float32) > own_done, power_half, 0.0)
    _, token = losses(from_blocks(recv_ref, 1), from_blocks(recv_ref, 2), coef, own_entering)
    out_ref[...] = jnp.broadcast_to(full_sum(token) / count, out_ref.shape)

    here = row[:, 0:1] == seq
    position = lax.broadcasted_iota(jnp.int32, power.shape, 1).astype(jnp.float32)
    own_done = jnp.sum(jnp.where(here, own_done, 0.0), axis=0, keepdims=True)
    own_entering = jnp.sum(jnp.where(here, own_entering, 0.0), axis=0, keepdims=True)
    coef = jnp.where(position > own_done, power, 0.0)
    white_ref[...], loss_ref[...] = losses(own_ref[...], ratio_ref[...], coef, own_entering)


def last_kernel(
    values_ref,
    white_ref,
    loss_ref,
    recv_ref,
    values_hbm,
    white_hbm,
    loss_hbm,
    policy_hbm,
    policy_ref,
    sent,
):
    writes = [
        pltpu.make_async_copy(source, target, sent.at[i])
        for i, (source, target) in enumerate(
            (
                (values_ref, values_hbm),
                (white_ref, white_hbm),
                (loss_ref, loss_hbm),
                (policy_ref, policy_hbm),
            )
        )
    ]
    for write in writes[:3]:
        write.start()
    policy_ref[0, 0] = jnp.sum(recv_ref[:, 0:1])
    writes[3].start()
    for write in writes:
        write.wait()


VMEM = pl.BlockSpec(memory_space=pltpu.VMEM)
ANY = pl.BlockSpec(memory_space=pl.ANY)


def on_chip(x):
    return pltpu.with_memory_space_constraint(x, pltpu.VMEM)


def on_chip_shape(shape):
    return pltpu.VMEM(shape, jnp.float32)


def exchange(x, axis, groups):
    return lax.all_to_all(x, axis, 0, 0, axis_index_groups=groups, tiled=True)


def pair_groups(blocks, peers):
    groups = []
    for first in range(0, blocks, 2 * ALONG_Z):
        for block in range(first, first + ALONG_Z):
            members = [b * peers + i for b in (block, block + ALONG_Z) for i in range(peers)]
            groups.append([members[i] for i in order_from(2 * peers, PAIR_FIRST)])
    return groups


def run_head(
    peers,
    hidden,
    norm_gain,
    value_weight,
    done_flags,
    valid_mask,
    new_logprob,
    old_logprob,
    discount,
    trace_decay,
    bootstrap,
):
    rollouts, length, width = hidden.shape
    f32 = jnp.float32
    steps = length.bit_length() - 1
    return pl.pallas_call(
        head_kernel,
        out_shape=(
            on_chip_shape((peers * HEAD_ROWS, 128)),
            on_chip_shape((rollouts, length)),
            on_chip_shape((rollouts * steps, length)),
            on_chip_shape((rollouts * steps // 2, length)),
            on_chip_shape((rollouts, length)),
            on_chip_shape((rollouts, length)),
            on_chip_shape((rollouts, 128)),
            on_chip_shape((rollouts, 128)),
            on_chip_shape((1, length)),
            on_chip_shape((1, 128)),
        ),
        in_specs=[ANY] * 10,
        out_specs=(VMEM,) * 10,
        scratch_shapes=[
            pltpu.VMEM(hidden.shape, hidden.dtype),
            pltpu.VMEM((width // 128, 128), norm_gain.dtype),
            pltpu.VMEM((width // 128, 128), value_weight.dtype),
            pltpu.VMEM(done_flags.shape, done_flags.dtype),
            pltpu.VMEM(valid_mask.shape, valid_mask.dtype),
            pltpu.VMEM(new_logprob.shape, f32),
            pltpu.VMEM(old_logprob.shape, f32),
            pltpu.SMEM(discount.shape, f32),
            pltpu.SMEM(trace_decay.shape, f32),
            pltpu.SMEM(bootstrap.shape, f32),
            pltpu.VMEM((2, length, 3 * 128), jnp.bfloat16),
            pltpu.VMEM((rollouts, 3 * 128, 128), jnp.bfloat16),
            pltpu.VMEM((length, 128), f32),
            pltpu.SemaphoreType.DMA((rollouts + 9,)),
        ],
        name="head",
    )(
        norm_gain.reshape(-1, 128),
        value_weight.reshape(-1, 128),
        done_flags,
        valid_mask,
        new_logprob,
        old_logprob,
        discount,
        trace_decay,
        bootstrap,
        hidden,
    )


def shards(
    hidden,
    norm_gain,
    value_weight,
    rewards,
    done_flags,
    valid_mask,
    new_logprob,
    old_logprob,
    discount,
    trace_decay,
    bootstrap,
):
    rollouts, length, width = hidden.shape
    peers, blocks = lax.axis_size("tensor"), lax.axis_size("seq")
    sent, gate, chain, triple, coef, power, fixed, trace, ratio, start = run_head(
        peers,
        hidden,
        norm_gain,
        value_weight,
        done_flags,
        valid_mask,
        new_logprob,
        old_logprob,
        discount,
        trace_decay,
        bootstrap,
    )
    got = exchange(sent.reshape(peers, 1, HEAD_ROWS * 128), "tensor", [order_from(peers, TENSOR_FIRST)])
    values, own, sent = pl.pallas_call(
        partial(local_kernel, width * peers),
        out_shape=(
            on_chip_shape((1, length)),
            on_chip_shape((1, length)),
            on_chip_shape((blocks * TOKEN_ROWS, 128)),
        ),
        in_specs=[VMEM] * 9,
        out_specs=(VMEM,) * 3,
        name="local",
    )(
        *map(
            on_chip,
            (
                got.reshape(peers * HEAD_ROWS, 128),
                rewards,
                gate,
                chain,
                triple,
                coef,
                fixed,
                trace,
                ratio,
            ),
        )
    )
    got = exchange(sent.reshape(blocks, 1, TOKEN_ROWS * 128), "seq", [order_from(blocks, SEQ_FIRST)])
    white, loss, sent = pl.pallas_call(
        final_kernel,
        out_shape=(
            on_chip_shape((1, length)),
            on_chip_shape((1, length)),
            on_chip_shape((2 * peers, 128)),
        ),
        in_specs=[VMEM] * 5,
        out_specs=(VMEM, VMEM, VMEM),
        name="final",
    )(*map(on_chip, (got.reshape(blocks * TOKEN_ROWS, 128), power, start, own, ratio)))
    groups = pair_groups(blocks, peers)
    got = exchange(sent.reshape(2 * peers, 1, 128), ("seq", "tensor"), groups)
    own_row = jax.ShapeDtypeStruct((1, length), jnp.float32)
    values, white, loss, policy = pl.pallas_call(
        last_kernel,
        out_shape=(own_row, own_row, own_row, jax.ShapeDtypeStruct((1, 1), jnp.float32)),
        in_specs=[VMEM] * 4,
        out_specs=(ANY,) * 4,
        scratch_shapes=[pltpu.SMEM((1, 1), jnp.float32), pltpu.SemaphoreType.DMA((4,))],
        name="last",
    )(*map(on_chip, (values, white, loss, got.reshape(2 * peers, 128))))
    return values, white, loss, policy.reshape(())


def solution(mesh):
    in_specs = (
        P(None, "seq", "tensor"),
        P("tensor"),
        P("tensor"),
        P(None, "seq"),
        P(None, "seq"),
        P("tensor", "seq"),
        P("tensor", "seq"),
        P("tensor", "seq"),
        P(),
        P(),
        P(),
    )
    out_specs = (P("tensor", "seq"), P("tensor", "seq"), P("tensor", "seq"), P())
    return jax.shard_map(
        shards, mesh=mesh, in_specs=in_specs, out_specs=out_specs, check_vma=False
    )
```

```python
from functools import partial

import jax
import jax.numpy as jnp
from jax import lax
from jax.experimental import pallas as pl
from jax.experimental.pallas import tpu as pltpu
from jax.sharding import PartitionSpec as P

EPS_NORM = 1e-06
EPS_WHITE = 1e-08
CLIP = 0.2

HEAD_ROWS = 34
TOKEN_ROWS = 3
WIDTH = 16
OFFSET, SLOPE, COUNT, MEAN_L, MEAN_C, VAR_L, COV, VAR_C, LAST_DONE = range(9)

CHUNK = 64

ALONG_Z = 16
SEQ_FIRST, PAIR_FIRST = 41, 13
TENSOR_ORDER = [5, 4, 7, 6, 3, 2, 1, 0]


def column(ref, shape):
    row = lax.broadcasted_iota(jnp.int32, shape, 0)
    out = jnp.full(shape, ref[0], jnp.float32)
    for r in range(1, shape[0]):
        out = jnp.where(row == r, ref[r], out)
    return out


def lane_sum(x):
    return jnp.sum(x, axis=1, keepdims=True)


def head_kernel(
    gain_hbm,
    weight_hbm,
    done_hbm,
    mask_hbm,
    new_hbm,
    old_hbm,
    discount_hbm,
    trace_hbm,
    bootstrap_hbm,
    hidden_ref,
    out_ref,
    gate_ref,
    chain_ref,
    triple_ref,
    coef_ref,
    power_ref,
    fixed_ref,
    trace_ref,
    ratio_ref,
    start_ref,
    held,
    gain_ref,
    weight_ref,
    done_ref,
    mask_ref,
    new_ref,
    old_ref,
    discount_smem,
    trace_smem,
    bootstrap_smem,
    split_ref,
    pick_ref,
    sums_ref,
    arrived,
):
    rollouts, length, width = held.shape
    peers = out_ref.shape[0] // HEAD_ROWS
    small = [
        pltpu.make_async_copy(source, target, arrived.at[rollouts + i])
        for i, (source, target) in enumerate(
            (
                (gain_hbm, gain_ref),
                (weight_hbm, weight_ref),
                (done_hbm, done_ref),
                (mask_hbm, mask_ref),
                (new_hbm, new_ref),
                (old_hbm, old_ref),
                (discount_hbm, discount_smem),
                (trace_hbm, trace_smem),
                (bootstrap_hbm, bootstrap_smem),
            )
        )
    ]
    copies = [
        pltpu.make_async_copy(hidden_ref.at[r], held.at[r], arrived.at[r]) for r in range(rollouts)
    ]
    for copy in copies[:1] + small + copies[1:]:
        copy.start()
    picked = lax.broadcasted_iota(jnp.int32, (3 * 128, 128), 0) % 128 // 64 * 8
    picked = lax.broadcasted_iota(jnp.int32, (3 * 128, 128), 1) - picked
    for r in range(rollouts):
        pick_ref[r] = jnp.where(picked == r, 1.0, 0.0).astype(jnp.bfloat16)
    for copy in small:
        copy.wait()

    scaled = gain_ref[...].astype(jnp.float32) * weight_ref[...].astype(jnp.float32)
    small_lane = lax.broadcasted_iota(jnp.int32, (8, 128), 1)

    def partial_sums(r, here):
        squares = products = jnp.zeros((CHUNK, 128), jnp.float32)
        for j in range(width // 128):
            wide = held[r, here, 128 * j : 128 * (j + 1)].astype(jnp.float32)
            squares = squares + wide * wide
            products = products + wide * scaled[j : j + 1, :]
        left = small_lane[0:1] < 64
        rest = jnp.where(left, squares, products)
        rest = rest + pltpu.roll(jnp.where(left, products, squares), 64, 1)
        for part in range(3):
            coarse = rest.astype(jnp.bfloat16)
            split_ref[r % 2, here, 128 * part : 128 * (part + 1)] = coarse
            rest = rest - coarse.astype(jnp.float32)

    def lane_sums(r):
        sums = jnp.dot(split_ref[r % 2], pick_ref[r], preferred_element_type=jnp.float32)
        sums_ref[...] = sums_ref[...] + sums if r else sums

    def finish():
        for half in range(length // 128):
            turned = jnp.transpose(sums_ref[128 * half : 128 * (half + 1), :])
            for peer in range(peers):
                for kind in range(2):
                    at = HEAD_ROWS * peer + 8 * (2 * kind + half)
                    out_ref[at : at + 8, :] = turned[8 * kind : 8 * (kind + 1)]

    shape = (rollouts, length)
    lane = lax.broadcasted_iota(jnp.int32, shape, 1)

    def piece_own():
        mask = mask_ref[...].astype(jnp.float32)
        ratio_ref[...] = mask * jnp.exp(new_ref[...] - old_ref[...])
        for peer in range(peers):
            at = HEAD_ROWS * peer + 32
            out_ref[at : at + 1, :] = mask[:, :128]
            out_ref[at + 1 : at + 2, :] = mask[:, 128:]
        start_lane = lax.broadcasted_iota(jnp.int32, (1, 128), 1)
        start = jnp.full((1, 128), bootstrap_smem[0], jnp.float32)
        for r in range(1, rollouts):
            start = jnp.where(start_lane == WIDTH * r, bootstrap_smem[r], start)
        start_ref[...] = start

    def piece_chain_start():
        discount, trace = column(discount_smem, shape), column(trace_smem, shape)
        alive = 1.0 - done_ref[...].astype(jnp.float32)
        gate_ref[...] = discount * alive
        chain_ref[0:rollouts, :] = discount * trace * alive
        trace_ref[...] = trace[:, :128]
        last_done = jnp.where(alive > 0.5, -1.0, lane.astype(jnp.float32))
        last_done = jnp.max(last_done, axis=1, keepdims=True)
        fixed_ref[...] = jnp.where(small_lane == LAST_DONE, last_done, 0.0)

    def piece_chain(at):
        step = 1 << at
        chain = chain_ref[rollouts * at : rollouts * (at + 1), :]
        later = pltpu.roll(chain, length - step, 1)
        chain = chain * jnp.where(lane < length - step, later, 1.0)
        if 2 * step < length:
            chain_ref[rollouts * (at + 1) : rollouts * (at + 2), :] = chain
            return
        coef_ref[...] = chain / column(trace_smem, shape)
        fixed_ref[...] = jnp.where(small_lane == SLOPE, chain[:, 0:1], fixed_ref[...])

    def piece_triple(at):
        step = 1 << at
        chain = chain_ref[rollouts * at : rollouts * (at + 1), :]
        later = pltpu.roll(chain, length - 2 * step, 1)
        triple = chain_ref[rollouts * (at + 1) : rollouts * (at + 2), :] * later
        triple_ref[rollouts * (at // 2) : rollouts * (at // 2 + 1), :] = triple

    def piece_power():
        discount = column(discount_smem, shape)
        left = length - 1 - lane
        power, factor, bit = discount, discount * column(trace_smem, shape), 1
        while bit < length:
            power = jnp.where(left & bit != 0, power * factor, power)
            factor = factor * factor
            bit *= 2
        power_ref[...] = power

    steps = length.bit_length() - 1
    pieces = [[] for _ in range(rollouts)]
    pieces[0] = [piece_chain_start]
    for at in range(steps):
        pieces[1 + at * (rollouts - 2) // steps].append(partial(piece_chain, at))
    for at in range(0, steps, 2):
        pieces[rollouts - 1].append(partial(piece_triple, at))
    pieces[0].append(piece_own)
    pieces[rollouts - 2].append(piece_power)

    for r in range(rollouts):
        copies[r].wait()
        for piece in pieces[r]:
            piece()
        if r:
            lane_sums(r - 1)
        for first in range(0, length, CHUNK):
            partial_sums(r, slice(first, first + CHUNK))
    lane_sums(rollouts - 1)
    finish()


def local_kernel(
    hidden_width,
    recv_ref,
    rewards_ref,
    gate_ref,
    chain_ref,
    triple_ref,
    coef_ref,
    fixed_ref,
    trace_ref,
    ratio_ref,
    values_ref,
    own_ref,
    out_ref,
):
    me = lax.axis_index("tensor")
    rollouts, length = rewards_ref.shape
    peers = recv_ref.shape[0] // HEAD_ROWS
    shape = (rollouts, length)
    total = recv_ref[0:32, :]
    for peer in range(1, peers):
        total = total + recv_ref[HEAD_ROWS * peer : HEAD_ROWS * peer + 32, :]
    squares = jnp.concatenate([total[0:8], total[8:16]], axis=1)
    products = jnp.concatenate([total[16:24], total[24:32]], axis=1)
    weight = jnp.concatenate(
        [
            recv_ref[pl.ds(32, peers, stride=HEAD_ROWS), :],
            recv_ref[pl.ds(33, peers, stride=HEAD_ROWS), :],
        ],
        axis=1,
    )
    member_row = lax.broadcasted_iota(jnp.int32, shape, 0)
    received, weight = weight, jnp.zeros(shape, jnp.float32)
    for slot, member in enumerate(TENSOR_ORDER):
        weight = jnp.where(member_row == member, received[slot : slot + 1], weight)
    values = products * lax.rsqrt(squares / hidden_width + EPS_NORM)
    lane = lax.broadcasted_iota(jnp.int32, shape, 1)
    inner_next = jnp.where(lane < length - 1, pltpu.roll(values, length - 1, 1), 0.0)
    local = rewards_ref[...] + gate_ref[...] * inner_next - values
    step, at = 1, 0
    while step < length:
        factors = (
            chain_ref[rollouts * at : rollouts * (at + 1), :],
            chain_ref[rollouts * (at + 1) : rollouts * (at + 2), :],
            triple_ref[rollouts * (at // 2) : rollouts * (at // 2 + 1), :],
        )
        later = [
            factor * jnp.where(lane < length - k * step, pltpu.roll(local, length - k * step, 1), 0.0)
            for k, factor in enumerate(factors, 1)
        ]
        local = (local + later[0]) + (later[1] + later[2])
        step, at = 4 * step, at + 2
    coef = coef_ref[...]
    count = lane_sum(weight)
    safe = 1.0 / jnp.maximum(count, 1.0)
    mean_l = lane_sum(weight * local) * safe
    mean_c = lane_sum(weight * coef) * safe
    off_l = weight * (local - mean_l)
    off_c = weight * (coef - mean_c)
    stats = {
        OFFSET: values[:, 0:1] + trace_ref[:, 0:1] * local[:, 0:1],
        COUNT: count,
        MEAN_L: mean_l,
        MEAN_C: mean_c,
        VAR_L: lane_sum(off_l * off_l),
        COV: lane_sum(off_l * off_c),
        VAR_C: lane_sum(off_c * off_c),
    }
    small_lane = lax.broadcasted_iota(jnp.int32, (rollouts, 128), 1)
    summary = fixed_ref[...]
    for at, stat in stats.items():
        summary = jnp.where(small_lane == at, stat, summary)
    summary = pltpu.roll(summary, 0, 1, stride=WIDTH, stride_axis=0)
    summary = jnp.sum(summary, axis=0, keepdims=True)
    mine = lax.broadcasted_iota(jnp.int32, shape, 0) == me
    own_local = jnp.sum(jnp.where(mine, local, 0.0), axis=0, keepdims=True)
    values_ref[...] = jnp.sum(jnp.where(mine, values, 0.0), axis=0, keepdims=True)
    row = lax.broadcasted_iota(jnp.int32, (8, 128), 0)
    own_ref[...] = own_local
    messages = []
    for half in range(2):
        lanes = slice(128 * half, 128 * (half + 1))
        message = jnp.where(row == 1, own_local[:, lanes], ratio_ref[:, lanes])
        messages.append(jnp.where(row == 0, summary, message)[0:TOKEN_ROWS])
    blocks = out_ref.shape[0] // TOKEN_ROWS
    for slot, member in enumerate(order_from(blocks, SEQ_FIRST)):
        half = member // ALONG_Z % 2
        out_ref[TOKEN_ROWS * slot : TOKEN_ROWS * (slot + 1), :] = messages[half]


def order_from(size, first):
    order = list(range(size))
    order[0], order[first] = order[first], order[0]
    return order


def in_order(rows, first):
    row = lax.broadcasted_iota(jnp.int32, rows.shape, 0)
    swapped = jnp.where(row == 0, rows[first : first + 1], rows)
    return jnp.where(row == first, rows[0:1], swapped)


def from_blocks(ref, at):
    blocks = ref.shape[0] // TOKEN_ROWS
    return in_order(ref[pl.ds(at, blocks, stride=TOKEN_ROWS), :], SEQ_FIRST)


def full_sum(x):
    return jnp.sum(jnp.sum(x, axis=0, keepdims=True), axis=1, keepdims=True)


def final_kernel(
    recv_ref, power_ref, start_ref, own_ref, ratio_ref, white_ref, loss_ref, out_ref
):
    tensor, seq = lax.axis_index("tensor"), lax.axis_index("seq")
    blocks = recv_ref.shape[0] // TOKEN_ROWS
    rollouts = power_ref.shape[0]
    shape = (blocks, 128)
    table = from_blocks(recv_ref, 0)
    row = lax.broadcasted_iota(jnp.int32, shape, 0)
    lane = lax.broadcasted_iota(jnp.int32, shape, 1)

    def stat(at):
        return pltpu.roll(table, 128 - at, 1)

    last = row == blocks - 1
    offset = jnp.where(last, start_ref[...], pltpu.roll(table, blocks - 1, 0))
    slope = jnp.where(last, 0.0, pltpu.roll(stat(SLOPE), blocks - 1, 0))
    step = 1
    while step < blocks:
        inside = row < blocks - step
        offset_later = jnp.where(inside, pltpu.roll(offset, blocks - step, 0), 0.0)
        slope_later = jnp.where(inside, pltpu.roll(slope, blocks - step, 0), 0.0)
        offset = offset + slope * offset_later
        slope = slope * slope_later
        step *= 2
    entering = offset
    used = (lane % WIDTH == 0) & (lane < WIDTH * rollouts)
    members = jnp.where(used, stat(COUNT), 0.0)
    block_mean = jnp.where(used, stat(MEAN_L) + entering * stat(MEAN_C), 0.0)
    count = full_sum(members)
    mean = full_sum(members * block_mean) / count
    within = stat(VAR_L) + entering * (2.0 * stat(COV) + entering * stat(VAR_C))
    apart = block_mean - mean
    variance = full_sum(jnp.where(used, within, 0.0) + members * apart * apart) / count
    scale = lax.rsqrt(variance + EPS_WHITE)

    mine = lane == WIDTH * tensor
    own_entering = lane_sum(jnp.where(mine, entering, 0.0))
    own_done = lane_sum(jnp.where(mine, stat(LAST_DONE), 0.0))
    power = power_ref[pl.ds(tensor, 1), :]

    def losses(local, ratio, coef, from_later):
        white = (local + coef * from_later - mean) * scale
        clipped = jnp.clip(ratio, 1.0 - CLIP, 1.0 + CLIP)
        return white, jnp.where(ratio > 0.0, -jnp.minimum(ratio * white, clipped * white), 0.0)

    half = seq // ALONG_Z % 2
    power_half = jnp.where(half == 0, power[:, :128], power[:, 128:])
    coef = jnp.where((lane + 128 * half).astype(jnp.float32) > own_done, power_half, 0.0)
    _, token = losses(from_blocks(recv_ref, 1), from_blocks(recv_ref, 2), coef, own_entering)
    out_ref[...] = jnp.broadcast_to(full_sum(token) / count, out_ref.shape)

    here = row[:, 0:1] == seq
    position = lax.broadcasted_iota(jnp.int32, power.shape, 1).astype(jnp.float32)
    own_done = jnp.sum(jnp.where(here, own_done, 0.0), axis=0, keepdims=True)
    own_entering = jnp.sum(jnp.where(here, own_entering, 0.0), axis=0, keepdims=True)
    coef = jnp.where(position > own_done, power, 0.0)
    white_ref[...], loss_ref[...] = losses(own_ref[...], ratio_ref[...], coef, own_entering)


def last_kernel(
    values_ref,
    white_ref,
    loss_ref,
    recv_ref,
    values_hbm,
    white_hbm,
    loss_hbm,
    policy_hbm,
    policy_ref,
    sent,
):
    writes = [
        pltpu.make_async_copy(source, target, sent.at[i])
        for i, (source, target) in enumerate(
            (
                (values_ref, values_hbm),
                (white_ref, white_hbm),
                (loss_ref, loss_hbm),
                (policy_ref, policy_hbm),
            )
        )
    ]
    for write in writes[:3]:
        write.start()
    policy_ref[0, 0] = jnp.sum(recv_ref[:, 0:1])
    writes[3].start()
    for write in writes:
        write.wait()


VMEM = pl.BlockSpec(memory_space=pltpu.VMEM)
ANY = pl.BlockSpec(memory_space=pl.ANY)


def on_chip(x):
    return pltpu.with_memory_space_constraint(x, pltpu.VMEM)


def on_chip_shape(shape):
    return pltpu.VMEM(shape, jnp.float32)


def exchange(x, axis, groups):
    return lax.all_to_all(x, axis, 0, 0, axis_index_groups=groups, tiled=True)


def pair_groups(blocks, peers):
    groups = []
    for first in range(0, blocks, 2 * ALONG_Z):
        for block in range(first, first + ALONG_Z):
            members = [b * peers + i for b in (block, block + ALONG_Z) for i in range(peers)]
            groups.append([members[i] for i in order_from(2 * peers, PAIR_FIRST)])
    return groups


def run_head(
    peers,
    hidden,
    norm_gain,
    value_weight,
    done_flags,
    valid_mask,
    new_logprob,
    old_logprob,
    discount,
    trace_decay,
    bootstrap,
):
    rollouts, length, width = hidden.shape
    f32 = jnp.float32
    steps = length.bit_length() - 1
    return pl.pallas_call(
        head_kernel,
        out_shape=(
            on_chip_shape((peers * HEAD_ROWS, 128)),
            on_chip_shape((rollouts, length)),
            on_chip_shape((rollouts * steps, length)),
            on_chip_shape((rollouts * steps // 2, length)),
            on_chip_shape((rollouts, length)),
            on_chip_shape((rollouts, length)),
            on_chip_shape((rollouts, 128)),
            on_chip_shape((rollouts, 128)),
            on_chip_shape((1, length)),
            on_chip_shape((1, 128)),
        ),
        in_specs=[ANY] * 10,
        out_specs=(VMEM,) * 10,
        scratch_shapes=[
            pltpu.VMEM(hidden.shape, hidden.dtype),
            pltpu.VMEM((width // 128, 128), norm_gain.dtype),
            pltpu.VMEM((width // 128, 128), value_weight.dtype),
            pltpu.VMEM(done_flags.shape, done_flags.dtype),
            pltpu.VMEM(valid_mask.shape, valid_mask.dtype),
            pltpu.VMEM(new_logprob.shape, f32),
            pltpu.VMEM(old_logprob.shape, f32),
            pltpu.SMEM(discount.shape, f32),
            pltpu.SMEM(trace_decay.shape, f32),
            pltpu.SMEM(bootstrap.shape, f32),
            pltpu.VMEM((2, length, 3 * 128), jnp.bfloat16),
            pltpu.VMEM((rollouts, 3 * 128, 128), jnp.bfloat16),
            pltpu.VMEM((length, 128), f32),
            pltpu.SemaphoreType.DMA((rollouts + 9,)),
        ],
        name="head",
    )(
        norm_gain.reshape(-1, 128),
        value_weight.reshape(-1, 128),
        done_flags,
        valid_mask,
        new_logprob,
        old_logprob,
        discount,
        trace_decay,
        bootstrap,
        hidden,
    )


def shards(
    hidden,
    norm_gain,
    value_weight,
    rewards,
    done_flags,
    valid_mask,
    new_logprob,
    old_logprob,
    discount,
    trace_decay,
    bootstrap,
):
    rollouts, length, width = hidden.shape
    peers, blocks = lax.axis_size("tensor"), lax.axis_size("seq")
    sent, gate, chain, triple, coef, power, fixed, trace, ratio, start = run_head(
        peers,
        hidden,
        norm_gain,
        value_weight,
        done_flags,
        valid_mask,
        new_logprob,
        old_logprob,
        discount,
        trace_decay,
        bootstrap,
    )
    got = exchange(sent.reshape(peers, 1, HEAD_ROWS * 128), "tensor", [TENSOR_ORDER])
    values, own, sent = pl.pallas_call(
        partial(local_kernel, width * peers),
        out_shape=(
            on_chip_shape((1, length)),
            on_chip_shape((1, length)),
            on_chip_shape((blocks * TOKEN_ROWS, 128)),
        ),
        in_specs=[VMEM] * 9,
        out_specs=(VMEM,) * 3,
        name="local",
    )(
        *map(
            on_chip,
            (
                got.reshape(peers * HEAD_ROWS, 128),
                rewards,
                gate,
                chain,
                triple,
                coef,
                fixed,
                trace,
                ratio,
            ),
        )
    )
    got = exchange(sent.reshape(blocks, 1, TOKEN_ROWS * 128), "seq", [order_from(blocks, SEQ_FIRST)])
    white, loss, sent = pl.pallas_call(
        final_kernel,
        out_shape=(
            on_chip_shape((1, length)),
            on_chip_shape((1, length)),
            on_chip_shape((2 * peers, 128)),
        ),
        in_specs=[VMEM] * 5,
        out_specs=(VMEM, VMEM, VMEM),
        name="final",
    )(*map(on_chip, (got.reshape(blocks * TOKEN_ROWS, 128), power, start, own, ratio)))
    groups = pair_groups(blocks, peers)
    got = exchange(sent.reshape(2 * peers, 1, 128), ("seq", "tensor"), groups)
    own_row = jax.ShapeDtypeStruct((1, length), jnp.float32)
    values, white, loss, policy = pl.pallas_call(
        last_kernel,
        out_shape=(own_row, own_row, own_row, jax.ShapeDtypeStruct((1, 1), jnp.float32)),
        in_specs=[VMEM] * 4,
        out_specs=(ANY,) * 4,
        scratch_shapes=[pltpu.SMEM((1, 1), jnp.float32), pltpu.SemaphoreType.DMA((4,))],
        name="last",
    )(*map(on_chip, (values, white, loss, got.reshape(2 * peers, 128))))
    return values, white, loss, policy.reshape(())


def solution(mesh):
    in_specs = (
        P(None, "seq", "tensor"),
        P("tensor"),
        P("tensor"),
        P(None, "seq"),
        P(None, "seq"),
        P("tensor", "seq"),
        P("tensor", "seq"),
        P("tensor", "seq"),
        P(),
        P(),
        P(),
    )
    out_specs = (P("tensor", "seq"), P("tensor", "seq"), P("tensor", "seq"), P())
    return jax.shard_map(
        shards, mesh=mesh, in_specs=in_specs, out_specs=out_specs, check_vma=False
    )
```

```python
from functools import partial

import jax
import jax.numpy as jnp
from jax import lax
from jax.experimental import pallas as pl
from jax.experimental.pallas import tpu as pltpu
from jax.sharding import PartitionSpec as P

EPS_NORM = 1e-06
EPS_WHITE = 1e-08
CLIP = 0.2

HEAD_ROWS = 34
TOKEN_ROWS = 3
WIDTH = 16
OFFSET, SLOPE, COUNT, MEAN_L, MEAN_C, VAR_L, COV, VAR_C, LAST_DONE = range(9)

CHUNK = 64

ALONG_Z = 16
SEQ_FIRST = 41
PAIR_ORDER = [13, 12, 15, 14, 11, 10, 9, 8, 5, 4, 7, 6, 3, 2, 1, 0]
TENSOR_ORDER = [5, 4, 7, 6, 3, 2, 1, 0]


def column(ref, shape):
    row = lax.broadcasted_iota(jnp.int32, shape, 0)
    out = jnp.full(shape, ref[0], jnp.float32)
    for r in range(1, shape[0]):
        out = jnp.where(row == r, ref[r], out)
    return out


def lane_sum(x):
    return jnp.sum(x, axis=1, keepdims=True)


def head_kernel(
    gain_hbm,
    weight_hbm,
    done_hbm,
    mask_hbm,
    new_hbm,
    old_hbm,
    discount_hbm,
    trace_hbm,
    bootstrap_hbm,
    hidden_ref,
    out_ref,
    gate_ref,
    chain_ref,
    triple_ref,
    coef_ref,
    power_ref,
    fixed_ref,
    trace_ref,
    ratio_ref,
    start_ref,
    held,
    gain_ref,
    weight_ref,
    done_ref,
    mask_ref,
    new_ref,
    old_ref,
    discount_smem,
    trace_smem,
    bootstrap_smem,
    split_ref,
    pick_ref,
    sums_ref,
    arrived,
):
    rollouts, length, width = held.shape
    peers = out_ref.shape[0] // HEAD_ROWS
    small = [
        pltpu.make_async_copy(source, target, arrived.at[rollouts + i])
        for i, (source, target) in enumerate(
            (
                (gain_hbm, gain_ref),
                (weight_hbm, weight_ref),
                (done_hbm, done_ref),
                (mask_hbm, mask_ref),
                (new_hbm, new_ref),
                (old_hbm, old_ref),
                (discount_hbm, discount_smem),
                (trace_hbm, trace_smem),
                (bootstrap_hbm, bootstrap_smem),
            )
        )
    ]
    copies = [
        pltpu.make_async_copy(hidden_ref.at[r], held.at[r], arrived.at[r]) for r in range(rollouts)
    ]
    for copy in copies[:1] + small + copies[1:]:
        copy.start()
    picked = lax.broadcasted_iota(jnp.int32, (3 * 128, 128), 0) % 128 // 64 * 8
    picked = lax.broadcasted_iota(jnp.int32, (3 * 128, 128), 1) - picked
    for r in range(rollouts):
        pick_ref[r] = jnp.where(picked == r, 1.0, 0.0).astype(jnp.bfloat16)
    for copy in small:
        copy.wait()

    scaled = gain_ref[...].astype(jnp.float32) * weight_ref[...].astype(jnp.float32)
    small_lane = lax.broadcasted_iota(jnp.int32, (8, 128), 1)

    def partial_sums(r, here):
        squares = products = jnp.zeros((CHUNK, 128), jnp.float32)
        for j in range(width // 128):
            wide = held[r, here, 128 * j : 128 * (j + 1)].astype(jnp.float32)
            squares = squares + wide * wide
            products = products + wide * scaled[j : j + 1, :]
        left = small_lane[0:1] < 64
        rest = jnp.where(left, squares, products)
        rest = rest + pltpu.roll(jnp.where(left, products, squares), 64, 1)
        for part in range(3):
            coarse = rest.astype(jnp.bfloat16)
            split_ref[r % 2, here, 128 * part : 128 * (part + 1)] = coarse
            rest = rest - coarse.astype(jnp.float32)

    def lane_sums(r):
        sums = jnp.dot(split_ref[r % 2], pick_ref[r], preferred_element_type=jnp.float32)
        sums_ref[...] = sums_ref[...] + sums if r else sums

    def finish():
        for half in range(length // 128):
            turned = jnp.transpose(sums_ref[128 * half : 128 * (half + 1), :])
            for peer in range(peers):
                for kind in range(2):
                    at = HEAD_ROWS * peer + 8 * (2 * kind + half)
                    out_ref[at : at + 8, :] = turned[8 * kind : 8 * (kind + 1)]

    shape = (rollouts, length)
    lane = lax.broadcasted_iota(jnp.int32, shape, 1)

    def piece_own():
        mask = mask_ref[...].astype(jnp.float32)
        ratio_ref[...] = mask * jnp.exp(new_ref[...] - old_ref[...])
        for peer in range(peers):
            at = HEAD_ROWS * peer + 32
            out_ref[at : at + 1, :] = mask[:, :128]
            out_ref[at + 1 : at + 2, :] = mask[:, 128:]
        start_lane = lax.broadcasted_iota(jnp.int32, (1, 128), 1)
        start = jnp.full((1, 128), bootstrap_smem[0], jnp.float32)
        for r in range(1, rollouts):
            start = jnp.where(start_lane == WIDTH * r, bootstrap_smem[r], start)
        start_ref[...] = start

    def piece_chain_start():
        discount, trace = column(discount_smem, shape), column(trace_smem, shape)
        alive = 1.0 - done_ref[...].astype(jnp.float32)
        gate_ref[...] = discount * alive
        chain_ref[0:rollouts, :] = discount * trace * alive
        trace_ref[...] = trace[:, :128]
        last_done = jnp.where(alive > 0.5, -1.0, lane.astype(jnp.float32))
        last_done = jnp.max(last_done, axis=1, keepdims=True)
        fixed_ref[...] = jnp.where(small_lane == LAST_DONE, last_done, 0.0)

    def piece_chain(at):
        step = 1 << at
        chain = chain_ref[rollouts * at : rollouts * (at + 1), :]
        later = pltpu.roll(chain, length - step, 1)
        chain = chain * jnp.where(lane < length - step, later, 1.0)
        if 2 * step < length:
            chain_ref[rollouts * (at + 1) : rollouts * (at + 2), :] = chain
            return
        coef_ref[...] = chain / column(trace_smem, shape)
        fixed_ref[...] = jnp.where(small_lane == SLOPE, chain[:, 0:1], fixed_ref[...])

    def piece_triple(at):
        step = 1 << at
        chain = chain_ref[rollouts * at : rollouts * (at + 1), :]
        later = pltpu.roll(chain, length - 2 * step, 1)
        triple = chain_ref[rollouts * (at + 1) : rollouts * (at + 2), :] * later
        triple_ref[rollouts * (at // 2) : rollouts * (at // 2 + 1), :] = triple

    def piece_power():
        discount = column(discount_smem, shape)
        left = length - 1 - lane
        power, factor, bit = discount, discount * column(trace_smem, shape), 1
        while bit < length:
            power = jnp.where(left & bit != 0, power * factor, power)
            factor = factor * factor
            bit *= 2
        power_ref[...] = power

    steps = length.bit_length() - 1
    pieces = [[] for _ in range(rollouts)]
    pieces[0] = [piece_chain_start]
    for at in range(steps):
        pieces[1 + at * (rollouts - 2) // steps].append(partial(piece_chain, at))
    for at in range(0, steps, 2):
        pieces[rollouts - 1].append(partial(piece_triple, at))
    pieces[0].append(piece_own)
    pieces[rollouts - 2].append(piece_power)

    for r in range(rollouts):
        copies[r].wait()
        for piece in pieces[r]:
            piece()
        if r:
            lane_sums(r - 1)
        for first in range(0, length, CHUNK):
            partial_sums(r, slice(first, first + CHUNK))
    lane_sums(rollouts - 1)
    finish()


def local_kernel(
    hidden_width,
    recv_ref,
    rewards_ref,
    gate_ref,
    chain_ref,
    triple_ref,
    coef_ref,
    fixed_ref,
    trace_ref,
    ratio_ref,
    values_ref,
    own_ref,
    out_ref,
):
    me = lax.axis_index("tensor")
    rollouts, length = rewards_ref.shape
    peers = recv_ref.shape[0] // HEAD_ROWS
    shape = (rollouts, length)
    total = recv_ref[0:32, :]
    for peer in range(1, peers):
        total = total + recv_ref[HEAD_ROWS * peer : HEAD_ROWS * peer + 32, :]
    squares = jnp.concatenate([total[0:8], total[8:16]], axis=1)
    products = jnp.concatenate([total[16:24], total[24:32]], axis=1)
    weight = jnp.concatenate(
        [
            recv_ref[pl.ds(32, peers, stride=HEAD_ROWS), :],
            recv_ref[pl.ds(33, peers, stride=HEAD_ROWS), :],
        ],
        axis=1,
    )
    member_row = lax.broadcasted_iota(jnp.int32, shape, 0)
    received, weight = weight, jnp.zeros(shape, jnp.float32)
    for slot, member in enumerate(TENSOR_ORDER):
        weight = jnp.where(member_row == member, received[slot : slot + 1], weight)
    values = products * lax.rsqrt(squares / hidden_width + EPS_NORM)
    lane = lax.broadcasted_iota(jnp.int32, shape, 1)
    inner_next = jnp.where(lane < length - 1, pltpu.roll(values, length - 1, 1), 0.0)
    local = rewards_ref[...] + gate_ref[...] * inner_next - values
    step, at = 1, 0
    while step < length:
        factors = (
            chain_ref[rollouts * at : rollouts * (at + 1), :],
            chain_ref[rollouts * (at + 1) : rollouts * (at + 2), :],
            triple_ref[rollouts * (at // 2) : rollouts * (at // 2 + 1), :],
        )
        later = [
            factor * jnp.where(lane < length - k * step, pltpu.roll(local, length - k * step, 1), 0.0)
            for k, factor in enumerate(factors, 1)
        ]
        local = (local + later[0]) + (later[1] + later[2])
        step, at = 4 * step, at + 2
    coef = coef_ref[...]
    count = lane_sum(weight)
    safe = 1.0 / jnp.maximum(count, 1.0)
    mean_l = lane_sum(weight * local) * safe
    mean_c = lane_sum(weight * coef) * safe
    off_l = weight * (local - mean_l)
    off_c = weight * (coef - mean_c)
    stats = {
        OFFSET: values[:, 0:1] + trace_ref[:, 0:1] * local[:, 0:1],
        COUNT: count,
        MEAN_L: mean_l,
        MEAN_C: mean_c,
        VAR_L: lane_sum(off_l * off_l),
        COV: lane_sum(off_l * off_c),
        VAR_C: lane_sum(off_c * off_c),
    }
    small_lane = lax.broadcasted_iota(jnp.int32, (rollouts, 128), 1)
    summary = fixed_ref[...]
    for at, stat in stats.items():
        summary = jnp.where(small_lane == at, stat, summary)
    summary = pltpu.roll(summary, 0, 1, stride=WIDTH, stride_axis=0)
    summary = jnp.sum(summary, axis=0, keepdims=True)
    mine = lax.broadcasted_iota(jnp.int32, shape, 0) == me
    own_local = jnp.sum(jnp.where(mine, local, 0.0), axis=0, keepdims=True)
    values_ref[...] = jnp.sum(jnp.where(mine, values, 0.0), axis=0, keepdims=True)
    row = lax.broadcasted_iota(jnp.int32, (8, 128), 0)
    own_ref[...] = own_local
    messages = []
    for half in range(2):
        lanes = slice(128 * half, 128 * (half + 1))
        message = jnp.where(row == 1, own_local[:, lanes], ratio_ref[:, lanes])
        messages.append(jnp.where(row == 0, summary, message)[0:TOKEN_ROWS])
    blocks = out_ref.shape[0] // TOKEN_ROWS
    for slot, member in enumerate(order_from(blocks, SEQ_FIRST)):
        half = member // ALONG_Z % 2
        out_ref[TOKEN_ROWS * slot : TOKEN_ROWS * (slot + 1), :] = messages[half]


def order_from(size, first):
    order = list(range(size))
    order[0], order[first] = order[first], order[0]
    return order


def in_order(rows, first):
    row = lax.broadcasted_iota(jnp.int32, rows.shape, 0)
    swapped = jnp.where(row == 0, rows[first : first + 1], rows)
    return jnp.where(row == first, rows[0:1], swapped)


def from_blocks(ref, at):
    blocks = ref.shape[0] // TOKEN_ROWS
    return in_order(ref[pl.ds(at, blocks, stride=TOKEN_ROWS), :], SEQ_FIRST)


def full_sum(x):
    return jnp.sum(jnp.sum(x, axis=0, keepdims=True), axis=1, keepdims=True)


def final_kernel(
    recv_ref, power_ref, start_ref, own_ref, ratio_ref, white_ref, loss_ref, out_ref
):
    tensor, seq = lax.axis_index("tensor"), lax.axis_index("seq")
    blocks = recv_ref.shape[0] // TOKEN_ROWS
    rollouts = power_ref.shape[0]
    shape = (blocks, 128)
    table = from_blocks(recv_ref, 0)
    row = lax.broadcasted_iota(jnp.int32, shape, 0)
    lane = lax.broadcasted_iota(jnp.int32, shape, 1)

    def stat(at):
        return pltpu.roll(table, 128 - at, 1)

    last = row == blocks - 1
    offset = jnp.where(last, start_ref[...], pltpu.roll(table, blocks - 1, 0))
    slope = jnp.where(last, 0.0, pltpu.roll(stat(SLOPE), blocks - 1, 0))
    step = 1
    while step < blocks:
        inside = row < blocks - step
        offset_later = jnp.where(inside, pltpu.roll(offset, blocks - step, 0), 0.0)
        slope_later = jnp.where(inside, pltpu.roll(slope, blocks - step, 0), 0.0)
        offset = offset + slope * offset_later
        slope = slope * slope_later
        step *= 2
    entering = offset
    used = (lane % WIDTH == 0) & (lane < WIDTH * rollouts)
    members = jnp.where(used, stat(COUNT), 0.0)
    block_mean = jnp.where(used, stat(MEAN_L) + entering * stat(MEAN_C), 0.0)
    count = full_sum(members)
    mean = full_sum(members * block_mean) / count
    within = stat(VAR_L) + entering * (2.0 * stat(COV) + entering * stat(VAR_C))
    apart = block_mean - mean
    variance = full_sum(jnp.where(used, within, 0.0) + members * apart * apart) / count
    scale = lax.rsqrt(variance + EPS_WHITE)

    mine = lane == WIDTH * tensor
    own_entering = lane_sum(jnp.where(mine, entering, 0.0))
    own_done = lane_sum(jnp.where(mine, stat(LAST_DONE), 0.0))
    power = power_ref[pl.ds(tensor, 1), :]

    def losses(local, ratio, coef, from_later):
        white = (local + coef * from_later - mean) * scale
        clipped = jnp.clip(ratio, 1.0 - CLIP, 1.0 + CLIP)
        return white, jnp.where(ratio > 0.0, -jnp.minimum(ratio * white, clipped * white), 0.0)

    half = seq // ALONG_Z % 2
    power_half = jnp.where(half == 0, power[:, :128], power[:, 128:])
    coef = jnp.where((lane + 128 * half).astype(jnp.float32) > own_done, power_half, 0.0)
    _, token = losses(from_blocks(recv_ref, 1), from_blocks(recv_ref, 2), coef, own_entering)
    out_ref[...] = jnp.broadcast_to(full_sum(token) / count, out_ref.shape)

    here = row[:, 0:1] == seq
    position = lax.broadcasted_iota(jnp.int32, power.shape, 1).astype(jnp.float32)
    own_done = jnp.sum(jnp.where(here, own_done, 0.0), axis=0, keepdims=True)
    own_entering = jnp.sum(jnp.where(here, own_entering, 0.0), axis=0, keepdims=True)
    coef = jnp.where(position > own_done, power, 0.0)
    white_ref[...], loss_ref[...] = losses(own_ref[...], ratio_ref[...], coef, own_entering)


def last_kernel(
    values_ref,
    white_ref,
    loss_ref,
    recv_ref,
    values_hbm,
    white_hbm,
    loss_hbm,
    policy_hbm,
    policy_ref,
    sent,
):
    writes = [
        pltpu.make_async_copy(source, target, sent.at[i])
        for i, (source, target) in enumerate(
            (
                (values_ref, values_hbm),
                (white_ref, white_hbm),
                (loss_ref, loss_hbm),
                (policy_ref, policy_hbm),
            )
        )
    ]
    for write in writes[:3]:
        write.start()
    policy_ref[0, 0] = jnp.sum(recv_ref[:, 0:1])
    writes[3].start()
    for write in writes:
        write.wait()


VMEM = pl.BlockSpec(memory_space=pltpu.VMEM)
ANY = pl.BlockSpec(memory_space=pl.ANY)


def on_chip(x):
    return pltpu.with_memory_space_constraint(x, pltpu.VMEM)


def on_chip_shape(shape):
    return pltpu.VMEM(shape, jnp.float32)


def exchange(x, axis, groups):
    return lax.all_to_all(x, axis, 0, 0, axis_index_groups=groups, tiled=True)


def pair_groups(blocks, peers):
    groups = []
    for first in range(0, blocks, 2 * ALONG_Z):
        for block in range(first, first + ALONG_Z):
            members = [b * peers + i for b in (block, block + ALONG_Z) for i in range(peers)]
            groups.append([members[i] for i in PAIR_ORDER])
    return groups


def run_head(
    peers,
    hidden,
    norm_gain,
    value_weight,
    done_flags,
    valid_mask,
    new_logprob,
    old_logprob,
    discount,
    trace_decay,
    bootstrap,
):
    rollouts, length, width = hidden.shape
    f32 = jnp.float32
    steps = length.bit_length() - 1
    return pl.pallas_call(
        head_kernel,
        out_shape=(
            on_chip_shape((peers * HEAD_ROWS, 128)),
            on_chip_shape((rollouts, length)),
            on_chip_shape((rollouts * steps, length)),
            on_chip_shape((rollouts * steps // 2, length)),
            on_chip_shape((rollouts, length)),
            on_chip_shape((rollouts, length)),
            on_chip_shape((rollouts, 128)),
            on_chip_shape((rollouts, 128)),
            on_chip_shape((1, length)),
            on_chip_shape((1, 128)),
        ),
        in_specs=[ANY] * 10,
        out_specs=(VMEM,) * 10,
        scratch_shapes=[
            pltpu.VMEM(hidden.shape, hidden.dtype),
            pltpu.VMEM((width // 128, 128), norm_gain.dtype),
            pltpu.VMEM((width // 128, 128), value_weight.dtype),
            pltpu.VMEM(done_flags.shape, done_flags.dtype),
            pltpu.VMEM(valid_mask.shape, valid_mask.dtype),
            pltpu.VMEM(new_logprob.shape, f32),
            pltpu.VMEM(old_logprob.shape, f32),
            pltpu.SMEM(discount.shape, f32),
            pltpu.SMEM(trace_decay.shape, f32),
            pltpu.SMEM(bootstrap.shape, f32),
            pltpu.VMEM((2, length, 3 * 128), jnp.bfloat16),
            pltpu.VMEM((rollouts, 3 * 128, 128), jnp.bfloat16),
            pltpu.VMEM((length, 128), f32),
            pltpu.SemaphoreType.DMA((rollouts + 9,)),
        ],
        name="head",
    )(
        norm_gain.reshape(-1, 128),
        value_weight.reshape(-1, 128),
        done_flags,
        valid_mask,
        new_logprob,
        old_logprob,
        discount,
        trace_decay,
        bootstrap,
        hidden,
    )


def shards(
    hidden,
    norm_gain,
    value_weight,
    rewards,
    done_flags,
    valid_mask,
    new_logprob,
    old_logprob,
    discount,
    trace_decay,
    bootstrap,
):
    rollouts, length, width = hidden.shape
    peers, blocks = lax.axis_size("tensor"), lax.axis_size("seq")
    sent, gate, chain, triple, coef, power, fixed, trace, ratio, start = run_head(
        peers,
        hidden,
        norm_gain,
        value_weight,
        done_flags,
        valid_mask,
        new_logprob,
        old_logprob,
        discount,
        trace_decay,
        bootstrap,
    )
    got = exchange(sent.reshape(peers, 1, HEAD_ROWS * 128), "tensor", [TENSOR_ORDER])
    values, own, sent = pl.pallas_call(
        partial(local_kernel, width * peers),
        out_shape=(
            on_chip_shape((1, length)),
            on_chip_shape((1, length)),
            on_chip_shape((blocks * TOKEN_ROWS, 128)),
        ),
        in_specs=[VMEM] * 9,
        out_specs=(VMEM,) * 3,
        name="local",
    )(
        *map(
            on_chip,
            (
                got.reshape(peers * HEAD_ROWS, 128),
                rewards,
                gate,
                chain,
                triple,
                coef,
                fixed,
                trace,
                ratio,
            ),
        )
    )
    got = exchange(sent.reshape(blocks, 1, TOKEN_ROWS * 128), "seq", [order_from(blocks, SEQ_FIRST)])
    white, loss, sent = pl.pallas_call(
        final_kernel,
        out_shape=(
            on_chip_shape((1, length)),
            on_chip_shape((1, length)),
            on_chip_shape((2 * peers, 128)),
        ),
        in_specs=[VMEM] * 5,
        out_specs=(VMEM, VMEM, VMEM),
        name="final",
    )(*map(on_chip, (got.reshape(blocks * TOKEN_ROWS, 128), power, start, own, ratio)))
    groups = pair_groups(blocks, peers)
    got = exchange(sent.reshape(2 * peers, 1, 128), ("seq", "tensor"), groups)
    own_row = jax.ShapeDtypeStruct((1, length), jnp.float32)
    values, white, loss, policy = pl.pallas_call(
        last_kernel,
        out_shape=(own_row, own_row, own_row, jax.ShapeDtypeStruct((1, 1), jnp.float32)),
        in_specs=[VMEM] * 4,
        out_specs=(ANY,) * 4,
        scratch_shapes=[pltpu.SMEM((1, 1), jnp.float32), pltpu.SemaphoreType.DMA((4,))],
        name="last",
    )(*map(on_chip, (values, white, loss, got.reshape(2 * peers, 128))))
    return values, white, loss, policy.reshape(())


def solution(mesh):
    in_specs = (
        P(None, "seq", "tensor"),
        P("tensor"),
        P("tensor"),
        P(None, "seq"),
        P(None, "seq"),
        P("tensor", "seq"),
        P("tensor", "seq"),
        P("tensor", "seq"),
        P(),
        P(),
        P(),
    )
    out_specs = (P("tensor", "seq"), P("tensor", "seq"), P("tensor", "seq"), P())
    return jax.shard_map(
        shards, mesh=mesh, in_specs=in_specs, out_specs=out_specs, check_vma=False
    )
```
